8 devices in a mesh: dp: 1 (over z), tp: 8 (over y, x, core).
Axes of the slice: x: 2, y: 2, z: 1, core: 2. Of those that a mesh axis runs over, the one named last changes fastest.
Arguments:
- x_in: bfloat16 [3, 3072, 5376], P('dp', 'tp')
- positions: int32 [3, 3072], P('dp', 'tp')
- grad_out: bfloat16 [3, 3072, 5376], P('dp', 'tp')
- w_query: bfloat16 [5376, 32, 128], P(None, 'tp')
- w_key: bfloat16 [5376, 16, 128], P(None, 'tp')
- w_value: bfloat16 [5376, 16, 128], P(None, 'tp')
- w_out: bfloat16 [32, 128, 5376], P('tp')
- gain_pre: float32 [5376], replicated
- gain_post: float32 [5376], replicated
Outputs:
- output 1: bfloat16 [3, 3072, 5376], P('dp', 'tp')
- output 2: bfloat16 [3, 3072, 5376], P('dp', 'tp')
- output 3: float32 [5376, 32, 128], P('dp', 'tp')
- output 4: float32 [5376, 16, 128], P('dp', 'tp')
- output 5: float32 [5376, 16, 128], P('dp', 'tp')
- output 6: float32 [32, 128, 5376], P(('dp', 'tp'))
- output 7: float32 [5376], P('dp')
- output 8: float32 [5376], P('dp')
All inputs are finite; a program needn't handle non-finite values.
Results may differ from the reference program's by a relative error of at most 0.0177591.
Values are sent between devices in bfloat16 or wider.
A program may use at most 1 GiB of HBM per device.

```python
import functools
import jax
import jax.numpy as jnp
from jax import lax

BATCH_ROWS = 3
SEQ_LEN = 3072
MODEL_DIM = 5376
NUM_HEADS = 32
KV_HEADS = 16
HEAD_DIM = 128
WINDOW = 4096
QUERY_BLOCK = 128
SOFT_CAP = 50.0
NORM_EPS = 1e-6
ROPE_THETA = 10000.0


def draw_positions(pos_key, n_rows, seq_len):
    key_off, key_hit, key_jump = jax.random.split(pos_key, 3)
    offset = jax.random.randint(key_off, (n_rows, 1), 0, WINDOW)
    hit_draw = jax.random.randint(key_hit, (n_rows, seq_len), 0, max(seq_len // 8, 1))
    jump_size = jax.random.randint(key_jump, (n_rows, seq_len), 1, 2 * WINDOW)
    pos_steps = 1 + jnp.where(hit_draw == 0, jump_size, 0)
    return (offset + jnp.cumsum(pos_steps, axis=1) - pos_steps[:, :1]).astype(jnp.int32)


def setup_inputs(seed: int = 0, part: int = 0) -> dict:
    base_key = jax.random.key(seed)
    part_key = jax.random.fold_in(base_key, part)
    key_x, key_pos, key_dy = jax.random.split(part_key, 3)
    key_q, key_k, key_v, key_o, key_gp, key_gq = jax.random.split(base_key, 6)
    act_shape = (BATCH_ROWS, SEQ_LEN, MODEL_DIM)
    in_scale = MODEL_DIM ** -0.5
    out_scale = (NUM_HEADS * HEAD_DIM) ** -0.5
    x_in = jax.random.normal(key_x, act_shape, jnp.float32).astype(jnp.bfloat16)
    positions = draw_positions(key_pos, BATCH_ROWS, SEQ_LEN)
    grad_out = jax.random.normal(key_dy, act_shape, jnp.float32).astype(jnp.bfloat16)
    w_query = (jax.random.normal(key_q, (MODEL_DIM, NUM_HEADS, HEAD_DIM), jnp.float32) * in_scale).astype(jnp.bfloat16)
    w_key = (jax.random.normal(key_k, (MODEL_DIM, KV_HEADS, HEAD_DIM), jnp.float32) * in_scale).astype(jnp.bfloat16)
    w_value = (jax.random.normal(key_v, (MODEL_DIM, KV_HEADS, HEAD_DIM), jnp.float32) * in_scale).astype(jnp.bfloat16)
    w_out = (jax.random.normal(key_o, (NUM_HEADS, HEAD_DIM, MODEL_DIM), jnp.float32) * out_scale).astype(jnp.bfloat16)
    gain_pre = 0.5 * jax.random.normal(key_gp, (MODEL_DIM,), jnp.float32)
    gain_post = 0.5 * jax.random.normal(key_gq, (MODEL_DIM,), jnp.float32)
    return {'x_in': x_in, 'positions': positions, 'grad_out': grad_out, 'w_query': w_query, 'w_key': w_key, 'w_value': w_value, 'w_out': w_out, 'gain_pre': gain_pre, 'gain_post': gain_post}


def rms_norm(hidden, scale_w):
    values = hidden.astype(jnp.float32)
    inv_rms = lax.rsqrt(jnp.mean(values * values, axis=-1, keepdims=True) + NORM_EPS)
    return (values * inv_rms * (1.0 + scale_w)).astype(jnp.bfloat16)


def rope_tables(positions, head_dim):
    half_dim = head_dim // 2
    inv_freq = ROPE_THETA ** (-2.0 * jnp.arange(half_dim, dtype=jnp.float32) / head_dim)
    angles = positions.astype(jnp.float32)[:, :, None] * inv_freq
    return jnp.cos(angles)[:, :, None, :], jnp.sin(angles)[:, :, None, :]


def apply_rope(values, cos_t, sin_t):
    half_dim = values.shape[-1] // 2
    lo_half = values[..., :half_dim]
    hi_half = values[..., half_dim:]
    return jnp.concatenate([lo_half * cos_t - hi_half * sin_t, hi_half * cos_t + lo_half * sin_t], axis=-1)


def block_probs(q_blk, k_blk, pos_q, pos_k):
    scores = jnp.einsum('bqkgd,bskd->bkgqs', q_blk.astype(jnp.float32), k_blk.astype(jnp.float32))
    capped = SOFT_CAP * jnp.tanh(scores / SOFT_CAP)
    pos_gap = pos_q[:, :, None] - pos_k[:, None, :]
    in_window = ((pos_gap >= 0) & (pos_gap < WINDOW))[:, None, None, :, :]
    return jax.nn.softmax(jnp.where(in_window, capped, -1e30), axis=-1)


def attention(q_all, k_all, v_all, positions):
    seq_len = positions.shape[1]
    q_block = min(QUERY_BLOCK, seq_len)
    slab_len = min(WINDOW + q_block, seq_len)

    def one_block(blk_idx):
        q_start = blk_idx * q_block
        k_start = jnp.maximum(q_start + q_block - slab_len, 0)
        q_blk = lax.dynamic_slice_in_dim(q_all, q_start, q_block, axis=1)
        k_blk = lax.dynamic_slice_in_dim(k_all, k_start, slab_len, axis=1)
        v_blk = lax.dynamic_slice_in_dim(v_all, k_start, slab_len, axis=1)
        pos_q = lax.dynamic_slice_in_dim(positions, q_start, q_block, axis=1)
        pos_k = lax.dynamic_slice_in_dim(positions, k_start, slab_len, axis=1)
        prob_blk = block_probs(q_blk, k_blk, pos_q, pos_k)
        out_blk = jnp.einsum('bkgqs,bskd->bqkgd', prob_blk.astype(jnp.bfloat16).astype(jnp.float32), v_blk.astype(jnp.float32))
        return out_blk.astype(jnp.bfloat16)

    blocks = lax.map(jax.checkpoint(one_block), jnp.arange(seq_len // q_block))
    return jnp.moveaxis(blocks, 0, 1).reshape(q_all.shape)


def forward(positions, x_in, w_query, w_key, w_value, w_out, gain_pre, gain_post):
    n_rows, seq_len = positions.shape
    num_heads, head_dim = w_query.shape[1], w_query.shape[2]
    kv_heads = w_key.shape[1]
    normed = rms_norm(x_in, gain_pre).astype(jnp.float32)
    cos_t, sin_t = rope_tables(positions, head_dim)
    q_lin = jnp.einsum('bsd,dhe->bshe', normed, w_query.astype(jnp.float32))
    k_lin = jnp.einsum('bsd,dhe->bshe', normed, w_key.astype(jnp.float32))
    v_lin = jnp.einsum('bsd,dhe->bshe', normed, w_value.astype(jnp.float32))
    q_all = (apply_rope(q_lin, cos_t, sin_t) * head_dim ** -0.5).astype(jnp.bfloat16)
    q_all = q_all.reshape(n_rows, seq_len, kv_heads, num_heads // kv_heads, head_dim)
    k_all = apply_rope(k_lin, cos_t, sin_t).astype(jnp.bfloat16)
    v_all = v_lin.astype(jnp.bfloat16)
    attn_out = attention(q_all, k_all, v_all, positions).reshape(n_rows, seq_len, num_heads, head_dim)
    proj_out = jnp.einsum('bshe,hed->bsd', attn_out.astype(jnp.float32), w_out.astype(jnp.float32)).astype(jnp.bfloat16)
    post_norm = rms_norm(proj_out, gain_post)
    return (x_in.astype(jnp.float32) + post_norm.astype(jnp.float32)).astype(jnp.bfloat16)


def reference(x_in, positions, grad_out, w_query, w_key, w_value, w_out, gain_pre, gain_post):
    y_out, pullback = jax.vjp(functools.partial(forward, positions), x_in, w_query, w_key, w_value, w_out, gain_pre, gain_post)
    grad_x, grad_wq, grad_wk, grad_wv, grad_wo, grad_pre, grad_post = pullback(grad_out)
    return (y_out, grad_x, grad_wq.astype(jnp.float32), grad_wk.astype(jnp.float32), grad_wv.astype(jnp.float32), grad_wo.astype(jnp.float32), grad_pre.astype(jnp.float32), grad_post.astype(jnp.float32))
```

```python
import functools

import jax
import jax.numpy as jnp
from jax import lax
from jax.experimental import pallas as pl
from jax.experimental.pallas import tpu as pltpu
from jax.sharding import PartitionSpec as P


WINDOW = 4096
SOFT_CAP = 50.0
NORM_EPS = 1e-6
ROPE_THETA = 10000.0
LOG2E = 1.4426950408889634
BLK = 256
LANES = 128


def dot_f32(lhs, rhs, lhs_dim, rhs_dim):
    return lax.dot_general(lhs, rhs, (((lhs_dim,), (rhs_dim,)), ((), ())), preferred_element_type=jnp.float32)


ROWS = 128
CHUNK = 16


def row_specs(seq, depth):
    whole = pl.BlockSpec((1, ROWS, depth), lambda i: (seq, i, 0))
    one = pl.BlockSpec((ROWS, depth), lambda i: (i, 0))
    vec = pl.BlockSpec((1, depth), lambda i: (0, 0))
    return whole, one, vec


def inverse_rms(values):
    return lax.rsqrt(jnp.mean(values * values, axis=-1, keepdims=True) + NORM_EPS)


def norm_grad(values, inv, d_out, gain):
    scaled = d_out * gain
    dot = jnp.mean(scaled * values, axis=-1, keepdims=True)
    return scaled * inv - values * (inv * inv * inv * dot)


def fold_rows(block):
    return sum(block[r:r + 8] for r in range(0, CHUNK, 8))


def pre_norm_kernel(x_ref, gain_ref, n_ref):
    gain = 1.0 + gain_ref[...]

    @pl.loop(0, ROWS // CHUNK)
    def _(c):
        rows = pl.ds(pl.multiple_of(c * CHUNK, CHUNK), CHUNK)
        values = x_ref[0, rows, :].astype(jnp.float32)
        n_ref[rows, :] = (values * inverse_rms(values) * gain).astype(n_ref.dtype)


def pre_norm(x_in, gain, seq):
    _, rows, depth = x_in.shape
    whole, one, vec = row_specs(seq, depth)
    return pl.pallas_call(
        pre_norm_kernel,
        grid=(rows // ROWS,),
        in_specs=[whole, vec],
        out_specs=one,
        out_shape=jax.ShapeDtypeStruct((rows, depth), jnp.bfloat16),
        compiler_params=pltpu.CompilerParams(vmem_limit_bytes=32 * 1024 * 1024),
        cost_estimate=pl.CostEstimate(flops=rows * depth * 400, bytes_accessed=4 * rows * depth, transcendentals=rows),
        name="pre_norm",
    )(x_in, gain)


def post_norm_kernel(first, proj_ref, x_ref, go_ref, gain_ref, dg_in_ref, *refs):
    y_ref, d_proj_ref, dg_ref, dg_scr = refs[0 if first else 1:]
    step = pl.program_id(0)
    gain = 1.0 + gain_ref[...]

    @pl.when(step == 0)
    def _():
        dg_scr[...] = jnp.zeros_like(dg_scr)

    @pl.loop(0, ROWS // CHUNK)
    def _(c):
        rows = pl.ds(pl.multiple_of(c * CHUNK, CHUNK), CHUNK)
        values = proj_ref[rows, :].astype(jnp.float32)
        inv = inverse_rms(values)
        unit = values * inv
        post = (unit * gain).astype(jnp.bfloat16).astype(jnp.float32)
        y_ref[0, rows, :] = (x_ref[0, rows, :].astype(jnp.float32) + post).astype(y_ref.dtype)
        d_out = go_ref[0, rows, :].astype(jnp.float32)
        dg_scr[...] += fold_rows(d_out * unit)
        d_proj_ref[rows, :] = norm_grad(values, inv, d_out, gain).astype(d_proj_ref.dtype)

    @pl.when(step == pl.num_programs(0) - 1)
    def _():
        dg_ref[...] = dg_in_ref[...] + jnp.sum(dg_scr[...], axis=0, keepdims=True)


def post_norm(proj, x_in, grad_out, gain, dg_in, y_prev, seq):
    _, rows, depth = x_in.shape
    whole, one, vec = row_specs(seq, depth)
    first = y_prev is None
    return pl.pallas_call(
        functools.partial(post_norm_kernel, first),
        grid=(rows // ROWS,),
        in_specs=[one, whole, whole, vec, vec] + ([] if first else [pl.BlockSpec(memory_space=pl.ANY)]),
        out_specs=[whole, one, vec],
        out_shape=[
            jax.ShapeDtypeStruct(x_in.shape, jnp.bfloat16),
            jax.ShapeDtypeStruct((rows, depth), jnp.bfloat16),
            jax.ShapeDtypeStruct((1, depth), jnp.float32),
        ],
        scratch_shapes=[pltpu.VMEM((8, depth), jnp.float32)],
        input_output_aliases={} if first else {5: 0},
        compiler_params=pltpu.CompilerParams(vmem_limit_bytes=32 * 1024 * 1024),
        cost_estimate=pl.CostEstimate(flops=rows * depth * 800, bytes_accessed=10 * rows * depth, transcendentals=rows),
        name="post_norm",
    )(proj, x_in, grad_out, gain, dg_in, *([] if first else [y_prev]))


def pre_grad_kernel(first, dn_ref, x_ref, go_ref, gain_ref, dg_in_ref, *refs):
    gx_ref, dg_ref, dg_scr = refs[0 if first else 1:]
    step = pl.program_id(0)
    gain = 1.0 + gain_ref[...]

    @pl.when(step == 0)
    def _():
        dg_scr[...] = jnp.zeros_like(dg_scr)

    @pl.loop(0, ROWS // CHUNK)
    def _(c):
        rows = pl.ds(pl.multiple_of(c * CHUNK, CHUNK), CHUNK)
        values = x_ref[0, rows, :].astype(jnp.float32)
        inv = inverse_rms(values)
        d_out = dn_ref[rows, :].astype(jnp.float32)
        dg_scr[...] += fold_rows(d_out * (values * inv))
        d_x = norm_grad(values, inv, d_out, gain).astype(jnp.bfloat16).astype(jnp.float32)
        gx_ref[0, rows, :] = (go_ref[0, rows, :].astype(jnp.float32) + d_x).astype(gx_ref.dtype)

    @pl.when(step == pl.num_programs(0) - 1)
    def _():
        dg_ref[...] = dg_in_ref[...] + jnp.sum(dg_scr[...], axis=0, keepdims=True)


def pre_grad(d_normed, x_in, grad_out, gain, dg_in, gx_prev, seq):
    _, rows, depth = x_in.shape
    whole, one, vec = row_specs(seq, depth)
    first = gx_prev is None
    return pl.pallas_call(
        functools.partial(pre_grad_kernel, first),
        grid=(rows // ROWS,),
        in_specs=[one, whole, whole, vec, vec] + ([] if first else [pl.BlockSpec(memory_space=pl.ANY)]),
        out_specs=[whole, vec],
        out_shape=[jax.ShapeDtypeStruct(x_in.shape, jnp.bfloat16), jax.ShapeDtypeStruct((1, depth), jnp.float32)],
        scratch_shapes=[pltpu.VMEM((8, depth), jnp.float32)],
        input_output_aliases={} if first else {5: 0},
        compiler_params=pltpu.CompilerParams(vmem_limit_bytes=32 * 1024 * 1024),
        cost_estimate=pl.CostEstimate(flops=rows * depth * 700, bytes_accessed=8 * rows * depth, transcendentals=rows),
        name="pre_grad",
    )(d_normed, x_in, grad_out, gain, dg_in, *([] if first else [gx_prev]))


def out_proj_kernel(o_ref, w_ref, r_ref):
    o_all = jnp.concatenate([o_ref[d] for d in range(o_ref.shape[0])], axis=1)
    r_ref[...] = jnp.dot(o_all, w_ref[...], preferred_element_type=jnp.float32).astype(r_ref.dtype)


def out_proj(o_mine, w_all):
    n_dev, rows, cols = o_mine.shape
    depth = w_all.shape[1]
    tile = 768
    return pl.pallas_call(
        out_proj_kernel,
        grid=(depth // tile,),
        in_specs=[
            pl.BlockSpec((n_dev, rows, cols), lambda i: (0, 0, 0), pipeline_mode=pl.Buffered(1)),
            pl.BlockSpec((n_dev * cols, tile), lambda i: (0, i)),
        ],
        out_specs=pl.BlockSpec((rows, tile), lambda i: (0, i)),
        out_shape=jax.ShapeDtypeStruct((rows, depth), jnp.bfloat16),
        compiler_params=pltpu.CompilerParams(vmem_limit_bytes=40 * 1024 * 1024),
        cost_estimate=pl.CostEstimate(flops=2 * n_dev * rows * cols * depth, bytes_accessed=2 * n_dev * cols * depth, transcendentals=0),
        name="out_proj",
    )(o_mine, w_all)


def grad_w_kernel(n_rows, head_dim, *refs):
    a_refs, d_refs, outs = refs[:n_rows], refs[n_rows:2 * n_rows], refs[2 * n_rows:]
    total = dot_f32(a_refs[0][...], d_refs[0][...], 0, 0)
    for a_ref, d_ref in zip(a_refs[1:], d_refs[1:]):
        total = total + dot_f32(a_ref[...], d_ref[...], 0, 0)
    col = 0
    for out in outs:
        for h in range(out.shape[1]):
            out[:, h, :] = total[:, col:col + head_dim]
            col += head_dim


def grad_w(normed, d_lin, heads, head_dim):
    seq_len, depth = normed[0].shape
    cols = d_lin[0].shape[1]
    n_rows = len(normed)
    tile = 256
    return pl.pallas_call(
        functools.partial(grad_w_kernel, n_rows, head_dim),
        grid=(depth // tile,),
        in_specs=[pl.BlockSpec((seq_len, tile), lambda i: (0, i))] * n_rows
        + [pl.BlockSpec((seq_len, cols), lambda i: (0, 0), pipeline_mode=pl.Buffered(1))] * n_rows,
        out_specs=[pl.BlockSpec((tile, h, head_dim), lambda i: (i, 0, 0)) for h in heads],
        out_shape=[jax.ShapeDtypeStruct((depth, h, head_dim), jnp.float32) for h in heads],
        compiler_params=pltpu.CompilerParams(vmem_limit_bytes=58 * 1024 * 1024),
        cost_estimate=pl.CostEstimate(flops=2 * n_rows * seq_len * depth * cols, bytes_accessed=2 * n_rows * seq_len * (depth + cols), transcendentals=0),
        name="grad_w",
    )(*normed, *d_lin)


def qkv_kernel(q_cols, k_cols, head_dim, q_scale, a_ref, w_ref, cos_ref, sin_ref, q_ref, k_ref, v_ref):
    lin = jnp.dot(a_ref[...], w_ref[...], preferred_element_type=jnp.float32)
    cos_t, sin_t = cos_ref[...], sin_ref[...]
    for h in range((q_cols + k_cols) // head_dim):
        col = h * head_dim
        part = lin[:, col:col + head_dim]
        part = part * cos_t + pltpu.roll(part, head_dim // 2, 1) * sin_t
        if col < q_cols:
            q_ref[:, col:col + head_dim] = (part * q_scale).astype(q_ref.dtype)
        else:
            k_ref[:, col - q_cols:col - q_cols + head_dim] = part.astype(k_ref.dtype)
    v_ref[...] = lin[:, q_cols + k_cols:].astype(v_ref.dtype)


def qkv_project(normed, w_all, cos_t, sin_t, q_cols, k_cols, head_dim):
    rows, depth = normed.shape
    cols = w_all.shape[1]
    v_cols = cols - q_cols - k_cols
    tile = 512
    return pl.pallas_call(
        functools.partial(qkv_kernel, q_cols, k_cols, head_dim, head_dim ** -0.5),
        grid=(rows // tile,),
        in_specs=[
            pl.BlockSpec((tile, depth), lambda i: (i, 0)),
            pl.BlockSpec((depth, cols), lambda i: (0, 0), pipeline_mode=pl.Buffered(1)),
            pl.BlockSpec((tile, head_dim), lambda i: (i, 0)),
            pl.BlockSpec((tile, head_dim), lambda i: (i, 0)),
        ],
        out_specs=[
            pl.BlockSpec((tile, q_cols), lambda i: (i, 0)),
            pl.BlockSpec((tile, k_cols), lambda i: (i, 0)),
            pl.BlockSpec((tile, v_cols), lambda i: (i, 0)),
        ],
        out_shape=[
            jax.ShapeDtypeStruct((rows, q_cols), jnp.bfloat16),
            jax.ShapeDtypeStruct((rows, k_cols), jnp.bfloat16),
            jax.ShapeDtypeStruct((rows, v_cols), jnp.bfloat16),
        ],
        compiler_params=pltpu.CompilerParams(vmem_limit_bytes=56 * 1024 * 1024),
        cost_estimate=pl.CostEstimate(flops=2 * rows * depth * cols, bytes_accessed=2 * (rows * depth + depth * cols + rows * cols), transcendentals=0),
        name="qkv_project",
    )(normed, w_all, cos_t, sin_t)


def stack_heads(block, groups, head_dim):
    return jnp.concatenate([block[:, g * head_dim:(g + 1) * head_dim] for g in range(groups)], axis=0)


def attn_fwd_kernel(groups, head_dim, first_ref, q_ref, k_ref, v_ref, pos_ref, key_pos_ref, o_ref, lse_ref, m_scr, l_scr, acc_scr):
    blk = pl.program_id(1)
    q_all = stack_heads(q_ref[...], groups, head_dim)
    floor_row = jnp.concatenate([pos_ref[...]] * groups, axis=1) - WINDOW
    wide = groups * BLK

    def visit(kb, diagonal):
        start = pl.multiple_of(kb * BLK, BLK)
        k_blk = k_ref[pl.ds(start, BLK), :]
        v_blk = v_ref[pl.ds(start, BLK), :]
        scores = dot_f32(k_blk, q_all, 1, 1)
        capped = jnp.tanh(scores * (1.0 / SOFT_CAP)) * (SOFT_CAP * LOG2E)
        keep = jnp.concatenate([key_pos_ref[pl.ds(start, BLK), :]] * (wide // LANES), axis=1) > floor_row
        if diagonal:
            key_idx = lax.broadcasted_iota(jnp.int32, (BLK, wide), 0)
            q_idx = lax.broadcasted_iota(jnp.int32, (BLK, wide), 1) % BLK
            keep = keep & (key_idx <= q_idx)
        capped = jnp.where(keep, capped, -1e30)
        top = jnp.max(capped, axis=0, keepdims=True)
        if diagonal:
            prob = jnp.exp2(capped - top)
            m_scr[...] = top
            l_scr[...] = jnp.sum(prob, axis=0, keepdims=True)
            acc_scr[...] = dot_f32(v_blk, prob.astype(jnp.bfloat16), 0, 0)
        else:
            m_old = m_scr[...]
            m_new = jnp.maximum(m_old, top)
            alpha = jnp.exp2(m_old - m_new)
            prob = jnp.exp2(capped - m_new)
            m_scr[...] = m_new
            l_scr[...] = l_scr[...] * alpha + jnp.sum(prob, axis=0, keepdims=True)
            acc_scr[...] = acc_scr[...] * alpha + dot_f32(v_blk, prob.astype(jnp.bfloat16), 0, 0)

    visit(blk, True)

    @pl.loop(first_ref[blk], blk)
    def _(kb):
        visit(kb, False)

    total = l_scr[...]
    out = (acc_scr[...] / total).T
    for g in range(groups):
        o_ref[:, g * head_dim:(g + 1) * head_dim] = out[g * BLK:(g + 1) * BLK, :].astype(o_ref.dtype)
    lse_ref[0, 0] = m_scr[...] + jnp.log2(total)


def attn_fwd(q_all, k_all, v_all, pos, key_pos, first_blk, groups, head_dim):
    seq_len, q_cols = q_all.shape
    kv_heads = k_all.shape[1] // head_dim
    n_blk = seq_len // BLK
    wide = groups * BLK
    pairs = seq_len * seq_len // 4 * groups * kv_heads
    return pl.pallas_call(
        functools.partial(attn_fwd_kernel, groups, head_dim),
        grid_spec=pltpu.PrefetchScalarGridSpec(
            num_scalar_prefetch=1,
            grid=(kv_heads, n_blk),
            in_specs=[
                pl.BlockSpec((BLK, groups * head_dim), lambda h, i, first: (i, h)),
                pl.BlockSpec((seq_len, head_dim), lambda h, i, first: (0, h)),
                pl.BlockSpec((seq_len, head_dim), lambda h, i, first: (0, h)),
                pl.BlockSpec((1, BLK), lambda h, i, first: (0, i)),
                pl.BlockSpec((seq_len, LANES), lambda h, i, first: (0, 0)),
            ],
            out_specs=[
                pl.BlockSpec((BLK, groups * head_dim), lambda h, i, first: (i, h)),
                pl.BlockSpec((1, 1, 1, wide), lambda h, i, first: (h, i, 0, 0)),
            ],
            scratch_shapes=[
                pltpu.VMEM((1, wide), jnp.float32),
                pltpu.VMEM((1, wide), jnp.float32),
                pltpu.VMEM((head_dim, wide), jnp.float32),
            ],
        ),
        out_shape=[
            jax.ShapeDtypeStruct((seq_len, q_cols), jnp.bfloat16),
            jax.ShapeDtypeStruct((kv_heads, n_blk, 1, wide), jnp.float32),
        ],
        compiler_params=pltpu.CompilerParams(vmem_limit_bytes=48 * 1024 * 1024),
        cost_estimate=pl.CostEstimate(flops=8 * pairs * head_dim, bytes_accessed=8 * seq_len * q_cols, transcendentals=2 * pairs),
        name="attn_fwd",
    )(first_blk, q_all, k_all, v_all, pos, key_pos)


def attn_bwd_kernel(groups, head_dim, q_scale, first_ref, q_ref, k_ref, v_ref, o_ref, do_ref, pos_ref, key_pos_ref, lse_ref, cos_ref, sin_ref,
                    out_ref, dq_scr, dk_scr, dv_scr, dq_out, dk_out, dv_out, dq_sem, kv_sem):
    head, blk = pl.program_id(0), pl.program_id(1)
    n_head, n_blk = pl.num_programs(0), pl.num_programs(1)
    half = head_dim // 2
    wide = groups * BLK
    q_width = groups * head_dim
    slot = blk % 2

    @pl.when(blk == 0)
    def _():
        dk_scr[...] = jnp.zeros_like(dk_scr)
        dv_scr[...] = jnp.zeros_like(dv_scr)

    q_all = stack_heads(q_ref[...], groups, head_dim)
    do_all = stack_heads(do_ref[...], groups, head_dim)
    o_all = stack_heads(o_ref[...], groups, head_dim)
    floor_row = jnp.concatenate([pos_ref[...]] * groups, axis=1) - WINDOW
    lse_row = lse_ref[0, 0]
    delta = jnp.sum((do_all.astype(jnp.float32) * o_all.astype(jnp.float32)).T, axis=0, keepdims=True)

    def visit(kb, diagonal):
        start = pl.multiple_of(kb * BLK, BLK)
        k_blk = k_ref[pl.ds(start, BLK), :]
        v_blk = v_ref[pl.ds(start, BLK), :]
        scores = dot_f32(k_blk, q_all, 1, 1)
        d_prob = dot_f32(v_blk, do_all, 1, 1)
        tanh_s = jnp.tanh(scores * (1.0 / SOFT_CAP))
        keep = jnp.concatenate([key_pos_ref[pl.ds(start, BLK), :]] * (wide // LANES), axis=1) > floor_row
        if diagonal:
            key_idx = lax.broadcasted_iota(jnp.int32, (BLK, wide), 0)
            q_idx = lax.broadcasted_iota(jnp.int32, (BLK, wide), 1) % BLK
            keep = keep & (key_idx <= q_idx)
        prob = jnp.exp2(jnp.where(keep, tanh_s * (SOFT_CAP * LOG2E) - lse_row, -1e30))
        d_score = (prob * (d_prob - delta) * (1.0 - tanh_s * tanh_s)).astype(jnp.bfloat16)
        dv_scr[pl.ds(start, BLK), :] += jnp.dot(prob.astype(jnp.bfloat16), do_all, preferred_element_type=jnp.float32)
        dk_scr[pl.ds(start, BLK), :] += jnp.dot(d_score, q_all, preferred_element_type=jnp.float32)
        dq_new = dot_f32(k_blk, d_score, 0, 0)
        if diagonal:
            dq_scr[...] = dq_new
        else:
            dq_scr[...] += dq_new

    visit(blk, True)

    @pl.loop(first_ref[blk], blk)
    def _(kb):
        visit(kb, False)

    def dq_copy(h, i):
        dst = out_ref.at[pl.ds(pl.multiple_of(i * BLK, BLK), BLK), pl.ds(pl.multiple_of(h * q_width, q_width), q_width)]
        return pltpu.make_async_copy(dq_out.at[slot], dst, dq_sem.at[slot])

    def kv_copy(which, src, h):
        col = n_head * q_width + which * n_head * head_dim + h * head_dim
        dst = out_ref.at[:, pl.ds(pl.multiple_of(col, head_dim), head_dim)]
        return pltpu.make_async_copy(src, dst, kv_sem.at[which])

    @pl.when(head * n_blk + blk >= 2)
    def _():
        dq_copy(head, blk).wait()

    d_q = dq_scr[...].T
    rows = pl.ds(pl.multiple_of(blk * BLK, BLK), BLK)
    cos_t, sin_t = cos_ref[rows, :], sin_ref[rows, :]
    for g in range(groups):
        part = d_q[g * BLK:(g + 1) * BLK, :]
        part = (part * cos_t - pltpu.roll(part, half, 1) * sin_t) * q_scale
        dq_out[slot, :, g * head_dim:(g + 1) * head_dim] = part.astype(dq_out.dtype)
    dq_copy(head, blk).start()

    @pl.when(blk == n_blk - 1)
    def _():
        @pl.loop(0, n_blk)
        def _(i):
            rows = pl.ds(pl.multiple_of(i * BLK, BLK), BLK)
            part = dk_scr[rows, :]
            part = part * cos_ref[rows, :] - pltpu.roll(part, half, 1) * sin_ref[rows, :]
            dk_out[rows, :] = part.astype(dk_out.dtype)
            dv_out[rows, :] = dv_scr[rows, :].astype(dv_out.dtype)

        kv_copy(0, dk_out, head).start()
        kv_copy(1, dv_out, head).start()
        kv_copy(0, dk_out, head).wait()
        kv_copy(1, dv_out, head).wait()

    @pl.when((blk == n_blk - 1) & (head == n_head - 1))
    def _():
        for s in range(2):
            pltpu.make_async_copy(dq_out.at[s], out_ref.at[pl.ds(0, BLK), pl.ds(0, q_width)], dq_sem.at[s]).wait()


def attn_bwd(q_all, k_all, v_all, o_all, d_o, pos, key_pos, lse, first_blk, cos_t, sin_t, groups, head_dim):
    seq_len, q_cols = q_all.shape
    k_cols = k_all.shape[1]
    kv_heads = k_cols // head_dim
    n_blk = seq_len // BLK
    wide = groups * BLK
    pairs = seq_len * seq_len // 4 * groups * kv_heads
    by_q = pl.BlockSpec((BLK, groups * head_dim), lambda h, i, first: (i, h))
    by_h = pl.BlockSpec((seq_len, head_dim), lambda h, i, first: (0, h))
    table = pl.BlockSpec((seq_len, LANES), lambda h, i, first: (0, 0))
    return pl.pallas_call(
        functools.partial(attn_bwd_kernel, groups, head_dim, head_dim ** -0.5),
        grid_spec=pltpu.PrefetchScalarGridSpec(
            num_scalar_prefetch=1,
            grid=(kv_heads, n_blk),
            in_specs=[
                by_q, by_h, by_h, by_q, by_q,
                pl.BlockSpec((1, BLK), lambda h, i, first: (0, i)),
                table,
                pl.BlockSpec((1, 1, 1, wide), lambda h, i, first: (h, i, 0, 0)),
                table, table,
            ],
            out_specs=pl.BlockSpec(memory_space=pl.ANY),
            scratch_shapes=[
                pltpu.VMEM((head_dim, wide), jnp.float32),
                pltpu.VMEM((seq_len, head_dim), jnp.float32),
                pltpu.VMEM((seq_len, head_dim), jnp.float32),
                pltpu.VMEM((2, BLK, groups * head_dim), jnp.bfloat16),
                pltpu.VMEM((seq_len, head_dim), jnp.bfloat16),
                pltpu.VMEM((seq_len, head_dim), jnp.bfloat16),
                pltpu.SemaphoreType.DMA((2,)),
                pltpu.SemaphoreType.DMA((2,)),
            ],
        ),
        out_shape=jax.ShapeDtypeStruct((seq_len, q_cols + 2 * k_cols), jnp.bfloat16),
        compiler_params=pltpu.CompilerParams(vmem_limit_bytes=48 * 1024 * 1024),
        cost_estimate=pl.CostEstimate(flops=20 * pairs * head_dim, bytes_accessed=16 * seq_len * q_cols, transcendentals=2 * pairs),
        name="attn_bwd",
    )(first_blk, q_all, k_all, v_all, o_all, d_o, pos, key_pos, lse, cos_t, sin_t)


def solution(mesh):
    act_spec = P('dp', 'tp', None)
    head_spec = P(None, 'tp', None)
    grad_spec = P('dp', 'tp', None)
    in_specs = (act_spec, P('dp', 'tp'), act_spec, head_spec, head_spec, head_spec, P('tp', None, None), P(None), P(None))
    out_specs = (act_spec, act_spec, grad_spec, grad_spec, grad_spec, P(('dp', 'tp'), None, None), P('dp'), P('dp'))

    def local_body(x_in, positions, grad_out, w_query, w_key, w_value, w_out, gain_pre, gain_post):
        n_rows, _, depth = x_in.shape
        heads_loc, head_dim = w_query.shape[1], w_query.shape[2]
        kv_loc = w_key.shape[1]
        groups = heads_loc // kv_loc
        q_cols, k_cols = heads_loc * head_dim, kv_loc * head_dim

        gain_pre_row, gain_post_row = gain_pre[None, :], gain_post[None, :]
        normed_all = []
        for b in range(n_rows):
            normed = pre_norm(x_in, gain_pre_row, b)
            normed_all.append(lax.all_gather(normed, 'tp', axis=0, tiled=True))
        w_out_loc = w_out.reshape(q_cols, depth)
        w_out_all = lax.all_gather(w_out_loc, 'tp', axis=0, tiled=True)

        pos_all = lax.all_gather(positions, 'tp', axis=1, tiled=True)
        seq_len = pos_all.shape[1]
        half = head_dim // 2
        inv_freq = ROPE_THETA ** (-2.0 * jnp.arange(half, dtype=jnp.float32) / head_dim)
        before = pos_all[:, None, :] <= pos_all[:, ::BLK, None] - WINDOW
        first_blk = jnp.sum(before.astype(jnp.int32), axis=-1) // BLK
        w_all = jnp.concatenate([w_query.reshape(depth, q_cols), w_key.reshape(depth, k_cols), w_value.reshape(depth, k_cols)], axis=1)

        saved, d_proj_all = [], []
        y_out, d_post = None, jnp.zeros((1, depth), jnp.float32)
        for b in range(n_rows):
            angles = pos_all[b].astype(jnp.float32)[:, None] * inv_freq
            cos_h, sin_h = jnp.cos(angles), jnp.sin(angles)
            cos_t = jnp.concatenate([cos_h, cos_h], axis=-1)
            sin_t = jnp.concatenate([-sin_h, sin_h], axis=-1)
            pos_b = pos_all[b][None, :]
            key_pos = jnp.broadcast_to(pos_all[b][:, None], (seq_len, LANES))
            q_b, k_b, v_b = qkv_project(normed_all[b], w_all, cos_t, sin_t, q_cols, k_cols, head_dim)
            o_b, lse_b = attn_fwd(q_b, k_b, v_b, pos_b, key_pos, first_blk[b], groups, head_dim)
            o_mine = lax.all_to_all(o_b.reshape(-1, seq_len // mesh.shape['tp'], q_cols), 'tp', split_axis=0, concat_axis=0, tiled=True)
            proj = out_proj(o_mine, w_out_all)
            y_out, d_proj, d_post = post_norm(proj, x_in, grad_out, gain_post_row, d_post, y_out, b)
            d_proj_all.append(lax.all_gather(d_proj, 'tp', axis=0, tiled=True))
            saved.append((q_b, k_b, v_b, o_b, pos_b, key_pos, lse_b, cos_t, sin_t))

        grad_x, d_pre = None, jnp.zeros((1, depth), jnp.float32)
        grad_wo = jnp.zeros((), jnp.float32)
        d_lin = []
        for b in range(n_rows):
            q_b, k_b, v_b, o_b, pos_b, key_pos, lse_b, cos_t, sin_t = saved[b]
            d_o = dot_f32(d_proj_all[b], w_out_loc, 1, 1).astype(jnp.bfloat16)
            d_lin.append(attn_bwd(q_b, k_b, v_b, o_b, d_o, pos_b, key_pos, lse_b, first_blk[b], cos_t, sin_t, groups, head_dim))
            d_normed = dot_f32(d_lin[b], w_all, 1, 1).astype(jnp.bfloat16)
            d_normed_loc = lax.psum_scatter(d_normed, 'tp', scatter_dimension=0, tiled=True)
            grad_x, d_pre = pre_grad(d_normed_loc, x_in, grad_out, gain_pre_row, d_pre, grad_x, b)
            grad_wo = grad_wo + dot_f32(o_b, d_proj_all[b], 0, 0)

        grad_wq, grad_wk, grad_wv = grad_w(normed_all, d_lin, (heads_loc, kv_loc, kv_loc), head_dim)
        grad_pre = lax.psum(d_pre[0], 'tp')
        grad_post = lax.psum(d_post[0], 'tp')
        return y_out, grad_x, grad_wq, grad_wk, grad_wv, grad_wo.reshape(w_out.shape), grad_pre, grad_post

    return jax.shard_map(local_body, mesh=mesh, in_specs=in_specs, out_specs=out_specs, check_vma=False)
```

```python
import functools

import jax
import jax.numpy as jnp
from jax import lax
from jax.experimental import pallas as pl
from jax.experimental.pallas import tpu as pltpu
from jax.sharding import PartitionSpec as P


WINDOW = 4096
SOFT_CAP = 50.0
NORM_EPS = 1e-6
ROPE_THETA = 10000.0
LOG2E = 1.4426950408889634
BLK = 256
LANES = 128


def dot_f32(lhs, rhs, lhs_dim, rhs_dim):
    return lax.dot_general(lhs, rhs, (((lhs_dim,), (rhs_dim,)), ((), ())), preferred_element_type=jnp.float32)


ROWS = 128
CHUNK = 16


def row_specs(seq, depth):
    whole = pl.BlockSpec((1, ROWS, depth), lambda i: (seq, i, 0))
    one = pl.BlockSpec((ROWS, depth), lambda i: (i, 0))
    vec = pl.BlockSpec((1, depth), lambda i: (0, 0))
    return whole, one, vec


def inverse_rms(values):
    return lax.rsqrt(jnp.mean(values * values, axis=-1, keepdims=True) + NORM_EPS)


def norm_grad(values, inv, d_out, gain):
    scaled = d_out * gain
    dot = jnp.mean(scaled * values, axis=-1, keepdims=True)
    return scaled * inv - values * (inv * inv * inv * dot)


def fold_rows(block):
    return sum(block[r:r + 8] for r in range(0, CHUNK, 8))


def pre_norm_kernel(x_ref, gain_ref, n_ref):
    gain = 1.0 + gain_ref[...]

    @pl.loop(0, ROWS // CHUNK)
    def _(c):
        rows = pl.ds(pl.multiple_of(c * CHUNK, CHUNK), CHUNK)
        values = x_ref[0, rows, :].astype(jnp.float32)
        n_ref[rows, :] = (values * inverse_rms(values) * gain).astype(n_ref.dtype)


def pre_norm(x_in, gain, seq):
    _, rows, depth = x_in.shape
    whole, one, vec = row_specs(seq, depth)
    return pl.pallas_call(
        pre_norm_kernel,
        grid=(rows // ROWS,),
        in_specs=[whole, vec],
        out_specs=one,
        out_shape=jax.ShapeDtypeStruct((rows, depth), jnp.bfloat16),
        compiler_params=pltpu.CompilerParams(vmem_limit_bytes=54 * 1024 * 1024),
        cost_estimate=pl.CostEstimate(flops=rows * depth * 400, bytes_accessed=4 * rows * depth, transcendentals=rows),
        name="pre_norm",
    )(x_in, gain)


def post_norm_kernel(first, proj_ref, x_ref, go_ref, gain_ref, dg_in_ref, *refs):
    y_ref, d_proj_ref, dg_ref, dg_scr = refs[0 if first else 1:]
    step = pl.program_id(0)
    gain = 1.0 + gain_ref[...]

    @pl.when(step == 0)
    def _():
        dg_scr[...] = jnp.zeros_like(dg_scr)

    @pl.loop(0, ROWS // CHUNK)
    def _(c):
        rows = pl.ds(pl.multiple_of(c * CHUNK, CHUNK), CHUNK)
        values = proj_ref[rows, :].astype(jnp.float32)
        inv = inverse_rms(values)
        unit = values * inv
        post = (unit * gain).astype(jnp.bfloat16).astype(jnp.float32)
        y_ref[0, rows, :] = (x_ref[0, rows, :].astype(jnp.float32) + post).astype(y_ref.dtype)
        d_out = go_ref[0, rows, :].astype(jnp.float32)
        dg_scr[...] += fold_rows(d_out * unit)
        d_proj_ref[rows, :] = norm_grad(values, inv, d_out, gain).astype(d_proj_ref.dtype)

    @pl.when(step == pl.num_programs(0) - 1)
    def _():
        dg_ref[...] = dg_in_ref[...] + jnp.sum(dg_scr[...], axis=0, keepdims=True)


def post_norm(proj, x_in, grad_out, gain, dg_in, y_prev, seq):
    _, rows, depth = x_in.shape
    whole, one, vec = row_specs(seq, depth)
    first = y_prev is None
    return pl.pallas_call(
        functools.partial(post_norm_kernel, first),
        grid=(rows // ROWS,),
        in_specs=[one, whole, whole, vec, vec] + ([] if first else [pl.BlockSpec(memory_space=pl.ANY)]),
        out_specs=[whole, one, vec],
        out_shape=[
            jax.ShapeDtypeStruct(x_in.shape, jnp.bfloat16),
            jax.ShapeDtypeStruct((rows, depth), jnp.bfloat16),
            jax.ShapeDtypeStruct((1, depth), jnp.float32),
        ],
        scratch_shapes=[pltpu.VMEM((8, depth), jnp.float32)],
        input_output_aliases={} if first else {5: 0},
        compiler_params=pltpu.CompilerParams(vmem_limit_bytes=54 * 1024 * 1024),
        cost_estimate=pl.CostEstimate(flops=rows * depth * 800, bytes_accessed=10 * rows * depth, transcendentals=rows),
        name="post_norm",
    )(proj, x_in, grad_out, gain, dg_in, *([] if first else [y_prev]))


def pre_grad_kernel(first, *refs):
    pieces, (x_ref, go_ref, gain_ref, dg_in_ref), refs = refs[:6], refs[6:10], refs[10:]
    gx_ref, dg_ref, dg_scr = refs[0 if first else 1:]
    step = pl.program_id(0)
    gain = 1.0 + gain_ref[...]

    @pl.when(step == 0)
    def _():
        dg_scr[...] = jnp.zeros_like(dg_scr)

    @pl.loop(0, ROWS // CHUNK)
    def _(c):
        rows = pl.ds(pl.multiple_of(c * CHUNK, CHUNK), CHUNK)
        values = x_ref[0, rows, :].astype(jnp.float32)
        inv = inverse_rms(values)
        halves = []
        for kept, near, far in (pieces[:3], pieces[3:]):
            halves.append(kept[0, rows, :].astype(jnp.float32) + near[0, rows, :].astype(jnp.float32) + far[rows, :].astype(jnp.float32))
        d_out = jnp.concatenate(halves, axis=1)
        dg_scr[...] += fold_rows(d_out * (values * inv))
        d_x = norm_grad(values, inv, d_out, gain).astype(jnp.bfloat16).astype(jnp.float32)
        gx_ref[0, rows, :] = (go_ref[0, rows, :].astype(jnp.float32) + d_x).astype(gx_ref.dtype)

    @pl.when(step == pl.num_programs(0) - 1)
    def _():
        dg_ref[...] = dg_in_ref[...] + jnp.sum(dg_scr[...], axis=0, keepdims=True)


def pre_grad(pieces, x_in, grad_out, gain, dg_in, gx_prev, seq):
    _, rows, depth = x_in.shape
    whole, _, vec = row_specs(seq, depth)
    pair = pl.BlockSpec((1, ROWS, depth // 2), lambda i: (0, i, 0))
    one = pl.BlockSpec((ROWS, depth // 2), lambda i: (i, 0))
    first = gx_prev is None
    return pl.pallas_call(
        functools.partial(pre_grad_kernel, first),
        grid=(rows // ROWS,),
        in_specs=[pair, pair, one, pair, pair, one, whole, whole, vec, vec] + ([] if first else [pl.BlockSpec(memory_space=pl.ANY)]),
        out_specs=[whole, vec],
        out_shape=[jax.ShapeDtypeStruct(x_in.shape, jnp.bfloat16), jax.ShapeDtypeStruct((1, depth), jnp.float32)],
        scratch_shapes=[pltpu.VMEM((8, depth), jnp.float32)],
        input_output_aliases={} if first else {10: 0},
        compiler_params=pltpu.CompilerParams(vmem_limit_bytes=54 * 1024 * 1024),
        cost_estimate=pl.CostEstimate(flops=rows * depth * 700, bytes_accessed=12 * rows * depth, transcendentals=rows),
        name="pre_grad",
    )(*pieces, x_in, grad_out, gain, dg_in, *([] if first else [gx_prev]))


def out_proj_kernel(o_ref, w_ref, r_ref):
    o_all = jnp.concatenate([o_ref[d] for d in range(o_ref.shape[0])], axis=1)
    r_ref[...] = jnp.dot(o_all, w_ref[...], preferred_element_type=jnp.float32).astype(r_ref.dtype)


def out_proj(o_mine, w_all):
    n_dev, rows, cols = o_mine.shape
    depth = w_all.shape[1]
    tile = 768
    return pl.pallas_call(
        out_proj_kernel,
        grid=(depth // tile,),
        in_specs=[
            pl.BlockSpec((n_dev, rows, cols), lambda i: (0, 0, 0), pipeline_mode=pl.Buffered(1)),
            pl.BlockSpec((n_dev * cols, tile), lambda i: (0, i)),
        ],
        out_specs=pl.BlockSpec((rows, tile), lambda i: (0, i)),
        out_shape=jax.ShapeDtypeStruct((rows, depth), jnp.bfloat16),
        compiler_params=pltpu.CompilerParams(vmem_limit_bytes=54 * 1024 * 1024),
        cost_estimate=pl.CostEstimate(flops=2 * n_dev * rows * cols * depth, bytes_accessed=2 * n_dev * cols * depth, transcendentals=0),
        name="out_proj",
    )(o_mine, w_all)


def pair_core_kernel(dst_ref, d_ref, w_ref, out_ref):
    out_ref[0] = jnp.dot(d_ref[...], w_ref[...], preferred_element_type=jnp.float32).astype(out_ref.dtype)


def grad_normed_pair(dst, d_lin, w_t, rows):
    cols, depth = w_t.shape
    half = depth // 2
    return pl.pallas_call(
        pair_core_kernel,
        grid_spec=pltpu.PrefetchScalarGridSpec(
            num_scalar_prefetch=1,
            grid=(2, 4),
            in_specs=[
                pl.BlockSpec((rows, cols), lambda h, r, dst: (dst[0] ^ (2 * r), 0)),
                pl.BlockSpec((cols, half), lambda h, r, dst: (0, h)),
            ],
            out_specs=pl.BlockSpec((1, rows, half), lambda h, r, dst: (r, 0, h)),
        ),
        out_shape=jax.ShapeDtypeStruct((4, rows, depth), jnp.bfloat16),
        compiler_params=pltpu.CompilerParams(vmem_limit_bytes=48 * 1024 * 1024),
        cost_estimate=pl.CostEstimate(flops=8 * rows * cols * depth, bytes_accessed=2 * (4 * rows * depth + cols * depth), transcendentals=0),
        name="grad_normed_pair",
    )(dst, d_lin, w_t)


def route(h, j):
    return jnp.where(h == 0, (2 * j + 1) % 5, (j + 2) % 4)


def own_core_kernel(dst_ref, d_ref, w_ref, add_ref, *outs):
    step = 4 * pl.program_id(0) + pl.program_id(1)
    value = jnp.dot(d_ref[...], w_ref[...], preferred_element_type=jnp.float32) + add_ref[0].astype(jnp.float32)
    value = value.astype(jnp.bfloat16)
    for i, out in enumerate(outs):
        @pl.when((step >= 2 * i) & (step < 2 * i + 2))
        def _(out=out):
            out[0] = value


def grad_normed_own(dst, d_lin, w_t, from_pair):
    _, rows, depth = from_pair.shape
    cols = w_t.shape[0]
    half = depth // 2
    outs = [pl.BlockSpec((1, rows, half), lambda h, j, dst, i=i: (jnp.clip(4 * h + j - 2 * i, 0, 1), 0, 0)) for i in range(4)]
    return pl.pallas_call(
        own_core_kernel,
        grid_spec=pltpu.PrefetchScalarGridSpec(
            num_scalar_prefetch=1,
            grid=(2, 4),
            in_specs=[
                pl.BlockSpec((rows, cols), lambda h, j, dst: (dst[0] ^ (2 * route(h, j)), 0)),
                pl.BlockSpec((cols, half), lambda h, j, dst: (0, h)),
                pl.BlockSpec((1, rows, half), lambda h, j, dst: (route(h, j), 0, h)),
            ],
            out_specs=outs,
        ),
        out_shape=[jax.ShapeDtypeStruct((2, rows, half), jnp.bfloat16)] * 4,
        compiler_params=pltpu.CompilerParams(vmem_limit_bytes=56 * 1024 * 1024),
        cost_estimate=pl.CostEstimate(flops=8 * rows * cols * depth, bytes_accessed=2 * (8 * rows * depth + cols * depth), transcendentals=0),
        name="grad_normed_own",
    )(dst, d_lin, w_t, from_pair)


def gain_sum_kernel(n_dev, pre_ref, post_ref, pre_out, post_out, slots, local_sem, send_sem, recv_sem):
    me = lax.axis_index('tp')
    sources = (pre_ref, post_ref)
    sends, locals_ = [], []
    for off in range(1, n_dev):
        for which, src in enumerate(sources):
            copy = pltpu.make_async_remote_copy(
                src_ref=src, dst_ref=slots.at[which, me], send_sem=send_sem.at[which, off], recv_sem=recv_sem.at[which, me],
                device_id={'tp': lax.rem(me + off, n_dev)}, device_id_type=pl.DeviceIdType.MESH)
            copy.start()
            sends.append(copy)
    for which, src in enumerate(sources):
        copy = pltpu.make_async_copy(src, slots.at[which, me], local_sem.at[which])
        copy.start()
        locals_.append(copy)
    for copy in locals_:
        copy.wait()
    for off in range(1, n_dev):
        other = lax.rem(me + off, n_dev)
        for which, src in enumerate(sources):
            pltpu.make_async_remote_copy(
                src_ref=src, dst_ref=slots.at[which, other], send_sem=send_sem.at[which, off], recv_sem=recv_sem.at[which, other],
                device_id={'tp': other}, device_id_type=pl.DeviceIdType.MESH).wait_recv()
    for copy in sends:
        copy.wait_send()
    for which, out in enumerate((pre_out, post_out)):
        total = slots[which, 0]
        for d in range(1, n_dev):
            total = total + slots[which, d]
        out[...] = total


def gain_sum(d_pre, d_post, n_dev):
    depth = d_pre.shape[1]
    vmem = pl.BlockSpec(memory_space=pltpu.VMEM)
    return pl.pallas_call(
        functools.partial(gain_sum_kernel, n_dev),
        in_specs=[vmem, vmem],
        out_specs=[vmem, vmem],
        out_shape=[jax.ShapeDtypeStruct((1, depth), jnp.float32)] * 2,
        scratch_shapes=[
            pltpu.VMEM((2, n_dev, 1, depth), jnp.float32),
            pltpu.SemaphoreType.DMA((2,)),
            pltpu.SemaphoreType.DMA((2, n_dev)),
            pltpu.SemaphoreType.DMA((2, n_dev)),
        ],
        compiler_params=pltpu.CompilerParams(has_side_effects=True),
        name="gain_sum",
    )(d_pre, d_post)


def grad_w_kernel(n_rows, head_dim, *refs):
    a_refs, d_refs, outs = refs[:n_rows], refs[n_rows:2 * n_rows], refs[2 * n_rows:]
    total = dot_f32(a_refs[0][...], d_refs[0][...], 0, 0)
    for a_ref, d_ref in zip(a_refs[1:], d_refs[1:]):
        total = total + dot_f32(a_ref[...], d_ref[...], 0, 0)
    col = 0
    for out in outs:
        for h in range(out.shape[1]):
            out[:, h, :] = total[:, col:col + head_dim]
            col += head_dim


def grad_w(normed, d_lin, heads, head_dim, col_blk):
    seq_len, depth = normed[0].shape
    cols = sum(heads) * head_dim
    n_rows = len(normed)
    tile = 384
    return pl.pallas_call(
        functools.partial(grad_w_kernel, n_rows, head_dim),
        grid=(depth // tile,),
        in_specs=[pl.BlockSpec((seq_len, tile), lambda i: (0, i))] * n_rows
        + [pl.BlockSpec((seq_len, cols), lambda i: (0, col_blk), pipeline_mode=pl.Buffered(1))] * n_rows,
        out_specs=[pl.BlockSpec((tile, h, head_dim), lambda i: (i, 0, 0)) for h in heads],
        out_shape=[jax.ShapeDtypeStruct((depth, h, head_dim), jnp.float32) for h in heads],
        compiler_params=pltpu.CompilerParams(vmem_limit_bytes=58 * 1024 * 1024),
        cost_estimate=pl.CostEstimate(flops=2 * n_rows * seq_len * depth * cols, bytes_accessed=2 * n_rows * seq_len * (depth + cols), transcendentals=0),
        name="grad_w",
    )(*normed, *d_lin)


def qkv_kernel(q_cols, k_cols, head_dim, q_scale, a_ref, w_ref, cos_ref, sin_ref, q_ref, k_ref, v_ref):
    lin = jnp.dot(a_ref[...], w_ref[...], preferred_element_type=jnp.float32)
    cos_t, sin_t = cos_ref[...], sin_ref[...]
    for h in range((q_cols + k_cols) // head_dim):
        col = h * head_dim
        part = lin[:, col:col + head_dim]
        part = part * cos_t + pltpu.roll(part, head_dim // 2, 1) * sin_t
        if col < q_cols:
            q_ref[:, col:col + head_dim] = (part * q_scale).astype(q_ref.dtype)
        else:
            k_ref[:, col - q_cols:col - q_cols + head_dim] = part.astype(k_ref.dtype)
    v_ref[...] = lin[:, q_cols + k_cols:].astype(v_ref.dtype)


def qkv_project(normed, w_all, cos_t, sin_t, q_cols, k_cols, head_dim):
    rows, depth = normed.shape
    cols = w_all.shape[1]
    v_cols = cols - q_cols - k_cols
    tile = 512
    return pl.pallas_call(
        functools.partial(qkv_kernel, q_cols, k_cols, head_dim, head_dim ** -0.5),
        grid=(rows // tile,),
        in_specs=[
            pl.BlockSpec((tile, depth), lambda i: (i, 0)),
            pl.BlockSpec((depth, cols), lambda i: (0, 0), pipeline_mode=pl.Buffered(1)),
            pl.BlockSpec((tile, head_dim), lambda i: (i, 0)),
            pl.BlockSpec((tile, head_dim), lambda i: (i, 0)),
        ],
        out_specs=[
            pl.BlockSpec((tile, q_cols), lambda i: (i, 0)),
            pl.BlockSpec((tile, k_cols), lambda i: (i, 0)),
            pl.BlockSpec((tile, v_cols), lambda i: (i, 0)),
        ],
        out_shape=[
            jax.ShapeDtypeStruct((rows, q_cols), jnp.bfloat16),
            jax.ShapeDtypeStruct((rows, k_cols), jnp.bfloat16),
            jax.ShapeDtypeStruct((rows, v_cols), jnp.bfloat16),
        ],
        compiler_params=pltpu.CompilerParams(vmem_limit_bytes=56 * 1024 * 1024),
        cost_estimate=pl.CostEstimate(flops=2 * rows * depth * cols, bytes_accessed=2 * (rows * depth + depth * cols + rows * cols), transcendentals=0),
        name="qkv_project",
    )(normed, w_all, cos_t, sin_t)


def stack_heads(block, groups, head_dim):
    return jnp.concatenate([block[:, g * head_dim:(g + 1) * head_dim] for g in range(groups)], axis=0)


def attn_fwd_kernel(groups, head_dim, first_ref, q_ref, k_ref, v_ref, pos_ref, key_pos_ref, o_ref, lse_ref, m_scr, l_scr, acc_scr):
    blk = pl.program_id(1)
    q_all = stack_heads(q_ref[...], groups, head_dim)
    floor_row = jnp.concatenate([pos_ref[...]] * groups, axis=1) - WINDOW
    wide = groups * BLK

    def visit(kb, diagonal):
        start = pl.multiple_of(kb * BLK, BLK)
        k_blk = k_ref[pl.ds(start, BLK), :]
        v_blk = v_ref[pl.ds(start, BLK), :]
        scores = dot_f32(k_blk, q_all, 1, 1)
        capped = jnp.tanh(scores * (1.0 / SOFT_CAP)) * (SOFT_CAP * LOG2E)
        keep = jnp.concatenate([key_pos_ref[pl.ds(start, BLK), :]] * (wide // LANES), axis=1) > floor_row
        if diagonal:
            key_idx = lax.broadcasted_iota(jnp.int32, (BLK, wide), 0)
            q_idx = lax.broadcasted_iota(jnp.int32, (BLK, wide), 1) % BLK
            keep = keep & (key_idx <= q_idx)
        capped = jnp.where(keep, capped, -1e30)
        top = jnp.max(capped, axis=0, keepdims=True)
        if diagonal:
            prob = jnp.exp2(capped - top)
            m_scr[...] = top
            l_scr[...] = jnp.sum(prob, axis=0, keepdims=True)
            acc_scr[...] = dot_f32(v_blk, prob.astype(jnp.bfloat16), 0, 0)
        else:
            m_old = m_scr[...]
            m_new = jnp.maximum(m_old, top)
            alpha = jnp.exp2(m_old - m_new)
            prob = jnp.exp2(capped - m_new)
            m_scr[...] = m_new
            l_scr[...] = l_scr[...] * alpha + jnp.sum(prob, axis=0, keepdims=True)
            acc_scr[...] = acc_scr[...] * alpha + dot_f32(v_blk, prob.astype(jnp.bfloat16), 0, 0)

    visit(blk, True)

    @pl.loop(first_ref[blk], blk)
    def _(kb):
        visit(kb, False)

    total = l_scr[...]
    out = (acc_scr[...] / total).T
    for g in range(groups):
        o_ref[:, g * head_dim:(g + 1) * head_dim] = out[g * BLK:(g + 1) * BLK, :].astype(o_ref.dtype)
    lse_ref[0, 0] = m_scr[...] + jnp.log2(total)


def attn_fwd(q_all, k_all, v_all, pos, key_pos, first_blk, groups, head_dim):
    seq_len, q_cols = q_all.shape
    kv_heads = k_all.shape[1] // head_dim
    n_blk = seq_len // BLK
    wide = groups * BLK
    pairs = seq_len * seq_len // 4 * groups * kv_heads
    return pl.pallas_call(
        functools.partial(attn_fwd_kernel, groups, head_dim),
        grid_spec=pltpu.PrefetchScalarGridSpec(
            num_scalar_prefetch=1,
            grid=(kv_heads, n_blk),
            in_specs=[
                pl.BlockSpec((BLK, groups * head_dim), lambda h, i, first: (i, h)),
                pl.BlockSpec((seq_len, head_dim), lambda h, i, first: (0, h)),
                pl.BlockSpec((seq_len, head_dim), lambda h, i, first: (0, h)),
                pl.BlockSpec((1, BLK), lambda h, i, first: (0, i)),
                pl.BlockSpec((seq_len, LANES), lambda h, i, first: (0, 0)),
            ],
            out_specs=[
                pl.BlockSpec((BLK, groups * head_dim), lambda h, i, first: (i, h)),
                pl.BlockSpec((1, 1, 1, wide), lambda h, i, first: (h, i, 0, 0)),
            ],
            scratch_shapes=[
                pltpu.VMEM((1, wide), jnp.float32),
                pltpu.VMEM((1, wide), jnp.float32),
                pltpu.VMEM((head_dim, wide), jnp.float32),
            ],
        ),
        out_shape=[
            jax.ShapeDtypeStruct((seq_len, q_cols), jnp.bfloat16),
            jax.ShapeDtypeStruct((kv_heads, n_blk, 1, wide), jnp.float32),
        ],
        compiler_params=pltpu.CompilerParams(vmem_limit_bytes=48 * 1024 * 1024),
        cost_estimate=pl.CostEstimate(flops=8 * pairs * head_dim, bytes_accessed=8 * seq_len * q_cols, transcendentals=2 * pairs),
        name="attn_fwd",
    )(first_blk, q_all, k_all, v_all, pos, key_pos)


def attn_bwd_kernel(groups, head_dim, q_scale, first_ref, q_ref, k_ref, v_ref, o_ref, do_ref, pos_ref, key_pos_ref, lse_ref, cos_ref, sin_ref,
                    out_ref, dq_scr, dk_scr, dv_scr, dq_out, dk_out, dv_out, dq_sem, kv_sem):
    head, blk = pl.program_id(0), pl.program_id(1)
    n_head, n_blk = pl.num_programs(0), pl.num_programs(1)
    half = head_dim // 2
    wide = groups * BLK
    q_width = groups * head_dim
    slot = blk % 2

    @pl.when(blk == 0)
    def _():
        dk_scr[...] = jnp.zeros_like(dk_scr)
        dv_scr[...] = jnp.zeros_like(dv_scr)

    q_all = stack_heads(q_ref[...], groups, head_dim)
    do_all = stack_heads(do_ref[...], groups, head_dim)
    o_all = stack_heads(o_ref[...], groups, head_dim)
    floor_row = jnp.concatenate([pos_ref[...]] * groups, axis=1) - WINDOW
    lse_row = lse_ref[0, 0]
    delta = jnp.sum((do_all.astype(jnp.float32) * o_all.astype(jnp.float32)).T, axis=0, keepdims=True)

    def visit(kb, diagonal):
        start = pl.multiple_of(kb * BLK, BLK)
        k_blk = k_ref[pl.ds(start, BLK), :]
        v_blk = v_ref[pl.ds(start, BLK), :]
        scores = dot_f32(k_blk, q_all, 1, 1)
        d_prob = dot_f32(v_blk, do_all, 1, 1)
        tanh_s = jnp.tanh(scores * (1.0 / SOFT_CAP))
        keep = jnp.concatenate([key_pos_ref[pl.ds(start, BLK), :]] * (wide // LANES), axis=1) > floor_row
        if diagonal:
            key_idx = lax.broadcasted_iota(jnp.int32, (BLK, wide), 0)
            q_idx = lax.broadcasted_iota(jnp.int32, (BLK, wide), 1) % BLK
            keep = keep & (key_idx <= q_idx)
        prob = jnp.exp2(jnp.where(keep, tanh_s * (SOFT_CAP * LOG2E) - lse_row, -1e30))
        d_score = (prob * (d_prob - delta) * (1.0 - tanh_s * tanh_s)).astype(jnp.bfloat16)
        dv_scr[pl.ds(start, BLK), :] += jnp.dot(prob.astype(jnp.bfloat16), do_all, preferred_element_type=jnp.float32)
        dk_scr[pl.ds(start, BLK), :] += jnp.dot(d_score, q_all, preferred_element_type=jnp.float32)
        dq_new = dot_f32(k_blk, d_score, 0, 0)
        if diagonal:
            dq_scr[...] = dq_new
        else:
            dq_scr[...] += dq_new

    visit(blk, True)

    @pl.loop(first_ref[blk], blk)
    def _(kb):
        visit(kb, False)

    def dq_copy(h, i):
        dst = out_ref.at[pl.ds(pl.multiple_of(i * BLK, BLK), BLK), pl.ds(pl.multiple_of(h * q_width, q_width), q_width)]
        return pltpu.make_async_copy(dq_out.at[slot], dst, dq_sem.at[slot])

    def kv_copy(which, src, h):
        col = n_head * q_width + which * n_head * head_dim + h * head_dim
        dst = out_ref.at[:, pl.ds(pl.multiple_of(col, head_dim), head_dim)]
        return pltpu.make_async_copy(src, dst, kv_sem.at[which])

    @pl.when(head * n_blk + blk >= 2)
    def _():
        dq_copy(head, blk).wait()

    d_q = dq_scr[...].T
    rows = pl.ds(pl.multiple_of(blk * BLK, BLK), BLK)
    cos_t, sin_t = cos_ref[rows, :], sin_ref[rows, :]
    for g in range(groups):
        part = d_q[g * BLK:(g + 1) * BLK, :]
        part = (part * cos_t - pltpu.roll(part, half, 1) * sin_t) * q_scale
        dq_out[slot, :, g * head_dim:(g + 1) * head_dim] = part.astype(dq_out.dtype)
    dq_copy(head, blk).start()

    @pl.when(blk == n_blk - 1)
    def _():
        @pl.loop(0, n_blk)
        def _(i):
            rows = pl.ds(pl.multiple_of(i * BLK, BLK), BLK)
            part = dk_scr[rows, :]
            part = part * cos_ref[rows, :] - pltpu.roll(part, half, 1) * sin_ref[rows, :]
            dk_out[rows, :] = part.astype(dk_out.dtype)
            dv_out[rows, :] = dv_scr[rows, :].astype(dv_out.dtype)

        kv_copy(0, dk_out, head).start()
        kv_copy(1, dv_out, head).start()
        kv_copy(0, dk_out, head).wait()
        kv_copy(1, dv_out, head).wait()

    @pl.when((blk == n_blk - 1) & (head == n_head - 1))
    def _():
        for s in range(2):
            pltpu.make_async_copy(dq_out.at[s], out_ref.at[pl.ds(0, BLK), pl.ds(0, q_width)], dq_sem.at[s]).wait()


def attn_bwd(q_all, k_all, v_all, o_all, d_o, pos, key_pos, lse, first_blk, cos_t, sin_t, groups, head_dim):
    seq_len, q_cols = q_all.shape
    k_cols = k_all.shape[1]
    kv_heads = k_cols // head_dim
    n_blk = seq_len // BLK
    wide = groups * BLK
    pairs = seq_len * seq_len // 4 * groups * kv_heads
    by_q = pl.BlockSpec((BLK, groups * head_dim), lambda h, i, first: (i, h))
    by_h = pl.BlockSpec((seq_len, head_dim), lambda h, i, first: (0, h))
    table = pl.BlockSpec((seq_len, LANES), lambda h, i, first: (0, 0))
    return pl.pallas_call(
        functools.partial(attn_bwd_kernel, groups, head_dim, head_dim ** -0.5),
        grid_spec=pltpu.PrefetchScalarGridSpec(
            num_scalar_prefetch=1,
            grid=(kv_heads, n_blk),
            in_specs=[
                by_q, by_h, by_h, by_q, by_q,
                pl.BlockSpec((1, BLK), lambda h, i, first: (0, i)),
                table,
                pl.BlockSpec((1, 1, 1, wide), lambda h, i, first: (h, i, 0, 0)),
                table, table,
            ],
            out_specs=pl.BlockSpec(memory_space=pl.ANY),
            scratch_shapes=[
                pltpu.VMEM((head_dim, wide), jnp.float32),
                pltpu.VMEM((seq_len, head_dim), jnp.float32),
                pltpu.VMEM((seq_len, head_dim), jnp.float32),
                pltpu.VMEM((2, BLK, groups * head_dim), jnp.bfloat16),
                pltpu.VMEM((seq_len, head_dim), jnp.bfloat16),
                pltpu.VMEM((seq_len, head_dim), jnp.bfloat16),
                pltpu.SemaphoreType.DMA((2,)),
                pltpu.SemaphoreType.DMA((2,)),
            ],
        ),
        out_shape=jax.ShapeDtypeStruct((seq_len, q_cols + 2 * k_cols), jnp.bfloat16),
        compiler_params=pltpu.CompilerParams(vmem_limit_bytes=48 * 1024 * 1024),
        cost_estimate=pl.CostEstimate(flops=20 * pairs * head_dim, bytes_accessed=16 * seq_len * q_cols, transcendentals=2 * pairs),
        name="attn_bwd",
    )(first_blk, q_all, k_all, v_all, o_all, d_o, pos, key_pos, lse, cos_t, sin_t)


def solution(mesh):
    act_spec = P('dp', 'tp', None)
    head_spec = P(None, 'tp', None)
    grad_spec = P('dp', 'tp', None)
    in_specs = (act_spec, P('dp', 'tp'), act_spec, head_spec, head_spec, head_spec, P('tp', None, None), P(None), P(None))
    out_specs = (act_spec, act_spec, grad_spec, grad_spec, grad_spec, P(('dp', 'tp'), None, None), P('dp'), P('dp'))

    def local_body(x_in, positions, grad_out, w_query, w_key, w_value, w_out, gain_pre, gain_post):
        n_rows, _, depth = x_in.shape
        n_dev = mesh.shape['tp']
        heads_loc, head_dim = w_query.shape[1], w_query.shape[2]
        kv_loc = w_key.shape[1]
        groups = heads_loc // kv_loc
        q_cols, k_cols = heads_loc * head_dim, kv_loc * head_dim

        gain_pre_row, gain_post_row = gain_pre[None, :], gain_post[None, :]
        normed_all = []
        for b in range(n_rows):
            normed = pre_norm(x_in, gain_pre_row, b)
            normed_all.append(lax.all_gather(normed, 'tp', axis=0, tiled=True))
        w_out_loc = w_out.reshape(q_cols, depth)
        w_out_all = lax.all_gather(w_out_loc, 'tp', axis=0, tiled=True)

        pos_all = lax.all_gather(positions, 'tp', axis=1, tiled=True)
        seq_len = pos_all.shape[1]
        half = head_dim // 2
        inv_freq = ROPE_THETA ** (-2.0 * jnp.arange(half, dtype=jnp.float32) / head_dim)
        before = pos_all[:, None, :] <= pos_all[:, ::BLK, None] - WINDOW
        first_blk = jnp.sum(before.astype(jnp.int32), axis=-1) // BLK
        w_all = jnp.concatenate([w_query.reshape(depth, q_cols), w_key.reshape(depth, k_cols), w_value.reshape(depth, k_cols)], axis=1)

        saved, d_proj_all = [], []
        y_out, d_post = None, jnp.zeros((1, depth), jnp.float32)
        for b in range(n_rows):
            angles = pos_all[b].astype(jnp.float32)[:, None] * inv_freq
            cos_h, sin_h = jnp.cos(angles), jnp.sin(angles)
            cos_t = jnp.concatenate([cos_h, cos_h], axis=-1)
            sin_t = jnp.concatenate([-sin_h, sin_h], axis=-1)
            pos_b = pos_all[b][None, :]
            key_pos = jnp.broadcast_to(pos_all[b][:, None], (seq_len, LANES))
            q_b, k_b, v_b = qkv_project(normed_all[b], w_all, cos_t, sin_t, q_cols, k_cols, head_dim)
            o_b, lse_b = attn_fwd(q_b, k_b, v_b, pos_b, key_pos, first_blk[b], groups, head_dim)
            o_mine = lax.all_to_all(o_b.reshape(-1, seq_len // n_dev, q_cols), 'tp', split_axis=0, concat_axis=0, tiled=True)
            proj = out_proj(o_mine, w_out_all)
            y_out, d_proj, d_post = post_norm(proj, x_in, grad_out, gain_post_row, d_post, y_out, b)
            d_proj_all.append(lax.all_gather(d_proj, 'tp', axis=0, tiled=True))
            saved.append((q_b, k_b, v_b, o_b, pos_b, key_pos, lse_b, cos_t, sin_t))

        me = lax.axis_index('tp')
        own_dst, pair_dst = me[None], me[None] ^ 1
        w_t = w_all.T

        def swap(value, bit):
            return lax.ppermute(value, 'tp', [(d, d ^ bit) for d in range(n_dev)])

        grad_x, d_pre = None, jnp.zeros((1, depth), jnp.float32)
        grad_wo = jnp.zeros((), jnp.float32)
        d_lin = []
        for b in range(n_rows):
            q_b, k_b, v_b, o_b, pos_b, key_pos, lse_b, cos_t, sin_t = saved[b]
            d_o = dot_f32(d_proj_all[b], w_out_loc, 1, 1).astype(jnp.bfloat16)
            d_lin.append(attn_bwd(q_b, k_b, v_b, o_b, d_o, pos_b, key_pos, lse_b, first_blk[b], cos_t, sin_t, groups, head_dim))
            pair = grad_normed_pair(pair_dst, d_lin[b], w_t, seq_len // n_dev)
            from_pair = swap(pair, 1)
            send_x, keep_x, send_y, keep_y = grad_normed_own(own_dst, d_lin[b], w_t, from_pair)
            near_x = swap(send_x, 2)
            near_y = swap(send_y, 4)
            fold_x = (keep_x[1].astype(jnp.float32) + near_x[1].astype(jnp.float32)).astype(jnp.bfloat16)
            fold_y = (keep_y[1].astype(jnp.float32) + near_y[1].astype(jnp.float32)).astype(jnp.bfloat16)
            far_x = swap(fold_x, 4)
            far_y = swap(fold_y, 2)
            grad_x, d_pre = pre_grad((keep_x, near_x, far_x, keep_y, near_y, far_y), x_in, grad_out, gain_pre_row, d_pre, grad_x, b)
            grad_wo = grad_wo + dot_f32(o_b, d_proj_all[b], 0, 0)

        grad_wq, = grad_w(normed_all, d_lin, (heads_loc,), head_dim, 0)
        grad_wk, grad_wv = grad_w(normed_all, d_lin, (kv_loc, kv_loc), head_dim, 1)
        grad_pre, grad_post = gain_sum(d_pre, d_post, n_dev)
        grad_pre, grad_post = grad_pre[0], grad_post[0]
        return y_out, grad_x, grad_wq, grad_wk, grad_wv, grad_wo.reshape(w_out.shape), grad_pre, grad_post

    return jax.shard_map(local_body, mesh=mesh, in_specs=in_specs, out_specs=out_specs, check_vma=False)
```

```python
import functools

import jax
import jax.numpy as jnp
from jax import lax
from jax.experimental import pallas as pl
from jax.experimental.pallas import tpu as pltpu
from jax.sharding import PartitionSpec as P


WINDOW = 4096
SOFT_CAP = 50.0
NORM_EPS = 1e-6
ROPE_THETA = 10000.0
LOG2E = 1.4426950408889634
BLK = 256
LANES = 128


def dot_f32(lhs, rhs, lhs_dim, rhs_dim):
    return lax.dot_general(lhs, rhs, (((lhs_dim,), (rhs_dim,)), ((), ())), preferred_element_type=jnp.float32)


ROWS = 64
CHUNK = 16


def row_specs(seq, depth):
    whole = pl.BlockSpec((1, ROWS, depth), lambda i: (seq, i, 0))
    one = pl.BlockSpec((ROWS, depth), lambda i: (i, 0))
    vec = pl.BlockSpec((1, depth), lambda i: (0, 0))
    return whole, one, vec


def inverse_rms(values):
    return lax.rsqrt(jnp.mean(values * values, axis=-1, keepdims=True) + NORM_EPS)


def norm_grad(values, inv, d_out, gain):
    scaled = d_out * gain
    dot = jnp.mean(scaled * values, axis=-1, keepdims=True)
    return scaled * inv - values * (inv * inv * inv * dot)


def fold_rows(block):
    return sum(block[r:r + 8] for r in range(0, CHUNK, 8))


def pre_norm_kernel(x_ref, gain_ref, n_ref):
    gain = 1.0 + gain_ref[...]

    @pl.loop(0, ROWS // CHUNK)
    def _(c):
        rows = pl.ds(pl.multiple_of(c * CHUNK, CHUNK), CHUNK)
        values = x_ref[0, rows, :].astype(jnp.float32)
        n_ref[rows, :] = (values * inverse_rms(values) * gain).astype(n_ref.dtype)


def pre_norm(x_in, gain, first_seq, count):
    _, rows, depth = x_in.shape
    steps = rows // ROWS
    return pl.pallas_call(
        pre_norm_kernel,
        grid=(count, steps),
        in_specs=[pl.BlockSpec((1, ROWS, depth), lambda s, i: (first_seq + s, i, 0)), pl.BlockSpec((1, depth), lambda s, i: (0, 0))],
        out_specs=pl.BlockSpec((ROWS, depth), lambda s, i: (s * steps + i, 0)),
        out_shape=jax.ShapeDtypeStruct((count * rows, depth), jnp.bfloat16),
        compiler_params=pltpu.CompilerParams(vmem_limit_bytes=54 * 1024 * 1024),
        cost_estimate=pl.CostEstimate(flops=count * rows * depth * 400, bytes_accessed=4 * count * rows * depth, transcendentals=count * rows),
        name="pre_norm",
    )(x_in, gain)


def post_norm_kernel(first, proj_ref, x_ref, go_ref, gain_ref, dg_in_ref, *refs):
    y_ref, d_proj_ref, dg_ref, dg_scr = refs[0 if first else 1:]
    step = pl.program_id(0)
    gain = 1.0 + gain_ref[...]

    @pl.when(step == 0)
    def _():
        dg_scr[...] = jnp.zeros_like(dg_scr)

    @pl.loop(0, ROWS // CHUNK)
    def _(c):
        rows = pl.ds(pl.multiple_of(c * CHUNK, CHUNK), CHUNK)
        values = proj_ref[rows, :].astype(jnp.float32)
        inv = inverse_rms(values)
        unit = values * inv
        post = (unit * gain).astype(jnp.bfloat16).astype(jnp.float32)
        y_ref[0, rows, :] = (x_ref[0, rows, :].astype(jnp.float32) + post).astype(y_ref.dtype)
        d_out = go_ref[0, rows, :].astype(jnp.float32)
        dg_scr[...] += fold_rows(d_out * unit)
        d_proj_ref[rows, :] = norm_grad(values, inv, d_out, gain).astype(d_proj_ref.dtype)

    @pl.when(step == pl.num_programs(0) - 1)
    def _():
        dg_ref[...] = dg_in_ref[...] + jnp.sum(dg_scr[...], axis=0, keepdims=True)


def post_norm(proj, x_in, grad_out, gain, dg_in, y_prev, seq):
    _, rows, depth = x_in.shape
    whole, one, vec = row_specs(seq, depth)
    first = y_prev is None
    return pl.pallas_call(
        functools.partial(post_norm_kernel, first),
        grid=(rows // ROWS,),
        in_specs=[one, whole, whole, vec, vec] + ([] if first else [pl.BlockSpec(memory_space=pl.ANY)]),
        out_specs=[whole, one, vec],
        out_shape=[
            jax.ShapeDtypeStruct(x_in.shape, jnp.bfloat16),
            jax.ShapeDtypeStruct((rows, depth), jnp.bfloat16),
            jax.ShapeDtypeStruct((1, depth), jnp.float32),
        ],
        scratch_shapes=[pltpu.VMEM((8, depth), jnp.float32)],
        input_output_aliases={} if first else {5: 0},
        compiler_params=pltpu.CompilerParams(vmem_limit_bytes=54 * 1024 * 1024),
        cost_estimate=pl.CostEstimate(flops=rows * depth * 800, bytes_accessed=10 * rows * depth, transcendentals=rows),
        name="post_norm",
    )(proj, x_in, grad_out, gain, dg_in, *([] if first else [y_prev]))


def pre_grad_kernel(first, *refs):
    pieces, (x_ref, go_ref, gain_ref, dg_in_ref), refs = refs[:6], refs[6:10], refs[10:]
    gx_ref, dg_ref, dg_scr = refs[0 if first else 1:]
    step = pl.program_id(0)
    gain = 1.0 + gain_ref[...]

    @pl.when(step == 0)
    def _():
        dg_scr[...] = jnp.zeros_like(dg_scr)

    @pl.loop(0, ROWS // CHUNK)
    def _(c):
        rows = pl.ds(pl.multiple_of(c * CHUNK, CHUNK), CHUNK)
        values = x_ref[0, rows, :].astype(jnp.float32)
        inv = inverse_rms(values)
        halves = []
        for kept, near, far in (pieces[:3], pieces[3:]):
            halves.append(kept[0, rows, :].astype(jnp.float32) + near[0, rows, :].astype(jnp.float32) + far[rows, :].astype(jnp.float32))
        d_out = jnp.concatenate(halves, axis=1)
        dg_scr[...] += fold_rows(d_out * (values * inv))
        d_x = norm_grad(values, inv, d_out, gain).astype(jnp.bfloat16).astype(jnp.float32)
        gx_ref[0, rows, :] = (go_ref[0, rows, :].astype(jnp.float32) + d_x).astype(gx_ref.dtype)

    @pl.when(step == pl.num_programs(0) - 1)
    def _():
        dg_ref[...] = dg_in_ref[...] + jnp.sum(dg_scr[...], axis=0, keepdims=True)


def pre_grad(pieces, x_in, grad_out, gain, dg_in, gx_prev, seq):
    _, rows, depth = x_in.shape
    whole, _, vec = row_specs(seq, depth)
    pair = pl.BlockSpec((1, ROWS, depth // 2), lambda i: (0, i, 0))
    one = pl.BlockSpec((ROWS, depth // 2), lambda i: (i, 0))
    first = gx_prev is None
    return pl.pallas_call(
        functools.partial(pre_grad_kernel, first),
        grid=(rows // ROWS,),
        in_specs=[pair, pair, one, pair, pair, one, whole, whole, vec, vec] + ([] if first else [pl.BlockSpec(memory_space=pl.ANY)]),
        out_specs=[whole, vec],
        out_shape=[jax.ShapeDtypeStruct(x_in.shape, jnp.bfloat16), jax.ShapeDtypeStruct((1, depth), jnp.float32)],
        scratch_shapes=[pltpu.VMEM((8, depth), jnp.float32)],
        input_output_aliases={} if first else {10: 0},
        compiler_params=pltpu.CompilerParams(vmem_limit_bytes=54 * 1024 * 1024),
        cost_estimate=pl.CostEstimate(flops=rows * depth * 700, bytes_accessed=12 * rows * depth, transcendentals=rows),
        name="pre_grad",
    )(*pieces, x_in, grad_out, gain, dg_in, *([] if first else [gx_prev]))


def out_proj_kernel(o_ref, w_ref, r_ref):
    o_all = jnp.concatenate([o_ref[d] for d in range(o_ref.shape[0])], axis=1)
    r_ref[...] = jnp.dot(o_all, w_ref[...], preferred_element_type=jnp.float32).astype(r_ref.dtype)


def out_proj(o_mine, w_all):
    n_dev, rows, cols = o_mine.shape
    depth = w_all.shape[1]
    tile = 768
    return pl.pallas_call(
        out_proj_kernel,
        grid=(depth // tile,),
        in_specs=[
            pl.BlockSpec((n_dev, rows, cols), lambda i: (0, 0, 0), pipeline_mode=pl.Buffered(1)),
            pl.BlockSpec((n_dev * cols, tile), lambda i: (0, i)),
        ],
        out_specs=pl.BlockSpec((rows, tile), lambda i: (0, i)),
        out_shape=jax.ShapeDtypeStruct((rows, depth), jnp.bfloat16),
        compiler_params=pltpu.CompilerParams(vmem_limit_bytes=54 * 1024 * 1024),
        cost_estimate=pl.CostEstimate(flops=2 * n_dev * rows * cols * depth, bytes_accessed=2 * n_dev * cols * depth, transcendentals=0),
        name="out_proj",
    )(o_mine, w_all)


def pair_core_kernel(dst_ref, d_ref, w_ref, out_ref):
    out_ref[0] = jnp.dot(d_ref[...], w_ref[...], preferred_element_type=jnp.float32).astype(out_ref.dtype)


def grad_normed_pair(dst, d_lin, w_t, rows):
    cols, depth = w_t.shape
    half = depth // 2
    return pl.pallas_call(
        pair_core_kernel,
        grid_spec=pltpu.PrefetchScalarGridSpec(
            num_scalar_prefetch=1,
            grid=(2, 4),
            in_specs=[
                pl.BlockSpec((rows, cols), lambda h, r, dst: (dst[0] ^ (2 * r), 0)),
                pl.BlockSpec((cols, half), lambda h, r, dst: (0, h)),
            ],
            out_specs=pl.BlockSpec((1, rows, half), lambda h, r, dst: (r, 0, h)),
        ),
        out_shape=jax.ShapeDtypeStruct((4, rows, depth), jnp.bfloat16),
        compiler_params=pltpu.CompilerParams(vmem_limit_bytes=48 * 1024 * 1024),
        cost_estimate=pl.CostEstimate(flops=8 * rows * cols * depth, bytes_accessed=2 * (4 * rows * depth + cols * depth), transcendentals=0),
        name="grad_normed_pair",
    )(dst, d_lin, w_t)


def route(h, j):
    return jnp.where(h == 0, (2 * j + 1) % 5, (j + 2) % 4)


def own_core_kernel(dst_ref, d_ref, w_ref, add_ref, *outs):
    step = 4 * pl.program_id(0) + pl.program_id(1)
    value = jnp.dot(d_ref[...], w_ref[...], preferred_element_type=jnp.float32) + add_ref[0].astype(jnp.float32)
    value = value.astype(jnp.bfloat16)
    for i, out in enumerate(outs):
        @pl.when((step >= 2 * i) & (step < 2 * i + 2))
        def _(out=out):
            out[0] = value


def grad_normed_own(dst, d_lin, w_t, from_pair):
    _, rows, depth = from_pair.shape
    cols = w_t.shape[0]
    half = depth // 2
    outs = [pl.BlockSpec((1, rows, half), lambda h, j, dst, i=i: (jnp.clip(4 * h + j - 2 * i, 0, 1), 0, 0)) for i in range(4)]
    return pl.pallas_call(
        own_core_kernel,
        grid_spec=pltpu.PrefetchScalarGridSpec(
            num_scalar_prefetch=1,
            grid=(2, 4),
            in_specs=[
                pl.BlockSpec((rows, cols), lambda h, j, dst: (dst[0] ^ (2 * route(h, j)), 0)),
                pl.BlockSpec((cols, half), lambda h, j, dst: (0, h)),
                pl.BlockSpec((1, rows, half), lambda h, j, dst: (route(h, j), 0, h)),
            ],
            out_specs=outs,
        ),
        out_shape=[jax.ShapeDtypeStruct((2, rows, half), jnp.bfloat16)] * 4,
        compiler_params=pltpu.CompilerParams(vmem_limit_bytes=56 * 1024 * 1024),
        cost_estimate=pl.CostEstimate(flops=8 * rows * cols * depth, bytes_accessed=2 * (8 * rows * depth + cols * depth), transcendentals=0),
        name="grad_normed_own",
    )(dst, d_lin, w_t, from_pair)


def fold_kernel(keep_x_ref, near_x_ref, keep_y_ref, near_y_ref, x_ref, y_ref):
    for out, kept, near in ((x_ref, keep_x_ref, near_x_ref), (y_ref, keep_y_ref, near_y_ref)):
        out[...] = (kept[0].astype(jnp.float32) + near[0].astype(jnp.float32)).astype(out.dtype)


def fold(keep_x, near_x, keep_y, near_y):
    _, rows, half = keep_x.shape
    tile = 96
    second = pl.BlockSpec((1, tile, half), lambda i: (1, i, 0))
    out = pl.BlockSpec((tile, half), lambda i: (i, 0))
    return pl.pallas_call(
        fold_kernel,
        grid=(rows // tile,),
        in_specs=[second] * 4,
        out_specs=[out, out],
        out_shape=[jax.ShapeDtypeStruct((rows, half), jnp.bfloat16)] * 2,
        compiler_params=pltpu.CompilerParams(vmem_limit_bytes=54 * 1024 * 1024),
        cost_estimate=pl.CostEstimate(flops=rows * half * 800, bytes_accessed=12 * rows * half, transcendentals=0),
        name="fold",
    )(keep_x, near_x, keep_y, near_y)


def gain_sum_kernel(n_dev, pre_ref, post_ref, pre_out, post_out, slots, local_sem, send_sem, recv_sem):
    me = lax.axis_index('tp')
    sources = (pre_ref, post_ref)
    sends, locals_ = [], []
    for off in range(1, n_dev):
        for which, src in enumerate(sources):
            copy = pltpu.make_async_remote_copy(
                src_ref=src, dst_ref=slots.at[which, me], send_sem=send_sem.at[which, off], recv_sem=recv_sem.at[which, me],
                device_id={'tp': lax.rem(me + off, n_dev)}, device_id_type=pl.DeviceIdType.MESH)
            copy.start()
            sends.append(copy)
    for which, src in enumerate(sources):
        copy = pltpu.make_async_copy(src, slots.at[which, me], local_sem.at[which])
        copy.start()
        locals_.append(copy)
    for copy in locals_:
        copy.wait()
    for off in range(1, n_dev):
        other = lax.rem(me + off, n_dev)
        for which, src in enumerate(sources):
            pltpu.make_async_remote_copy(
                src_ref=src, dst_ref=slots.at[which, other], send_sem=send_sem.at[which, off], recv_sem=recv_sem.at[which, other],
                device_id={'tp': other}, device_id_type=pl.DeviceIdType.MESH).wait_recv()
    for copy in sends:
        copy.wait_send()
    for which, out in enumerate((pre_out, post_out)):
        total = slots[which, 0]
        for d in range(1, n_dev):
            total = total + slots[which, d]
        out[...] = total


def gain_sum(d_pre, d_post, n_dev):
    depth = d_pre.shape[1]
    vmem = pl.BlockSpec(memory_space=pltpu.VMEM)
    return pl.pallas_call(
        functools.partial(gain_sum_kernel, n_dev),
        in_specs=[vmem, vmem],
        out_specs=[vmem, vmem],
        out_shape=[jax.ShapeDtypeStruct((1, depth), jnp.float32)] * 2,
        scratch_shapes=[
            pltpu.VMEM((2, n_dev, 1, depth), jnp.float32),
            pltpu.SemaphoreType.DMA((2,)),
            pltpu.SemaphoreType.DMA((2, n_dev)),
            pltpu.SemaphoreType.DMA((2, n_dev)),
        ],
        compiler_params=pltpu.CompilerParams(has_side_effects=True),
        name="gain_sum",
    )(d_pre, d_post)


def grad_w_kernel(n_out, head_dim, a_ref, d_ref, *refs):
    prev, outs = refs[:-n_out], refs[-n_out:]
    n_dev, rows, tile = a_ref.shape
    total = dot_f32(a_ref[...].reshape(n_dev * rows, tile), d_ref[...], 0, 0)
    col = 0
    for i, out in enumerate(outs):
        for h in range(out.shape[1]):
            part = total[:, col:col + head_dim]
            out[:, h, :] = part + prev[i][:, h, :] if prev else part
            col += head_dim


def grad_w(gathered, slot, rows, d_lin, heads, head_dim, prev):
    n_dev, _, depth = gathered.shape
    seq_len, cols = d_lin.shape
    tile = 384
    outs = [pl.BlockSpec((tile, h, head_dim), lambda i: (i, 0, 0)) for h in heads]
    return pl.pallas_call(
        functools.partial(grad_w_kernel, len(heads), head_dim),
        grid=(depth // tile,),
        in_specs=[
            pl.BlockSpec((n_dev, rows, tile), lambda i: (0, slot, i)),
            pl.BlockSpec((seq_len, cols), lambda i: (0, 0), pipeline_mode=pl.Buffered(1)),
        ] + (outs if prev else []),
        out_specs=outs,
        out_shape=[jax.ShapeDtypeStruct((depth, h, head_dim), jnp.float32) for h in heads],
        input_output_aliases={2 + i: i for i in range(len(prev))},
        compiler_params=pltpu.CompilerParams(vmem_limit_bytes=56 * 1024 * 1024),
        cost_estimate=pl.CostEstimate(flops=2 * seq_len * depth * cols, bytes_accessed=2 * seq_len * (depth + cols) + 8 * depth * cols, transcendentals=0),
        name="grad_w",
    )(gathered, d_lin, *prev)


def qkv_kernel(q_cols, k_cols, head_dim, q_scale, a_ref, w_ref, cos_ref, sin_ref, q_ref, k_ref, v_ref):
    n_dev, rows, depth = a_ref.shape
    lin = jnp.dot(a_ref[...].reshape(n_dev * rows, depth), w_ref[...], preferred_element_type=jnp.float32)
    cos_t, sin_t = cos_ref[...], sin_ref[...]
    for h in range((q_cols + k_cols) // head_dim):
        col = h * head_dim
        part = lin[:, col:col + head_dim]
        part = part * cos_t + pltpu.roll(part, head_dim // 2, 1) * sin_t
        if col < q_cols:
            q_ref[:, col:col + head_dim] = (part * q_scale).astype(q_ref.dtype)
        else:
            k_ref[:, col - q_cols:col - q_cols + head_dim] = part.astype(k_ref.dtype)
    v_ref[...] = lin[:, q_cols + k_cols:].astype(v_ref.dtype)


def qkv_project(gathered, slot, rows, w_all, cos_t, sin_t, q_cols, k_cols, head_dim):
    n_dev, _, depth = gathered.shape
    cols = w_all.shape[1]
    v_cols = cols - q_cols - k_cols
    seq_len, tile = n_dev * rows, 2 * rows
    by_row = [pl.BlockSpec((tile, width), lambda i: (i, 0)) for width in (head_dim, head_dim, q_cols, k_cols, v_cols)]
    return pl.pallas_call(
        functools.partial(qkv_kernel, q_cols, k_cols, head_dim, head_dim ** -0.5),
        grid=(n_dev // 2,),
        in_specs=[
            pl.BlockSpec((2, rows, depth), lambda i: (i, slot, 0)),
            pl.BlockSpec((depth, cols), lambda i: (0, 0), pipeline_mode=pl.Buffered(1)),
        ] + by_row[:2],
        out_specs=by_row[2:],
        out_shape=[jax.ShapeDtypeStruct((seq_len, width), jnp.bfloat16) for width in (q_cols, k_cols, v_cols)],
        compiler_params=pltpu.CompilerParams(vmem_limit_bytes=58 * 1024 * 1024),
        cost_estimate=pl.CostEstimate(flops=2 * seq_len * depth * cols, bytes_accessed=2 * (seq_len * depth + depth * cols + seq_len * cols), transcendentals=0),
        name="qkv_project",
    )(gathered, w_all, cos_t, sin_t)


def stack_heads(block, groups, head_dim):
    return jnp.concatenate([block[:, g * head_dim:(g + 1) * head_dim] for g in range(groups)], axis=0)


def keep_mask(key_pos, floor_row, wide, diagonal):
    keep = jnp.concatenate([key_pos] * (wide // LANES), axis=1) > floor_row
    if diagonal:
        key_idx = lax.broadcasted_iota(jnp.int32, (BLK, wide), 0)
        q_idx = lax.broadcasted_iota(jnp.int32, (BLK, wide), 1) % BLK
        keep = keep & (key_idx <= q_idx)
    return keep


def visit_pairs(visit, first, blk):
    odd = (blk - first) % 2

    @pl.when(odd == 0)
    def _():
        visit([blk], True)

    @pl.when(odd == 1)
    def _():
        visit([blk, blk - 1], True)

    @pl.loop(0, (blk - first) // 2)
    def _(i):
        visit([first + 2 * i, first + 2 * i + 1], False)


def attn_fwd_kernel(groups, head_dim, first_ref, q_ref, k_ref, v_ref, pos_ref, key_pos_ref, o_ref, lse_ref, m_scr, l_scr, acc_scr):
    blk = pl.program_id(1)
    q_all = stack_heads(q_ref[...], groups, head_dim)
    floor_row = jnp.concatenate([pos_ref[...]] * groups, axis=1) - WINDOW
    wide = groups * BLK

    def visit(blocks, with_diagonal):
        rows = [pl.ds(pl.multiple_of(kb * BLK, BLK), BLK) for kb in blocks]
        scores = [dot_f32(k_ref[r, :], q_all, 1, 1) for r in rows]
        capped = []
        for i, r in enumerate(rows):
            keep = keep_mask(key_pos_ref[r, :], floor_row, wide, with_diagonal and i == 0)
            capped.append(jnp.where(keep, jnp.tanh(scores[i] * (1.0 / SOFT_CAP)) * (SOFT_CAP * LOG2E), -1e30))
        top = functools.reduce(jnp.maximum, [jnp.max(c, axis=0, keepdims=True) for c in capped])
        if not with_diagonal:
            m_old = m_scr[...]
            top = jnp.maximum(m_old, top)
            alpha = jnp.exp2(m_old - top)
        m_scr[...] = top
        probs = [jnp.exp2(c - top) for c in capped]
        total = sum(jnp.sum(p, axis=0, keepdims=True) for p in probs)
        acc = sum(dot_f32(v_ref[r, :], p.astype(jnp.bfloat16), 0, 0) for r, p in zip(rows, probs))
        if with_diagonal:
            l_scr[...] = total
            acc_scr[...] = acc
        else:
            l_scr[...] = l_scr[...] * alpha + total
            acc_scr[...] = acc_scr[...] * alpha + acc

    visit_pairs(visit, first_ref[blk], blk)

    total = l_scr[...]
    out = (acc_scr[...] / total).T
    for g in range(groups):
        o_ref[:, g * head_dim:(g + 1) * head_dim] = out[g * BLK:(g + 1) * BLK, :].astype(o_ref.dtype)
    lse_ref[0, 0] = m_scr[...] + jnp.log2(total)


def attn_fwd(q_all, k_all, v_all, pos, key_pos, first_blk, groups, head_dim):
    seq_len, q_cols = q_all.shape
    kv_heads = k_all.shape[1] // head_dim
    n_blk = seq_len // BLK
    wide = groups * BLK
    pairs = seq_len * seq_len // 4 * groups * kv_heads
    return pl.pallas_call(
        functools.partial(attn_fwd_kernel, groups, head_dim),
        grid_spec=pltpu.PrefetchScalarGridSpec(
            num_scalar_prefetch=1,
            grid=(kv_heads, n_blk),
            in_specs=[
                pl.BlockSpec((BLK, groups * head_dim), lambda h, i, first: (i, h)),
                pl.BlockSpec((seq_len, head_dim), lambda h, i, first: (0, h)),
                pl.BlockSpec((seq_len, head_dim), lambda h, i, first: (0, h)),
                pl.BlockSpec((1, BLK), lambda h, i, first: (0, i)),
                pl.BlockSpec((seq_len, LANES), lambda h, i, first: (0, 0)),
            ],
            out_specs=[
                pl.BlockSpec((BLK, groups * head_dim), lambda h, i, first: (i, h)),
                pl.BlockSpec((1, 1, 1, wide), lambda h, i, first: (h, i, 0, 0)),
            ],
            scratch_shapes=[
                pltpu.VMEM((1, wide), jnp.float32),
                pltpu.VMEM((1, wide), jnp.float32),
                pltpu.VMEM((head_dim, wide), jnp.float32),
            ],
        ),
        out_shape=[
            jax.ShapeDtypeStruct((seq_len, q_cols), jnp.bfloat16),
            jax.ShapeDtypeStruct((kv_heads, n_blk, 1, wide), jnp.float32),
        ],
        compiler_params=pltpu.CompilerParams(vmem_limit_bytes=48 * 1024 * 1024),
        cost_estimate=pl.CostEstimate(flops=8 * pairs * head_dim, bytes_accessed=8 * seq_len * q_cols, transcendentals=2 * pairs),
        name="attn_fwd",
    )(first_blk, q_all, k_all, v_all, pos, key_pos)


def attn_bwd_kernel(groups, head_dim, q_scale, first_ref, q_ref, k_ref, v_ref, o_ref, do_ref, pos_ref, key_pos_ref, lse_ref, cos_ref, sin_ref,
                    out_ref, delta_scr, dq_scr, dk_scr, dv_scr, dq_out, dk_out, dv_out, dq_sem, kv_sem):
    head, blk = pl.program_id(0), pl.program_id(1)
    n_head, n_blk = pl.num_programs(0), pl.num_programs(1)
    half = head_dim // 2
    wide = groups * BLK
    q_width = groups * head_dim
    slot = blk % 2

    @pl.when(blk == 0)
    def _():
        @pl.loop(0, n_blk)
        def _(i):
            rows = pl.ds(pl.multiple_of(i * BLK, BLK), BLK)
            dk_scr[rows, :] = jnp.zeros((BLK, head_dim), jnp.float32)
            dv_scr[rows, :] = jnp.zeros((BLK, head_dim), jnp.float32)

    q_all = stack_heads(q_ref[...], groups, head_dim)
    do_all = stack_heads(do_ref[...], groups, head_dim)
    o_all = stack_heads(o_ref[...], groups, head_dim)
    floor_row = jnp.concatenate([pos_ref[...]] * groups, axis=1) - WINDOW
    lse_row = lse_ref[0, 0]

    def visit(blocks, with_diagonal):
        if with_diagonal:
            delta = jnp.sum((do_all.astype(jnp.float32) * o_all.astype(jnp.float32)).T, axis=0, keepdims=True)
            delta_scr[...] = delta
        else:
            delta = delta_scr[...]
        rows = [pl.ds(pl.multiple_of(kb * BLK, BLK), BLK) for kb in blocks]
        k_blks = [k_ref[r, :] for r in rows]
        scores = [dot_f32(k_blk, q_all, 1, 1) for k_blk in k_blks]
        d_probs = [dot_f32(v_ref[r, :], do_all, 1, 1) for r in rows]
        dq_new = None
        for i, r in enumerate(rows):
            tanh_s = jnp.tanh(scores[i] * (1.0 / SOFT_CAP))
            keep = keep_mask(key_pos_ref[r, :], floor_row, wide, with_diagonal and i == 0)
            prob = jnp.exp2(jnp.where(keep, tanh_s * (SOFT_CAP * LOG2E) - lse_row, -1e30))
            d_score = (prob * (d_probs[i] - delta) * (1.0 - tanh_s * tanh_s)).astype(jnp.bfloat16)
            dv_scr[r, :] += jnp.dot(prob.astype(jnp.bfloat16), do_all, preferred_element_type=jnp.float32)
            dk_scr[r, :] += jnp.dot(d_score, q_all, preferred_element_type=jnp.float32)
            term = dot_f32(k_blks[i], d_score, 0, 0)
            dq_new = term if dq_new is None else dq_new + term
        if with_diagonal:
            dq_scr[...] = dq_new
        else:
            dq_scr[...] += dq_new

    visit_pairs(visit, first_ref[blk], blk)

    def dq_copy(h, i):
        dst = out_ref.at[pl.ds(pl.multiple_of(i * BLK, BLK), BLK), pl.ds(pl.multiple_of(h * q_width, q_width), q_width)]
        return pltpu.make_async_copy(dq_out.at[slot], dst, dq_sem.at[slot])

    def kv_copy(which, src, h):
        col = n_head * q_width + which * n_head * head_dim + h * head_dim
        dst = out_ref.at[:, pl.ds(pl.multiple_of(col, head_dim), head_dim)]
        return pltpu.make_async_copy(src, dst, kv_sem.at[which])

    @pl.when(head * n_blk + blk >= 2)
    def _():
        dq_copy(head, blk).wait()

    d_q = dq_scr[...].T
    rows = pl.ds(pl.multiple_of(blk * BLK, BLK), BLK)
    cos_t, sin_t = cos_ref[rows, :], sin_ref[rows, :]
    for g in range(groups):
        part = d_q[g * BLK:(g + 1) * BLK, :]
        part = (part * cos_t - pltpu.roll(part, half, 1) * sin_t) * q_scale
        dq_out[slot, :, g * head_dim:(g + 1) * head_dim] = part.astype(dq_out.dtype)
    dq_copy(head, blk).start()

    @pl.when(blk == n_blk - 1)
    def _():
        @pl.loop(0, n_blk)
        def _(i):
            rows = pl.ds(pl.multiple_of(i * BLK, BLK), BLK)
            part = dk_scr[rows, :]
            part = part * cos_ref[rows, :] - pltpu.roll(part, half, 1) * sin_ref[rows, :]
            dk_out[rows, :] = part.astype(dk_out.dtype)
            dv_out[rows, :] = dv_scr[rows, :].astype(dv_out.dtype)

        kv_copy(0, dk_out, head).start()
        kv_copy(1, dv_out, head).start()
        kv_copy(0, dk_out, head).wait()
        kv_copy(1, dv_out, head).wait()

    @pl.when((blk == n_blk - 1) & (head == n_head - 1))
    def _():
        for s in range(2):
            pltpu.make_async_copy(dq_out.at[s], out_ref.at[pl.ds(0, BLK), pl.ds(0, q_width)], dq_sem.at[s]).wait()


def attn_bwd(q_all, k_all, v_all, o_all, d_o, pos, key_pos, lse, first_blk, cos_t, sin_t, groups, head_dim):
    seq_len, q_cols = q_all.shape
    k_cols = k_all.shape[1]
    kv_heads = k_cols // head_dim
    n_blk = seq_len // BLK
    wide = groups * BLK
    pairs = seq_len * seq_len // 4 * groups * kv_heads
    by_q = pl.BlockSpec((BLK, groups * head_dim), lambda h, i, first: (i, h))
    by_h = pl.BlockSpec((seq_len, head_dim), lambda h, i, first: (0, h))
    table = pl.BlockSpec((seq_len, LANES), lambda h, i, first: (0, 0))
    return pl.pallas_call(
        functools.partial(attn_bwd_kernel, groups, head_dim, head_dim ** -0.5),
        grid_spec=pltpu.PrefetchScalarGridSpec(
            num_scalar_prefetch=1,
            grid=(kv_heads, n_blk),
            in_specs=[
                by_q, by_h, by_h, by_q, by_q,
                pl.BlockSpec((1, BLK), lambda h, i, first: (0, i)),
                table,
                pl.BlockSpec((1, 1, 1, wide), lambda h, i, first: (h, i, 0, 0)),
                table, table,
            ],
            out_specs=pl.BlockSpec(memory_space=pl.ANY),
            scratch_shapes=[
                pltpu.VMEM((1, wide), jnp.float32),
                pltpu.VMEM((head_dim, wide), jnp.float32),
                pltpu.VMEM((seq_len, head_dim), jnp.float32),
                pltpu.VMEM((seq_len, head_dim), jnp.float32),
                pltpu.VMEM((2, BLK, groups * head_dim), jnp.bfloat16),
                pltpu.VMEM((seq_len, head_dim), jnp.bfloat16),
                pltpu.VMEM((seq_len, head_dim), jnp.bfloat16),
                pltpu.SemaphoreType.DMA((2,)),
                pltpu.SemaphoreType.DMA((2,)),
            ],
        ),
        out_shape=jax.ShapeDtypeStruct((seq_len, q_cols + 2 * k_cols), jnp.bfloat16),
        compiler_params=pltpu.CompilerParams(vmem_limit_bytes=48 * 1024 * 1024),
        cost_estimate=pl.CostEstimate(flops=20 * pairs * head_dim, bytes_accessed=16 * seq_len * q_cols, transcendentals=2 * pairs),
        name="attn_bwd",
    )(first_blk, q_all, k_all, v_all, o_all, d_o, pos, key_pos, lse, cos_t, sin_t)


SEQ_ORDER = (1, 2, 0)
GW_ORDER = (1, 0, 2)
GWO_ORDER = (2, 1, 0)


def solution(mesh):
    act_spec = P('dp', 'tp', None)
    head_spec = P(None, 'tp', None)
    grad_spec = P('dp', 'tp', None)
    in_specs = (act_spec, P('dp', 'tp'), act_spec, head_spec, head_spec, head_spec, P('tp', None, None), P(None), P(None))
    out_specs = (act_spec, act_spec, grad_spec, grad_spec, grad_spec, P(('dp', 'tp'), None, None), P('dp'), P('dp'))

    def local_body(x_in, positions, grad_out, w_query, w_key, w_value, w_out, gain_pre, gain_post):
        _, _, depth = x_in.shape
        n_dev = mesh.shape['tp']
        heads_loc, head_dim = w_query.shape[1], w_query.shape[2]
        kv_loc = w_key.shape[1]
        groups = heads_loc // kv_loc
        q_cols, k_cols = heads_loc * head_dim, kv_loc * head_dim

        gain_pre_row, gain_post_row = gain_pre[None, :], gain_post[None, :]
        rows = x_in.shape[1]
        w_out_loc = w_out.reshape(q_cols, depth)
        w_out_all = lax.all_gather(w_out_loc, 'tp', axis=0, tiled=True)
        gathered = {}
        for first_seq, count in ((1, 2), (0, 1)):
            normed = pre_norm(x_in, gain_pre_row, first_seq, count)
            whole = lax.all_gather(normed, 'tp', axis=0, tiled=True).reshape(n_dev, count * rows, depth)
            gathered.update({first_seq + i: (whole, i) for i in range(count)})

        pos_all = lax.all_gather(positions, 'tp', axis=1, tiled=True)
        seq_len = pos_all.shape[1]
        half = head_dim // 2
        inv_freq = ROPE_THETA ** (-2.0 * jnp.arange(half, dtype=jnp.float32) / head_dim)
        before = pos_all[:, None, :] <= pos_all[:, ::BLK, None] - WINDOW
        first_blk = jnp.sum(before.astype(jnp.int32), axis=-1) // BLK
        w_all = jnp.concatenate([w_query.reshape(depth, q_cols), w_key.reshape(depth, k_cols), w_value.reshape(depth, k_cols)], axis=1)
        w_t = w_all.T
        me = lax.axis_index('tp')
        own_dst, pair_dst = me[None], me[None] ^ 1

        def swap(value, bit):
            return lax.ppermute(value, 'tp', [(d, d ^ bit) for d in range(n_dev)])

        saved, d_proj_all = {}, {}
        y_out, d_post = None, jnp.zeros((1, depth), jnp.float32)
        for b in SEQ_ORDER:
            angles = pos_all[b].astype(jnp.float32)[:, None] * inv_freq
            cos_h, sin_h = jnp.cos(angles), jnp.sin(angles)
            cos_t = jnp.concatenate([cos_h, cos_h], axis=-1)
            sin_t = jnp.concatenate([-sin_h, sin_h], axis=-1)
            pos_b = pos_all[b][None, :]
            key_pos = jnp.broadcast_to(pos_all[b][:, None], (seq_len, LANES))
            q_b, k_b, v_b = qkv_project(*gathered[b], rows, w_all, cos_t, sin_t, q_cols, k_cols, head_dim)
            o_b, lse_b = attn_fwd(q_b, k_b, v_b, pos_b, key_pos, first_blk[b], groups, head_dim)
            o_mine = lax.all_to_all(o_b.reshape(n_dev, rows, q_cols), 'tp', split_axis=0, concat_axis=0, tiled=True)
            proj = out_proj(o_mine, w_out_all)
            y_out, d_proj, d_post = post_norm(proj, x_in, grad_out, gain_post_row, d_post, y_out, b)
            d_proj_all[b] = lax.all_gather(d_proj, 'tp', axis=0, tiled=True)
            saved[b] = (q_b, k_b, v_b, o_b, pos_b, key_pos, lse_b, cos_t, sin_t)

        grad_x, d_pre = None, jnp.zeros((1, depth), jnp.float32)
        d_lin = {}
        for b in SEQ_ORDER:
            q_b, k_b, v_b, o_b, pos_b, key_pos, lse_b, cos_t, sin_t = saved[b]
            d_o = dot_f32(d_proj_all[b], w_out_loc, 1, 1).astype(jnp.bfloat16)
            d_lin[b] = attn_bwd(q_b, k_b, v_b, o_b, d_o, pos_b, key_pos, lse_b, first_blk[b], cos_t, sin_t, groups, head_dim)
            pair = grad_normed_pair(pair_dst, d_lin[b], w_t, rows)
            from_pair = swap(pair, 1)
            send_x, keep_x, send_y, keep_y = grad_normed_own(own_dst, d_lin[b], w_t, from_pair)
            near_x = swap(send_x, 2)
            near_y = swap(send_y, 4)
            fold_x, fold_y = fold(keep_x, near_x, keep_y, near_y)
            far_x = swap(fold_x, 4)
            far_y = swap(fold_y, 2)
            grad_x, d_pre = pre_grad((keep_x, near_x, far_x, keep_y, near_y, far_y), x_in, grad_out, gain_pre_row, d_pre, grad_x, b)
        grad_wo = jnp.zeros((), jnp.float32)
        for b in GWO_ORDER:
            grad_wo = grad_wo + dot_f32(saved[b][3], d_proj_all[b], 0, 0)
        grads = ()
        for b in GW_ORDER:
            grads = grad_w(*gathered[b], rows, d_lin[b], (heads_loc, kv_loc, kv_loc), head_dim, grads)
        grad_wq, grad_wk, grad_wv = grads
        grad_pre, grad_post = gain_sum(d_pre, d_post, n_dev)
        grad_pre, grad_post = grad_pre[0], grad_post[0]
        return y_out, grad_x, grad_wq, grad_wk, grad_wv, grad_wo.reshape(w_out.shape), grad_pre, grad_post

    return jax.shard_map(local_body, mesh=mesh, in_specs=in_specs, out_specs=out_specs, check_vma=False)
```

```python
import functools

import jax
import jax.numpy as jnp
from jax import lax
from jax.experimental import pallas as pl
from jax.experimental.pallas import tpu as pltpu
from jax.sharding import PartitionSpec as P


WINDOW = 4096
SOFT_CAP = 50.0
NORM_EPS = 1e-6
ROPE_THETA = 10000.0
LOG2E = 1.4426950408889634
BLK = 256
LANES = 128


def dot_f32(lhs, rhs, lhs_dim, rhs_dim):
    return lax.dot_general(lhs, rhs, (((lhs_dim,), (rhs_dim,)), ((), ())), preferred_element_type=jnp.float32)


ROWS = 64
CHUNK = 16


def row_specs(seq, depth):
    whole = pl.BlockSpec((1, ROWS, depth), lambda i: (seq, i, 0))
    one = pl.BlockSpec((ROWS, depth), lambda i: (i, 0))
    vec = pl.BlockSpec((1, depth), lambda i: (0, 0))
    return whole, one, vec


def inverse_rms(values):
    return lax.rsqrt(jnp.mean(values * values, axis=-1, keepdims=True) + NORM_EPS)


def norm_grad(values, inv, d_out, gain):
    scaled = d_out * gain
    dot = jnp.mean(scaled * values, axis=-1, keepdims=True)
    return scaled * inv - values * (inv * inv * inv * dot)


def fold_rows(block):
    return sum(block[r:r + 8] for r in range(0, CHUNK, 8))


def pre_norm_kernel(x_ref, gain_ref, n_ref):
    gain = 1.0 + gain_ref[...]

    @pl.loop(0, ROWS // CHUNK)
    def _(c):
        rows = pl.ds(pl.multiple_of(c * CHUNK, CHUNK), CHUNK)
        values = x_ref[0, rows, :].astype(jnp.float32)
        n_ref[rows, :] = (values * inverse_rms(values) * gain).astype(n_ref.dtype)


def pre_norm(x_in, gain, first_seq, count):
    _, rows, depth = x_in.shape
    steps = rows // ROWS
    return pl.pallas_call(
        pre_norm_kernel,
        grid=(count, steps),
        in_specs=[pl.BlockSpec((1, ROWS, depth), lambda s, i: (first_seq + s, i, 0)), pl.BlockSpec((1, depth), lambda s, i: (0, 0))],
        out_specs=pl.BlockSpec((ROWS, depth), lambda s, i: (s * steps + i, 0)),
        out_shape=jax.ShapeDtypeStruct((count * rows, depth), jnp.bfloat16),
        compiler_params=pltpu.CompilerParams(vmem_limit_bytes=54 * 1024 * 1024),
        cost_estimate=pl.CostEstimate(flops=count * rows * depth * 400, bytes_accessed=4 * count * rows * depth, transcendentals=count * rows),
        name="pre_norm",
    )(x_in, gain)


def post_norm_kernel(first, proj_ref, x_ref, go_ref, gain_ref, dg_in_ref, *refs):
    y_ref, d_proj_ref, dg_ref, dg_scr = refs[0 if first else 1:]
    step = pl.program_id(0)
    gain = 1.0 + gain_ref[...]

    @pl.when(step == 0)
    def _():
        dg_scr[...] = jnp.zeros_like(dg_scr)

    @pl.loop(0, ROWS // CHUNK)
    def _(c):
        rows = pl.ds(pl.multiple_of(c * CHUNK, CHUNK), CHUNK)
        values = proj_ref[rows, :].astype(jnp.float32)
        inv = inverse_rms(values)
        unit = values * inv
        post = (unit * gain).astype(jnp.bfloat16).astype(jnp.float32)
        y_ref[0, rows, :] = (x_ref[0, rows, :].astype(jnp.float32) + post).astype(y_ref.dtype)
        d_out = go_ref[0, rows, :].astype(jnp.float32)
        dg_scr[...] += fold_rows(d_out * unit)
        d_proj_ref[rows, :] = norm_grad(values, inv, d_out, gain).astype(d_proj_ref.dtype)

    @pl.when(step == pl.num_programs(0) - 1)
    def _():
        dg_ref[...] = dg_in_ref[...] + jnp.sum(dg_scr[...], axis=0, keepdims=True)


def post_norm(proj, x_in, grad_out, gain, dg_in, y_prev, seq):
    _, rows, depth = x_in.shape
    whole, one, vec = row_specs(seq, depth)
    first = y_prev is None
    return pl.pallas_call(
        functools.partial(post_norm_kernel, first),
        grid=(rows // ROWS,),
        in_specs=[one, whole, whole, vec, vec] + ([] if first else [pl.BlockSpec(memory_space=pl.ANY)]),
        out_specs=[whole, one, vec],
        out_shape=[
            jax.ShapeDtypeStruct(x_in.shape, jnp.bfloat16),
            jax.ShapeDtypeStruct((rows, depth), jnp.bfloat16),
            jax.ShapeDtypeStruct((1, depth), jnp.float32),
        ],
        scratch_shapes=[pltpu.VMEM((8, depth), jnp.float32)],
        input_output_aliases={} if first else {5: 0},
        compiler_params=pltpu.CompilerParams(vmem_limit_bytes=54 * 1024 * 1024),
        cost_estimate=pl.CostEstimate(flops=rows * depth * 800, bytes_accessed=10 * rows * depth, transcendentals=rows),
        name="post_norm",
    )(proj, x_in, grad_out, gain, dg_in, *([] if first else [y_prev]))


def pre_grad_kernel(first, *refs):
    pieces, (x_ref, go_ref, gain_ref, dg_in_ref), refs = refs[:6], refs[6:10], refs[10:]
    gx_ref, dg_ref, dg_scr = refs[0 if first else 1:]
    step = pl.program_id(0)
    gain = 1.0 + gain_ref[...]

    @pl.when(step == 0)
    def _():
        dg_scr[...] = jnp.zeros_like(dg_scr)

    @pl.loop(0, ROWS // CHUNK)
    def _(c):
        rows = pl.ds(pl.multiple_of(c * CHUNK, CHUNK), CHUNK)
        values = x_ref[0, rows, :].astype(jnp.float32)
        inv = inverse_rms(values)
        halves = []
        for kept, near, far in (pieces[:3], pieces[3:]):
            halves.append(kept[0, rows, :].astype(jnp.float32) + near[0, rows, :].astype(jnp.float32) + far[rows, :].astype(jnp.float32))
        d_out = jnp.concatenate(halves, axis=1)
        dg_scr[...] += fold_rows(d_out * (values * inv))
        d_x = norm_grad(values, inv, d_out, gain).astype(jnp.bfloat16).astype(jnp.float32)
        gx_ref[0, rows, :] = (go_ref[0, rows, :].astype(jnp.float32) + d_x).astype(gx_ref.dtype)

    @pl.when(step == pl.num_programs(0) - 1)
    def _():
        dg_ref[...] = dg_in_ref[...] + jnp.sum(dg_scr[...], axis=0, keepdims=True)


def pre_grad(pieces, x_in, grad_out, gain, dg_in, gx_prev, seq):
    _, rows, depth = x_in.shape
    whole, _, vec = row_specs(seq, depth)
    pair = pl.BlockSpec((1, ROWS, depth // 2), lambda i: (0, i, 0))
    one = pl.BlockSpec((ROWS, depth // 2), lambda i: (i, 0))
    first = gx_prev is None
    return pl.pallas_call(
        functools.partial(pre_grad_kernel, first),
        grid=(rows // ROWS,),
        in_specs=[pair, pair, one, pair, pair, one, whole, whole, vec, vec] + ([] if first else [pl.BlockSpec(memory_space=pl.ANY)]),
        out_specs=[whole, vec],
        out_shape=[jax.ShapeDtypeStruct(x_in.shape, jnp.bfloat16), jax.ShapeDtypeStruct((1, depth), jnp.float32)],
        scratch_shapes=[pltpu.VMEM((8, depth), jnp.float32)],
        input_output_aliases={} if first else {10: 0},
        compiler_params=pltpu.CompilerParams(vmem_limit_bytes=54 * 1024 * 1024),
        cost_estimate=pl.CostEstimate(flops=rows * depth * 700, bytes_accessed=12 * rows * depth, transcendentals=rows),
        name="pre_grad",
    )(*pieces, x_in, grad_out, gain, dg_in, *([] if first else [gx_prev]))


def out_proj_kernel(me_ref, o_ref, *refs):
    pieces, r_ref = refs[:-1], refs[-1]
    o_all = jnp.concatenate([o_ref[me_ref[0] ^ k] for k in PIECE_DEVICES], axis=1)
    w_all = jnp.concatenate([piece[...] for piece in pieces], axis=0)
    r_ref[...] = jnp.dot(o_all, w_all, preferred_element_type=jnp.float32).astype(r_ref.dtype)


def out_proj(me, o_mine, pieces):
    n_dev, rows, cols = o_mine.shape
    depth = pieces[0].shape[1]
    tile = 768
    return pl.pallas_call(
        out_proj_kernel,
        grid_spec=pltpu.PrefetchScalarGridSpec(
            num_scalar_prefetch=1,
            grid=(depth // tile,),
            in_specs=[pl.BlockSpec((n_dev, rows, cols), lambda i, me: (0, 0, 0), pipeline_mode=pl.Buffered(1))]
            + [pl.BlockSpec((piece.shape[0], tile), lambda i, me: (0, i)) for piece in pieces],
            out_specs=pl.BlockSpec((rows, tile), lambda i, me: (0, i)),
        ),
        out_shape=jax.ShapeDtypeStruct((rows, depth), jnp.bfloat16),
        compiler_params=pltpu.CompilerParams(vmem_limit_bytes=40 * 1024 * 1024),
        cost_estimate=pl.CostEstimate(flops=2 * n_dev * rows * cols * depth, bytes_accessed=2 * n_dev * cols * depth, transcendentals=0),
        name="out_proj",
    )(me, o_mine, *pieces)


PIECE_DEVICES = (0, 1, 2, 4, 3, 5, 6, 7)


PIECE = 1024


def for_columns(width, visit):
    @pl.loop(0, width // PIECE)
    def _(c):
        visit(pl.ds(pl.multiple_of(c * PIECE, PIECE), PIECE))

    if width % PIECE:
        visit(pl.ds(width // PIECE * PIECE, width % PIECE))


def pair_core_kernel(dst_ref, d0_ref, d1_ref, w_ref, out_ref):
    rows = d0_ref.shape[0]
    d_two = jnp.concatenate([d0_ref[...], d1_ref[...]], axis=0)

    def visit(cols):
        value = jnp.dot(d_two, w_ref[:, cols], preferred_element_type=jnp.float32).astype(out_ref.dtype)
        out_ref[0, :, cols] = value[:rows]
        out_ref[1, :, cols] = value[rows:]

    for_columns(w_ref.shape[1], visit)


def grad_normed_pair(dst, d_lin, w_t, rows):
    cols, depth = w_t.shape
    half = depth // 2
    return pl.pallas_call(
        pair_core_kernel,
        grid_spec=pltpu.PrefetchScalarGridSpec(
            num_scalar_prefetch=1,
            grid=(2, 2),
            in_specs=[
                pl.BlockSpec((rows, cols), lambda h, p, dst: (dst[0] ^ (4 * p), 0)),
                pl.BlockSpec((rows, cols), lambda h, p, dst: (dst[0] ^ (4 * p + 2), 0)),
                pl.BlockSpec((cols, half), lambda h, p, dst: (0, h)),
            ],
            out_specs=pl.BlockSpec((2, rows, half), lambda h, p, dst: (p, 0, h)),
        ),
        out_shape=jax.ShapeDtypeStruct((4, rows, depth), jnp.bfloat16),
        compiler_params=pltpu.CompilerParams(vmem_limit_bytes=54 * 1024 * 1024),
        cost_estimate=pl.CostEstimate(flops=8 * rows * cols * depth, bytes_accessed=2 * (4 * rows * depth + cols * depth), transcendentals=0),
        name="grad_normed_pair",
    )(dst, d_lin, d_lin, w_t)


def route(h, j):
    return jnp.where(h == 0, (2 * j + 1) % 5, (j + 2) % 4)


def own_core_kernel(dst_ref, d0_ref, d1_ref, w_ref, add0_ref, add1_ref, *refs):
    outs, (stage, sem) = refs[:4], refs[4:]
    rows = d0_ref.shape[0]
    step = 2 * pl.program_id(0) + pl.program_id(1)
    slot = step % 2
    d_two = jnp.concatenate([d0_ref[...], d1_ref[...]], axis=0)

    def copy_out(out):
        return pltpu.make_async_copy(stage.at[slot], out, sem.at[slot])

    @pl.when(step >= 2)
    def _():
        copy_out(outs[0]).wait()

    def visit(cols):
        value = jnp.dot(d_two, w_ref[:, cols], preferred_element_type=jnp.float32)
        stage[slot, 0, :, cols] = (value[:rows] + add0_ref[0, :, cols].astype(jnp.float32)).astype(stage.dtype)
        stage[slot, 1, :, cols] = (value[rows:] + add1_ref[0, :, cols].astype(jnp.float32)).astype(stage.dtype)

    for_columns(w_ref.shape[1], visit)
    for i, out in enumerate(outs):
        @pl.when(step == i)
        def _(out=out):
            copy_out(out).start()

    @pl.when(step == 3)
    def _():
        for s in range(2):
            pltpu.make_async_copy(stage.at[s], outs[0], sem.at[s]).wait()


def grad_normed_own(dst, d_lin, w_t, from_pair):
    _, rows, depth = from_pair.shape
    cols = w_t.shape[0]
    half = depth // 2
    return pl.pallas_call(
        own_core_kernel,
        grid_spec=pltpu.PrefetchScalarGridSpec(
            num_scalar_prefetch=1,
            grid=(2, 2),
            in_specs=[
                pl.BlockSpec((rows, cols), lambda h, p, dst: (dst[0] ^ (2 * route(h, 2 * p)), 0)),
                pl.BlockSpec((rows, cols), lambda h, p, dst: (dst[0] ^ (2 * route(h, 2 * p + 1)), 0)),
                pl.BlockSpec((cols, half), lambda h, p, dst: (0, h)),
                pl.BlockSpec((1, rows, half), lambda h, p, dst: (route(h, 2 * p), 0, h)),
                pl.BlockSpec((1, rows, half), lambda h, p, dst: (route(h, 2 * p + 1), 0, h)),
            ],
            out_specs=[pl.BlockSpec(memory_space=pl.ANY)] * 4,
            scratch_shapes=[pltpu.VMEM((2, 2, rows, half), jnp.bfloat16), pltpu.SemaphoreType.DMA((2,))],
        ),
        out_shape=[jax.ShapeDtypeStruct((2, rows, half), jnp.bfloat16)] * 4,
        compiler_params=pltpu.CompilerParams(vmem_limit_bytes=56 * 1024 * 1024),
        cost_estimate=pl.CostEstimate(flops=8 * rows * cols * depth, bytes_accessed=2 * (8 * rows * depth + cols * depth), transcendentals=0),
        name="grad_normed_own",
    )(dst, d_lin, d_lin, w_t, from_pair, from_pair)


def fold_kernel(keep_x_ref, near_x_ref, keep_y_ref, near_y_ref, x_ref, y_ref):
    for out, kept, near in ((x_ref, keep_x_ref, near_x_ref), (y_ref, keep_y_ref, near_y_ref)):
        out[...] = (kept[0].astype(jnp.float32) + near[0].astype(jnp.float32)).astype(out.dtype)


def fold(keep_x, near_x, keep_y, near_y):
    _, rows, half = keep_x.shape
    tile = 96
    second = pl.BlockSpec((1, tile, half), lambda i: (1, i, 0))
    out = pl.BlockSpec((tile, half), lambda i: (i, 0))
    return pl.pallas_call(
        fold_kernel,
        grid=(rows // tile,),
        in_specs=[second] * 4,
        out_specs=[out, out],
        out_shape=[jax.ShapeDtypeStruct((rows, half), jnp.bfloat16)] * 2,
        compiler_params=pltpu.CompilerParams(vmem_limit_bytes=54 * 1024 * 1024),
        cost_estimate=pl.CostEstimate(flops=rows * half * 800, bytes_accessed=12 * rows * half, transcendentals=0),
        name="fold",
    )(keep_x, near_x, keep_y, near_y)


def gain_sum_kernel(n_dev, pre_ref, post_ref, pre_out, post_out, slots, local_sem, send_sem, recv_sem):
    me = lax.axis_index('tp')
    sources = (pre_ref, post_ref)
    sends, locals_ = [], []
    for off in range(1, n_dev):
        for which, src in enumerate(sources):
            copy = pltpu.make_async_remote_copy(
                src_ref=src, dst_ref=slots.at[which, me], send_sem=send_sem.at[which, off], recv_sem=recv_sem.at[which, me],
                device_id={'tp': lax.rem(me + off, n_dev)}, device_id_type=pl.DeviceIdType.MESH)
            copy.start()
            sends.append(copy)
    for which, src in enumerate(sources):
        copy = pltpu.make_async_copy(src, slots.at[which, me], local_sem.at[which])
        copy.start()
        locals_.append(copy)
    for copy in locals_:
        copy.wait()
    for off in range(1, n_dev):
        other = lax.rem(me + off, n_dev)
        for which, src in enumerate(sources):
            pltpu.make_async_remote_copy(
                src_ref=src, dst_ref=slots.at[which, other], send_sem=send_sem.at[which, off], recv_sem=recv_sem.at[which, other],
                device_id={'tp': other}, device_id_type=pl.DeviceIdType.MESH).wait_recv()
    for copy in sends:
        copy.wait_send()
    for which, out in enumerate((pre_out, post_out)):
        total = slots[which, 0]
        for d in range(1, n_dev):
            total = total + slots[which, d]
        out[...] = total


def gain_sum(d_pre, d_post, n_dev):
    depth = d_pre.shape[1]
    vmem = pl.BlockSpec(memory_space=pltpu.VMEM)
    return pl.pallas_call(
        functools.partial(gain_sum_kernel, n_dev),
        in_specs=[vmem, vmem],
        out_specs=[vmem, vmem],
        out_shape=[jax.ShapeDtypeStruct((1, depth), jnp.float32)] * 2,
        scratch_shapes=[
            pltpu.VMEM((2, n_dev, 1, depth), jnp.float32),
            pltpu.SemaphoreType.DMA((2,)),
            pltpu.SemaphoreType.DMA((2, n_dev)),
            pltpu.SemaphoreType.DMA((2, n_dev)),
        ],
        compiler_params=pltpu.CompilerParams(has_side_effects=True),
        name="gain_sum",
    )(d_pre, d_post)


def grad_w_kernel(has_prev, split, head_dim, a_ref, d_ref, *refs):
    outs = refs[1:] if has_prev else refs
    n_dev, rows, tile = a_ref.shape
    step = 256

    @pl.loop(0, tile // step)
    def _(m):
        cols = pl.ds(pl.multiple_of(m * step, step), step)
        total = dot_f32(a_ref[:, :, cols].reshape(n_dev * rows, step), d_ref[...], 0, 0)
        if has_prev:
            total = total + refs[0][cols, :]
        if not split:
            outs[0][cols, :] = total
            return
        col = 0
        for out in outs:
            for h in range(out.shape[1]):
                out[cols, h, :] = total[:, col:col + head_dim]
                col += head_dim


def grad_w(gathered, slot, rows, d_lin, heads, head_dim, prev, last):
    n_dev, _, depth = gathered.shape
    seq_len, cols = d_lin.shape
    tile = 768
    flat = pl.BlockSpec((tile, cols), lambda i: (i, 0))
    has_prev = prev is not None
    if last:
        out_specs = [pl.BlockSpec((tile, h, head_dim), lambda i: (i, 0, 0)) for h in heads]
        out_shape = [jax.ShapeDtypeStruct((depth, h, head_dim), jnp.float32) for h in heads]
    else:
        out_specs, out_shape = flat, jax.ShapeDtypeStruct((depth, cols), jnp.float32)
    return pl.pallas_call(
        functools.partial(grad_w_kernel, has_prev, last, head_dim),
        grid=(depth // tile,),
        in_specs=[
            pl.BlockSpec((n_dev, rows, tile), lambda i: (0, slot, i)),
            pl.BlockSpec((seq_len, cols), lambda i: (0, 0), pipeline_mode=pl.Buffered(1)),
        ] + ([flat] if has_prev else []),
        out_specs=out_specs,
        out_shape=out_shape,
        input_output_aliases={2: 0} if has_prev and not last else {},
        compiler_params=pltpu.CompilerParams(vmem_limit_bytes=58 * 1024 * 1024),
        cost_estimate=pl.CostEstimate(flops=2 * seq_len * depth * cols, bytes_accessed=2 * seq_len * (depth + cols) + 8 * depth * cols, transcendentals=0),
        name="grad_w",
    )(gathered, d_lin, *([prev] if has_prev else []))


def grad_wo_kernel(has_prev, o_ref, d_ref, *refs):
    out = refs[-1]
    total = dot_f32(o_ref[...], d_ref[...], 0, 0)
    out[...] = total + refs[0][...] if has_prev else total


def grad_wo_sum(o_all, d_proj, prev):
    seq_len, cols = o_all.shape
    depth = d_proj.shape[1]
    tile = 768
    has_prev = prev is not None
    flat = pl.BlockSpec((cols, tile), lambda i: (0, i))
    return pl.pallas_call(
        functools.partial(grad_wo_kernel, has_prev),
        grid=(depth // tile,),
        in_specs=[
            pl.BlockSpec((seq_len, cols), lambda i: (0, 0), pipeline_mode=pl.Buffered(1)),
            pl.BlockSpec((seq_len, tile), lambda i: (0, i)),
        ] + ([flat] if has_prev else []),
        out_specs=flat,
        out_shape=jax.ShapeDtypeStruct((cols, depth), jnp.float32),
        input_output_aliases={2: 0} if has_prev else {},
        compiler_params=pltpu.CompilerParams(vmem_limit_bytes=54 * 1024 * 1024),
        cost_estimate=pl.CostEstimate(flops=2 * seq_len * depth * cols, bytes_accessed=2 * seq_len * (depth + cols) + 8 * depth * cols, transcendentals=0),
        name="grad_wo",
    )(o_all, d_proj, *([prev] if has_prev else []))


def qkv_kernel(q_cols, k_cols, head_dim, q_scale, a_ref, w_ref, cos_ref, sin_ref, q_ref, k_ref, v_ref):
    n_dev, rows, depth = a_ref.shape
    lin = jnp.dot(a_ref[...].reshape(n_dev * rows, depth), w_ref[...], preferred_element_type=jnp.float32)
    cos_t, sin_t = cos_ref[...], sin_ref[...]
    for h in range((q_cols + k_cols) // head_dim):
        col = h * head_dim
        part = lin[:, col:col + head_dim]
        part = part * cos_t + pltpu.roll(part, head_dim // 2, 1) * sin_t
        if col < q_cols:
            q_ref[:, col:col + head_dim] = (part * q_scale).astype(q_ref.dtype)
        else:
            k_ref[:, col - q_cols:col - q_cols + head_dim] = part.astype(k_ref.dtype)
    v_ref[...] = lin[:, q_cols + k_cols:].astype(v_ref.dtype)


def qkv_project(gathered, slot, rows, w_all, cos_t, sin_t, q_cols, k_cols, head_dim):
    n_dev, _, depth = gathered.shape
    cols = w_all.shape[1]
    v_cols = cols - q_cols - k_cols
    seq_len, tile = n_dev * rows, 2 * rows
    by_row = [pl.BlockSpec((tile, width), lambda i: (i, 0)) for width in (head_dim, head_dim, q_cols, k_cols, v_cols)]
    return pl.pallas_call(
        functools.partial(qkv_kernel, q_cols, k_cols, head_dim, head_dim ** -0.5),
        grid=(n_dev // 2,),
        in_specs=[
            pl.BlockSpec((2, rows, depth), lambda i: (i, slot, 0)),
            pl.BlockSpec((depth, cols), lambda i: (0, 0), pipeline_mode=pl.Buffered(1)),
        ] + by_row[:2],
        out_specs=by_row[2:],
        out_shape=[jax.ShapeDtypeStruct((seq_len, width), jnp.bfloat16) for width in (q_cols, k_cols, v_cols)],
        compiler_params=pltpu.CompilerParams(vmem_limit_bytes=58 * 1024 * 1024),
        cost_estimate=pl.CostEstimate(flops=2 * seq_len * depth * cols, bytes_accessed=2 * (seq_len * depth + depth * cols + seq_len * cols), transcendentals=0),
        name="qkv_project",
    )(gathered, w_all, cos_t, sin_t)


def stack_heads(block, groups, head_dim):
    return jnp.concatenate([block[:, g * head_dim:(g + 1) * head_dim] for g in range(groups)], axis=0)


def keep_mask(key_pos, floor_row, wide, diagonal):
    keep = jnp.concatenate([key_pos] * (wide // LANES), axis=1) > floor_row
    if diagonal:
        key_idx = lax.broadcasted_iota(jnp.int32, (BLK, wide), 0)
        q_idx = lax.broadcasted_iota(jnp.int32, (BLK, wide), 1) % BLK
        keep = keep & (key_idx <= q_idx)
    return keep


def visit_pairs(visit, first, blk):
    odd = (blk - first) % 2

    @pl.when(odd == 0)
    def _():
        visit([blk], True)

    @pl.when(odd == 1)
    def _():
        visit([blk, blk - 1], True)

    @pl.loop(0, (blk - first) // 2)
    def _(i):
        visit([first + 2 * i, first + 2 * i + 1], False)


def attn_fwd_kernel(groups, head_dim, first_ref, q_ref, k_ref, v_ref, pos_ref, key_pos_ref, o_ref, lse_ref, m_scr, l_scr, acc_scr):
    blk = pl.program_id(1)
    q_all = stack_heads(q_ref[...], groups, head_dim)
    floor_row = jnp.concatenate([pos_ref[...]] * groups, axis=1) - WINDOW
    wide = groups * BLK

    def visit(blocks, with_diagonal):
        rows = [pl.ds(pl.multiple_of(kb * BLK, BLK), BLK) for kb in blocks]
        scores = [dot_f32(k_ref[r, :], q_all, 1, 1) for r in rows]
        capped = []
        for i, r in enumerate(rows):
            keep = keep_mask(key_pos_ref[r, :], floor_row, wide, with_diagonal and i == 0)
            capped.append(jnp.where(keep, jnp.tanh(scores[i] * (1.0 / SOFT_CAP)) * (SOFT_CAP * LOG2E), -1e30))
        top = functools.reduce(jnp.maximum, [jnp.max(c, axis=0, keepdims=True) for c in capped])
        if not with_diagonal:
            m_old = m_scr[...]
            top = jnp.maximum(m_old, top)
            alpha = jnp.exp2(m_old - top)
        m_scr[...] = top
        probs = [jnp.exp2(c - top) for c in capped]
        total = sum(jnp.sum(p, axis=0, keepdims=True) for p in probs)
        acc = sum(dot_f32(v_ref[r, :], p.astype(jnp.bfloat16), 0, 0) for r, p in zip(rows, probs))
        if with_diagonal:
            l_scr[...] = total
            acc_scr[...] = acc
        else:
            l_scr[...] = l_scr[...] * alpha + total
            acc_scr[...] = acc_scr[...] * alpha + acc

    visit_pairs(visit, first_ref[blk], blk)

    total = l_scr[...]
    out = (acc_scr[...] / total).T
    for g in range(groups):
        o_ref[:, g * head_dim:(g + 1) * head_dim] = out[g * BLK:(g + 1) * BLK, :].astype(o_ref.dtype)
    lse_ref[0, 0] = m_scr[...] + jnp.log2(total)


def attn_fwd(q_all, k_all, v_all, pos, key_pos, first_blk, groups, head_dim):
    seq_len, q_cols = q_all.shape
    kv_heads = k_all.shape[1] // head_dim
    n_blk = seq_len // BLK
    wide = groups * BLK
    pairs = seq_len * seq_len // 4 * groups * kv_heads
    return pl.pallas_call(
        functools.partial(attn_fwd_kernel, groups, head_dim),
        grid_spec=pltpu.PrefetchScalarGridSpec(
            num_scalar_prefetch=1,
            grid=(kv_heads, n_blk),
            in_specs=[
                pl.BlockSpec((BLK, groups * head_dim), lambda h, i, first: (i, h)),
                pl.BlockSpec((seq_len, head_dim), lambda h, i, first: (0, h)),
                pl.BlockSpec((seq_len, head_dim), lambda h, i, first: (0, h)),
                pl.BlockSpec((1, BLK), lambda h, i, first: (0, i)),
                pl.BlockSpec((seq_len, LANES), lambda h, i, first: (0, 0)),
            ],
            out_specs=[
                pl.BlockSpec((BLK, groups * head_dim), lambda h, i, first: (i, h)),
                pl.BlockSpec((1, 1, 1, wide), lambda h, i, first: (h, i, 0, 0)),
            ],
            scratch_shapes=[
                pltpu.VMEM((1, wide), jnp.float32),
                pltpu.VMEM((1, wide), jnp.float32),
                pltpu.VMEM((head_dim, wide), jnp.float32),
            ],
        ),
        out_shape=[
            jax.ShapeDtypeStruct((seq_len, q_cols), jnp.bfloat16),
            jax.ShapeDtypeStruct((kv_heads, n_blk, 1, wide), jnp.float32),
        ],
        compiler_params=pltpu.CompilerParams(vmem_limit_bytes=48 * 1024 * 1024),
        cost_estimate=pl.CostEstimate(flops=8 * pairs * head_dim, bytes_accessed=8 * seq_len * q_cols, transcendentals=2 * pairs),
        name="attn_fwd",
    )(first_blk, q_all, k_all, v_all, pos, key_pos)


def attn_bwd_kernel(groups, head_dim, q_scale, first_ref, q_ref, k_ref, v_ref, o_ref, do_ref, pos_ref, key_pos_ref, lse_ref, cos_ref, sin_ref,
                    out_ref, delta_scr, dq_scr, dk_scr, dv_scr, dq_out, dk_out, dv_out, dq_sem, kv_sem):
    head, blk = pl.program_id(0), pl.program_id(1)
    n_head, n_blk = pl.num_programs(0), pl.num_programs(1)
    half = head_dim // 2
    wide = groups * BLK
    q_width = groups * head_dim
    slot = blk % 2

    @pl.when(blk == 0)
    def _():
        @pl.loop(0, n_blk)
        def _(i):
            rows = pl.ds(pl.multiple_of(i * BLK, BLK), BLK)
            dk_scr[rows, :] = jnp.zeros((BLK, head_dim), jnp.float32)
            dv_scr[rows, :] = jnp.zeros((BLK, head_dim), jnp.float32)

    q_all = stack_heads(q_ref[...], groups, head_dim)
    do_all = stack_heads(do_ref[...], groups, head_dim)
    o_all = stack_heads(o_ref[...], groups, head_dim)
    floor_row = jnp.concatenate([pos_ref[...]] * groups, axis=1) - WINDOW
    lse_row = lse_ref[0, 0]

    def visit(blocks, with_diagonal):
        if with_diagonal:
            delta = jnp.sum((do_all.astype(jnp.float32) * o_all.astype(jnp.float32)).T, axis=0, keepdims=True)
            delta_scr[...] = delta
        else:
            delta = delta_scr[...]
        rows = [pl.ds(pl.multiple_of(kb * BLK, BLK), BLK) for kb in blocks]
        k_blks = [k_ref[r, :] for r in rows]
        scores = [dot_f32(k_blk, q_all, 1, 1) for k_blk in k_blks]
        d_probs = [dot_f32(v_ref[r, :], do_all, 1, 1) for r in rows]
        dq_new = None
        for i, r in enumerate(rows):
            tanh_s = jnp.tanh(scores[i] * (1.0 / SOFT_CAP))
            keep = keep_mask(key_pos_ref[r, :], floor_row, wide, with_diagonal and i == 0)
            prob = jnp.exp2(jnp.where(keep, tanh_s * (SOFT_CAP * LOG2E) - lse_row, -1e30))
            d_score = (prob * (d_probs[i] - delta) * (1.0 - tanh_s * tanh_s)).astype(jnp.bfloat16)
            dv_scr[r, :] += jnp.dot(prob.astype(jnp.bfloat16), do_all, preferred_element_type=jnp.float32)
            dk_scr[r, :] += jnp.dot(d_score, q_all, preferred_element_type=jnp.float32)
            term = dot_f32(k_blks[i], d_score, 0, 0)
            dq_new = term if dq_new is None else dq_new + term
        if with_diagonal:
            dq_scr[...] = dq_new
        else:
            dq_scr[...] += dq_new

    visit_pairs(visit, first_ref[blk], blk)

    def dq_copy(h, i):
        dst = out_ref.at[pl.ds(pl.multiple_of(i * BLK, BLK), BLK), pl.ds(pl.multiple_of(h * q_width, q_width), q_width)]
        return pltpu.make_async_copy(dq_out.at[slot], dst, dq_sem.at[slot])

    def kv_copy(which, src, h):
        col = n_head * q_width + which * n_head * head_dim + h * head_dim
        dst = out_ref.at[:, pl.ds(pl.multiple_of(col, head_dim), head_dim)]
        return pltpu.make_async_copy(src, dst, kv_sem.at[which])

    @pl.when(head * n_blk + blk >= 2)
    def _():
        dq_copy(head, blk).wait()

    d_q = dq_scr[...].T
    rows = pl.ds(pl.multiple_of(blk * BLK, BLK), BLK)
    cos_t, sin_t = cos_ref[rows, :], sin_ref[rows, :]
    for g in range(groups):
        part = d_q[g * BLK:(g + 1) * BLK, :]
        part = (part * cos_t - pltpu.roll(part, half, 1) * sin_t) * q_scale
        dq_out[slot, :, g * head_dim:(g + 1) * head_dim] = part.astype(dq_out.dtype)
    dq_copy(head, blk).start()

    @pl.when(blk == n_blk - 1)
    def _():
        @pl.loop(0, n_blk)
        def _(i):
            rows = pl.ds(pl.multiple_of(i * BLK, BLK), BLK)
            part = dk_scr[rows, :]
            part = part * cos_ref[rows, :] - pltpu.roll(part, half, 1) * sin_ref[rows, :]
            dk_out[rows, :] = part.astype(dk_out.dtype)
            dv_out[rows, :] = dv_scr[rows, :].astype(dv_out.dtype)

        kv_copy(0, dk_out, head).start()
        kv_copy(1, dv_out, head).start()
        kv_copy(0, dk_out, head).wait()
        kv_copy(1, dv_out, head).wait()

    @pl.when((blk == n_blk - 1) & (head == n_head - 1))
    def _():
        for s in range(2):
            pltpu.make_async_copy(dq_out.at[s], out_ref.at[pl.ds(0, BLK), pl.ds(0, q_width)], dq_sem.at[s]).wait()


def attn_bwd(q_all, k_all, v_all, o_all, d_o, pos, key_pos, lse, first_blk, cos_t, sin_t, groups, head_dim):
    seq_len, q_cols = q_all.shape
    k_cols = k_all.shape[1]
    kv_heads = k_cols // head_dim
    n_blk = seq_len // BLK
    wide = groups * BLK
    pairs = seq_len * seq_len // 4 * groups * kv_heads
    by_q = pl.BlockSpec((BLK, groups * head_dim), lambda h, i, first: (i, h))
    by_h = pl.BlockSpec((seq_len, head_dim), lambda h, i, first: (0, h))
    table = pl.BlockSpec((seq_len, LANES), lambda h, i, first: (0, 0))
    return pl.pallas_call(
        functools.partial(attn_bwd_kernel, groups, head_dim, head_dim ** -0.5),
        grid_spec=pltpu.PrefetchScalarGridSpec(
            num_scalar_prefetch=1,
            grid=(kv_heads, n_blk),
            in_specs=[
                by_q, by_h, by_h, by_q, by_q,
                pl.BlockSpec((1, BLK), lambda h, i, first: (0, i)),
                table,
                pl.BlockSpec((1, 1, 1, wide), lambda h, i, first: (h, i, 0, 0)),
                table, table,
            ],
            out_specs=pl.BlockSpec(memory_space=pl.ANY),
            scratch_shapes=[
                pltpu.VMEM((1, wide), jnp.float32),
                pltpu.VMEM((head_dim, wide), jnp.float32),
                pltpu.VMEM((seq_len, head_dim), jnp.float32),
                pltpu.VMEM((seq_len, head_dim), jnp.float32),
                pltpu.VMEM((2, BLK, groups * head_dim), jnp.bfloat16),
                pltpu.VMEM((seq_len, head_dim), jnp.bfloat16),
                pltpu.VMEM((seq_len, head_dim), jnp.bfloat16),
                pltpu.SemaphoreType.DMA((2,)),
                pltpu.SemaphoreType.DMA((2,)),
            ],
        ),
        out_shape=jax.ShapeDtypeStruct((seq_len, q_cols + 2 * k_cols), jnp.bfloat16),
        compiler_params=pltpu.CompilerParams(vmem_limit_bytes=48 * 1024 * 1024),
        cost_estimate=pl.CostEstimate(flops=20 * pairs * head_dim, bytes_accessed=16 * seq_len * q_cols, transcendentals=2 * pairs),
        name="attn_bwd",
    )(first_blk, q_all, k_all, v_all, o_all, d_o, pos, key_pos, lse, cos_t, sin_t)


SEQ_ORDER = (1, 2, 0)
GW_ORDER = (1, 0, 2)
GWO_ORDER = (1, 0, 2)


def solution(mesh):
    act_spec = P('dp', 'tp', None)
    head_spec = P(None, 'tp', None)
    grad_spec = P('dp', 'tp', None)
    in_specs = (act_spec, P('dp', 'tp'), act_spec, head_spec, head_spec, head_spec, P('tp', None, None), P(None), P(None))
    out_specs = (act_spec, act_spec, grad_spec, grad_spec, grad_spec, P(('dp', 'tp'), None, None), P('dp'), P('dp'))

    def local_body(x_in, positions, grad_out, w_query, w_key, w_value, w_out, gain_pre, gain_post):
        _, _, depth = x_in.shape
        n_dev = mesh.shape['tp']
        heads_loc, head_dim = w_query.shape[1], w_query.shape[2]
        kv_loc = w_key.shape[1]
        groups = heads_loc // kv_loc
        q_cols, k_cols = heads_loc * head_dim, kv_loc * head_dim

        gain_pre_row, gain_post_row = gain_pre[None, :], gain_post[None, :]
        rows = x_in.shape[1]
        gathered = {}
        for b in SEQ_ORDER:
            normed = pre_norm(x_in, gain_pre_row, b, 1)
            gathered[b] = (lax.all_gather(normed, 'tp', axis=0, tiled=True).reshape(n_dev, rows, depth), 0)

        def swap(value, bit):
            return lax.ppermute(value, 'tp', [(d, d ^ bit) for d in range(n_dev)])

        w_out_loc = w_out.reshape(q_cols, depth)
        mid = q_cols // 2
        near_w = {bit: swap(w_out_loc, bit) for bit in (1, 2, 4)}
        far_w = (swap(near_w[2][:mid], 4), swap(near_w[4][mid:], 2))
        other_core = [swap(near_w[2], 1), swap(near_w[4], 1)]
        far_other = [swap(part, 1) for part in far_w]
        w_out_pieces = (w_out_loc, near_w[1], near_w[2], near_w[4], *other_core, *far_w, *far_other)

        pos_all = lax.all_gather(positions, 'tp', axis=1, tiled=True)
        seq_len = pos_all.shape[1]
        half = head_dim // 2
        inv_freq = ROPE_THETA ** (-2.0 * jnp.arange(half, dtype=jnp.float32) / head_dim)
        before = pos_all[:, None, :] <= pos_all[:, ::BLK, None] - WINDOW
        first_blk = jnp.sum(before.astype(jnp.int32), axis=-1) // BLK
        w_all = jnp.concatenate([w_query.reshape(depth, q_cols), w_key.reshape(depth, k_cols), w_value.reshape(depth, k_cols)], axis=1)
        w_t = w_all.T
        me = lax.axis_index('tp')[None]

        saved, d_proj_all = {}, {}
        y_out, d_post = None, jnp.zeros((1, depth), jnp.float32)
        for b in SEQ_ORDER:
            angles = pos_all[b].astype(jnp.float32)[:, None] * inv_freq
            cos_h, sin_h = jnp.cos(angles), jnp.sin(angles)
            cos_t = jnp.concatenate([cos_h, cos_h], axis=-1)
            sin_t = jnp.concatenate([-sin_h, sin_h], axis=-1)
            pos_b = pos_all[b][None, :]
            key_pos = jnp.broadcast_to(pos_all[b][:, None], (seq_len, LANES))
            q_b, k_b, v_b = qkv_project(*gathered[b], rows, w_all, cos_t, sin_t, q_cols, k_cols, head_dim)
            o_b, lse_b = attn_fwd(q_b, k_b, v_b, pos_b, key_pos, first_blk[b], groups, head_dim)
            o_mine = lax.all_to_all(o_b.reshape(n_dev, rows, q_cols), 'tp', split_axis=0, concat_axis=0, tiled=True)
            proj = out_proj(me, o_mine, w_out_pieces)
            y_out, d_proj, d_post = post_norm(proj, x_in, grad_out, gain_post_row, d_post, y_out, b)
            d_proj_all[b] = lax.all_gather(d_proj, 'tp', axis=0, tiled=True)
            saved[b] = (q_b, k_b, v_b, o_b, pos_b, key_pos, lse_b, cos_t, sin_t)

        grad_x, d_pre = None, jnp.zeros((1, depth), jnp.float32)
        d_lin = {}
        for b in SEQ_ORDER:
            q_b, k_b, v_b, o_b, pos_b, key_pos, lse_b, cos_t, sin_t = saved[b]
            d_o = dot_f32(d_proj_all[b], w_out_loc, 1, 1).astype(jnp.bfloat16)
            d_lin[b] = attn_bwd(q_b, k_b, v_b, o_b, d_o, pos_b, key_pos, lse_b, first_blk[b], cos_t, sin_t, groups, head_dim)
            pair = grad_normed_pair(me ^ 1, d_lin[b], w_t, rows)
            from_pair = swap(pair, 1)
            send_x, keep_x, send_y, keep_y = grad_normed_own(me, d_lin[b], w_t, from_pair)
            near_x = swap(send_x, 2)
            near_y = swap(send_y, 4)
            fold_x, fold_y = fold(keep_x, near_x, keep_y, near_y)
            far_x = swap(fold_x, 4)
            far_y = swap(fold_y, 2)
            grad_x, d_pre = pre_grad((keep_x, near_x, far_x, keep_y, near_y, far_y), x_in, grad_out, gain_pre_row, d_pre, grad_x, b)
        grad_wo = None
        for b in GWO_ORDER:
            grad_wo = grad_wo_sum(saved[b][3], d_proj_all[b], grad_wo)
        grads = None
        for b in GW_ORDER:
            grads = grad_w(*gathered[b], rows, d_lin[b], (heads_loc, kv_loc, kv_loc), head_dim, grads, b == GW_ORDER[-1])
        grad_wq, grad_wk, grad_wv = grads
        grad_pre, grad_post = gain_sum(d_pre, d_post, n_dev)
        grad_pre, grad_post = grad_pre[0], grad_post[0]
        return y_out, grad_x, grad_wq, grad_wk, grad_wv, grad_wo.reshape(w_out.shape), grad_pre, grad_post

    return jax.shard_map(local_body, mesh=mesh, in_specs=in_specs, out_specs=out_specs, check_vma=False)
```

```python
import functools

import jax
import jax.numpy as jnp
from jax import lax
from jax.experimental import pallas as pl
from jax.experimental.pallas import tpu as pltpu
from jax.sharding import PartitionSpec as P


WINDOW = 4096
SOFT_CAP = 50.0
NORM_EPS = 1e-6
ROPE_THETA = 10000.0
LOG2E = 1.4426950408889634
BLK = 256
LANES = 128


def dot_f32(lhs, rhs, lhs_dim, rhs_dim):
    return lax.dot_general(lhs, rhs, (((lhs_dim,), (rhs_dim,)), ((), ())), preferred_element_type=jnp.float32)


ROWS = 64
CHUNK = 16


def row_specs(seq, depth):
    whole = pl.BlockSpec((1, ROWS, depth), lambda i: (seq, i, 0))
    one = pl.BlockSpec((ROWS, depth), lambda i: (i, 0))
    vec = pl.BlockSpec((1, depth), lambda i: (0, 0))
    return whole, one, vec


def inverse_rms(values):
    return lax.rsqrt(jnp.mean(values * values, axis=-1, keepdims=True) + NORM_EPS)


def norm_grad(values, inv, d_out, gain):
    scaled = d_out * gain
    dot = jnp.mean(scaled * values, axis=-1, keepdims=True)
    return scaled * inv - values * (inv * inv * inv * dot)


def fold_rows(block):
    return sum(block[r:r + 8] for r in range(0, CHUNK, 8))


def pre_norm_kernel(x_ref, gain_ref, n_ref):
    gain = 1.0 + gain_ref[...]

    @pl.loop(0, ROWS // CHUNK)
    def _(c):
        rows = pl.ds(pl.multiple_of(c * CHUNK, CHUNK), CHUNK)
        values = x_ref[0, rows, :].astype(jnp.float32)
        n_ref[rows, :] = (values * inverse_rms(values) * gain).astype(n_ref.dtype)


def pre_norm(x_in, gain, first_seq, count):
    _, rows, depth = x_in.shape
    steps = rows // ROWS
    return pl.pallas_call(
        pre_norm_kernel,
        grid=(count, steps),
        in_specs=[pl.BlockSpec((1, ROWS, depth), lambda s, i: (first_seq + s, i, 0)), pl.BlockSpec((1, depth), lambda s, i: (0, 0))],
        out_specs=pl.BlockSpec((ROWS, depth), lambda s, i: (s * steps + i, 0)),
        out_shape=jax.ShapeDtypeStruct((count * rows, depth), jnp.bfloat16),
        compiler_params=pltpu.CompilerParams(vmem_limit_bytes=54 * 1024 * 1024),
        cost_estimate=pl.CostEstimate(flops=count * rows * depth * 400, bytes_accessed=4 * count * rows * depth, transcendentals=count * rows),
        name="pre_norm",
    )(x_in, gain)


def post_norm_kernel(first, proj_ref, x_ref, go_ref, gain_ref, dg_in_ref, *refs):
    y_ref, d_proj_ref, dg_ref, dg_scr = refs[0 if first else 1:]
    step = pl.program_id(0)
    gain = 1.0 + gain_ref[...]

    @pl.when(step == 0)
    def _():
        dg_scr[...] = jnp.zeros_like(dg_scr)

    @pl.loop(0, ROWS // CHUNK)
    def _(c):
        rows = pl.ds(pl.multiple_of(c * CHUNK, CHUNK), CHUNK)
        values = proj_ref[rows, :].astype(jnp.float32)
        inv = inverse_rms(values)
        unit = values * inv
        post = (unit * gain).astype(jnp.bfloat16).astype(jnp.float32)
        y_ref[0, rows, :] = (x_ref[0, rows, :].astype(jnp.float32) + post).astype(y_ref.dtype)
        d_out = go_ref[0, rows, :].astype(jnp.float32)
        dg_scr[...] += fold_rows(d_out * unit)
        d_proj_ref[rows, :] = norm_grad(values, inv, d_out, gain).astype(d_proj_ref.dtype)

    @pl.when(step == pl.num_programs(0) - 1)
    def _():
        dg_ref[...] = dg_in_ref[...] + jnp.sum(dg_scr[...], axis=0, keepdims=True)


def post_norm(proj, x_in, grad_out, gain, dg_in, y_prev, seq):
    _, rows, depth = x_in.shape
    whole, one, vec = row_specs(seq, depth)
    first = y_prev is None
    return pl.pallas_call(
        functools.partial(post_norm_kernel, first),
        grid=(rows // ROWS,),
        in_specs=[one, whole, whole, vec, vec] + ([] if first else [pl.BlockSpec(memory_space=pl.ANY)]),
        out_specs=[whole, one, vec],
        out_shape=[
            jax.ShapeDtypeStruct(x_in.shape, jnp.bfloat16),
            jax.ShapeDtypeStruct((rows, depth), jnp.bfloat16),
            jax.ShapeDtypeStruct((1, depth), jnp.float32),
        ],
        scratch_shapes=[pltpu.VMEM((8, depth), jnp.float32)],
        input_output_aliases={} if first else {5: 0},
        compiler_params=pltpu.CompilerParams(vmem_limit_bytes=54 * 1024 * 1024),
        cost_estimate=pl.CostEstimate(flops=rows * depth * 800, bytes_accessed=10 * rows * depth, transcendentals=rows),
        name="post_norm",
    )(proj, x_in, grad_out, gain, dg_in, *([] if first else [y_prev]))


def pre_grad_kernel(first, *refs):
    pieces, (x_ref, go_ref, gain_ref, dg_in_ref), refs = refs[:6], refs[6:10], refs[10:]
    gx_ref, dg_ref, dg_scr = refs[0 if first else 1:]
    step = pl.program_id(0)
    gain = 1.0 + gain_ref[...]

    @pl.when(step == 0)
    def _():
        dg_scr[...] = jnp.zeros_like(dg_scr)

    @pl.loop(0, ROWS // CHUNK)
    def _(c):
        rows = pl.ds(pl.multiple_of(c * CHUNK, CHUNK), CHUNK)
        values = x_ref[0, rows, :].astype(jnp.float32)
        inv = inverse_rms(values)
        halves = []
        for kept, near, far in (pieces[:3], pieces[3:]):
            halves.append(kept[0, rows, :].astype(jnp.float32) + near[0, rows, :].astype(jnp.float32) + far[rows, :].astype(jnp.float32))
        d_out = jnp.concatenate(halves, axis=1)
        dg_scr[...] += fold_rows(d_out * (values * inv))
        d_x = norm_grad(values, inv, d_out, gain).astype(jnp.bfloat16).astype(jnp.float32)
        gx_ref[0, rows, :] = (go_ref[0, rows, :].astype(jnp.float32) + d_x).astype(gx_ref.dtype)

    @pl.when(step == pl.num_programs(0) - 1)
    def _():
        dg_ref[...] = dg_in_ref[...] + jnp.sum(dg_scr[...], axis=0, keepdims=True)


def pre_grad(pieces, x_in, grad_out, gain, dg_in, gx_prev, seq):
    _, rows, depth = x_in.shape
    whole, _, vec = row_specs(seq, depth)
    pair = pl.BlockSpec((1, ROWS, depth // 2), lambda i: (0, i, 0))
    one = pl.BlockSpec((ROWS, depth // 2), lambda i: (i, 0))
    first = gx_prev is None
    return pl.pallas_call(
        functools.partial(pre_grad_kernel, first),
        grid=(rows // ROWS,),
        in_specs=[pair, pair, one, pair, pair, one, whole, whole, vec, vec] + ([] if first else [pl.BlockSpec(memory_space=pl.ANY)]),
        out_specs=[whole, vec],
        out_shape=[jax.ShapeDtypeStruct(x_in.shape, jnp.bfloat16), jax.ShapeDtypeStruct((1, depth), jnp.float32)],
        scratch_shapes=[pltpu.VMEM((8, depth), jnp.float32)],
        input_output_aliases={} if first else {10: 0},
        compiler_params=pltpu.CompilerParams(vmem_limit_bytes=54 * 1024 * 1024),
        cost_estimate=pl.CostEstimate(flops=rows * depth * 700, bytes_accessed=12 * rows * depth, transcendentals=rows),
        name="pre_grad",
    )(*pieces, x_in, grad_out, gain, dg_in, *([] if first else [gx_prev]))


def out_proj_kernel(me_ref, o_ref, *refs):
    pieces, r_ref = refs[:-1], refs[-1]
    o_all = jnp.concatenate([o_ref[me_ref[0] ^ k] for k in PIECE_DEVICES], axis=1)
    w_all = jnp.concatenate([piece[...] for piece in pieces], axis=0)
    r_ref[...] = jnp.dot(o_all, w_all, preferred_element_type=jnp.float32).astype(r_ref.dtype)


def out_proj(me, o_mine, pieces):
    n_dev, rows, cols = o_mine.shape
    depth = pieces[0].shape[1]
    tile = 768
    return pl.pallas_call(
        out_proj_kernel,
        grid_spec=pltpu.PrefetchScalarGridSpec(
            num_scalar_prefetch=1,
            grid=(depth // tile,),
            in_specs=[pl.BlockSpec((n_dev, rows, cols), lambda i, me: (0, 0, 0), pipeline_mode=pl.Buffered(1))]
            + [pl.BlockSpec((piece.shape[0], tile), lambda i, me: (0, i)) for piece in pieces],
            out_specs=pl.BlockSpec((rows, tile), lambda i, me: (0, i)),
        ),
        out_shape=jax.ShapeDtypeStruct((rows, depth), jnp.bfloat16),
        compiler_params=pltpu.CompilerParams(vmem_limit_bytes=40 * 1024 * 1024),
        cost_estimate=pl.CostEstimate(flops=2 * n_dev * rows * cols * depth, bytes_accessed=2 * n_dev * cols * depth, transcendentals=0),
        name="out_proj",
    )(me, o_mine, *pieces)


PIECE_DEVICES = (0, 1, 2, 4, 3, 5, 6, 7)


PIECE = 1024


def for_columns(width, visit):
    @pl.loop(0, width // PIECE)
    def _(c):
        visit(pl.ds(pl.multiple_of(c * PIECE, PIECE), PIECE))

    if width % PIECE:
        visit(pl.ds(width // PIECE * PIECE, width % PIECE))


def pair_core_kernel(dst_ref, d0_ref, d1_ref, w_ref, out_ref):
    rows = d0_ref.shape[0]
    d_two = jnp.concatenate([d0_ref[...], d1_ref[...]], axis=0)

    def visit(cols):
        value = jnp.dot(d_two, w_ref[:, cols], preferred_element_type=jnp.float32).astype(out_ref.dtype)
        out_ref[0, :, cols] = value[:rows]
        out_ref[1, :, cols] = value[rows:]

    for_columns(w_ref.shape[1], visit)


def grad_normed_pair(dst, d_lin, w_t, rows):
    cols, depth = w_t.shape
    half = depth // 2
    return pl.pallas_call(
        pair_core_kernel,
        grid_spec=pltpu.PrefetchScalarGridSpec(
            num_scalar_prefetch=1,
            grid=(2, 2),
            in_specs=[
                pl.BlockSpec((rows, cols), lambda h, p, dst: (dst[0] ^ (4 * p), 0)),
                pl.BlockSpec((rows, cols), lambda h, p, dst: (dst[0] ^ (4 * p + 2), 0)),
                pl.BlockSpec((cols, half), lambda h, p, dst: (0, h)),
            ],
            out_specs=pl.BlockSpec((2, rows, half), lambda h, p, dst: (p, 0, h)),
        ),
        out_shape=jax.ShapeDtypeStruct((4, rows, depth), jnp.bfloat16),
        compiler_params=pltpu.CompilerParams(vmem_limit_bytes=54 * 1024 * 1024),
        cost_estimate=pl.CostEstimate(flops=8 * rows * cols * depth, bytes_accessed=2 * (4 * rows * depth + cols * depth), transcendentals=0),
        name="grad_normed_pair",
    )(dst, d_lin, d_lin, w_t)


def route(h, j):
    return jnp.where(h == 0, (2 * j + 1) % 5, (j + 2) % 4)


def own_core_kernel(dst_ref, d0_ref, d1_ref, w_ref, add0_ref, add1_ref, *refs):
    outs, (stage, sem) = refs[:4], refs[4:]
    rows = d0_ref.shape[0]
    step = 2 * pl.program_id(0) + pl.program_id(1)
    slot = step % 2
    d_two = jnp.concatenate([d0_ref[...], d1_ref[...]], axis=0)

    def copy_out(out):
        return pltpu.make_async_copy(stage.at[slot], out, sem.at[slot])

    @pl.when(step >= 2)
    def _():
        copy_out(outs[0]).wait()

    def visit(cols):
        value = jnp.dot(d_two, w_ref[:, cols], preferred_element_type=jnp.float32)
        stage[slot, 0, :, cols] = (value[:rows] + add0_ref[0, :, cols].astype(jnp.float32)).astype(stage.dtype)
        stage[slot, 1, :, cols] = (value[rows:] + add1_ref[0, :, cols].astype(jnp.float32)).astype(stage.dtype)

    for_columns(w_ref.shape[1], visit)
    for i, out in enumerate(outs):
        @pl.when(step == i)
        def _(out=out):
            copy_out(out).start()

    @pl.when(step == 3)
    def _():
        for s in range(2):
            pltpu.make_async_copy(stage.at[s], outs[0], sem.at[s]).wait()


def grad_normed_own(dst, d_lin, w_t, from_pair):
    _, rows, depth = from_pair.shape
    cols = w_t.shape[0]
    half = depth // 2
    return pl.pallas_call(
        own_core_kernel,
        grid_spec=pltpu.PrefetchScalarGridSpec(
            num_scalar_prefetch=1,
            grid=(2, 2),
            in_specs=[
                pl.BlockSpec((rows, cols), lambda h, p, dst: (dst[0] ^ (2 * route(h, 2 * p)), 0)),
                pl.BlockSpec((rows, cols), lambda h, p, dst: (dst[0] ^ (2 * route(h, 2 * p + 1)), 0)),
                pl.BlockSpec((cols, half), lambda h, p, dst: (0, h)),
                pl.BlockSpec((1, rows, half), lambda h, p, dst: (route(h, 2 * p), 0, h)),
                pl.BlockSpec((1, rows, half), lambda h, p, dst: (route(h, 2 * p + 1), 0, h)),
            ],
            out_specs=[pl.BlockSpec(memory_space=pl.ANY)] * 4,
            scratch_shapes=[pltpu.VMEM((2, 2, rows, half), jnp.bfloat16), pltpu.SemaphoreType.DMA((2,))],
        ),
        out_shape=[jax.ShapeDtypeStruct((2, rows, half), jnp.bfloat16)] * 4,
        compiler_params=pltpu.CompilerParams(vmem_limit_bytes=56 * 1024 * 1024),
        cost_estimate=pl.CostEstimate(flops=8 * rows * cols * depth, bytes_accessed=2 * (8 * rows * depth + cols * depth), transcendentals=0),
        name="grad_normed_own",
    )(dst, d_lin, d_lin, w_t, from_pair, from_pair)


def fold_kernel(keep_x_ref, near_x_ref, keep_y_ref, near_y_ref, x_ref, y_ref):
    for out, kept, near in ((x_ref, keep_x_ref, near_x_ref), (y_ref, keep_y_ref, near_y_ref)):
        out[...] = (kept[0].astype(jnp.float32) + near[0].astype(jnp.float32)).astype(out.dtype)


def fold(keep_x, near_x, keep_y, near_y):
    _, rows, half = keep_x.shape
    tile = 96
    second = pl.BlockSpec((1, tile, half), lambda i: (1, i, 0))
    out = pl.BlockSpec((tile, half), lambda i: (i, 0))
    return pl.pallas_call(
        fold_kernel,
        grid=(rows // tile,),
        in_specs=[second] * 4,
        out_specs=[out, out],
        out_shape=[jax.ShapeDtypeStruct((rows, half), jnp.bfloat16)] * 2,
        compiler_params=pltpu.CompilerParams(vmem_limit_bytes=54 * 1024 * 1024),
        cost_estimate=pl.CostEstimate(flops=rows * half * 800, bytes_accessed=12 * rows * half, transcendentals=0),
        name="fold",
    )(keep_x, near_x, keep_y, near_y)


def gain_sum_kernel(n_dev, pre_ref, post_ref, pre_out, post_out, slots, local_sem, send_sem, recv_sem):
    me = lax.axis_index('tp')
    sources = (pre_ref, post_ref)
    sends, locals_ = [], []
    for off in range(1, n_dev):
        for which, src in enumerate(sources):
            copy = pltpu.make_async_remote_copy(
                src_ref=src, dst_ref=slots.at[which, me], send_sem=send_sem.at[which, off], recv_sem=recv_sem.at[which, me],
                device_id={'tp': lax.rem(me + off, n_dev)}, device_id_type=pl.DeviceIdType.MESH)
            copy.start()
            sends.append(copy)
    for which, src in enumerate(sources):
        copy = pltpu.make_async_copy(src, slots.at[which, me], local_sem.at[which])
        copy.start()
        locals_.append(copy)
    for copy in locals_:
        copy.wait()
    for off in range(1, n_dev):
        other = lax.rem(me + off, n_dev)
        for which, src in enumerate(sources):
            pltpu.make_async_remote_copy(
                src_ref=src, dst_ref=slots.at[which, other], send_sem=send_sem.at[which, off], recv_sem=recv_sem.at[which, other],
                device_id={'tp': other}, device_id_type=pl.DeviceIdType.MESH).wait_recv()
    for copy in sends:
        copy.wait_send()
    for which, out in enumerate((pre_out, post_out)):
        total = slots[which, 0]
        for d in range(1, n_dev):
            total = total + slots[which, d]
        out[...] = total


def gain_sum(d_pre, d_post, n_dev):
    depth = d_pre.shape[1]
    vmem = pl.BlockSpec(memory_space=pltpu.VMEM)
    return pl.pallas_call(
        functools.partial(gain_sum_kernel, n_dev),
        in_specs=[vmem, vmem],
        out_specs=[vmem, vmem],
        out_shape=[jax.ShapeDtypeStruct((1, depth), jnp.float32)] * 2,
        scratch_shapes=[
            pltpu.VMEM((2, n_dev, 1, depth), jnp.float32),
            pltpu.SemaphoreType.DMA((2,)),
            pltpu.SemaphoreType.DMA((2, n_dev)),
            pltpu.SemaphoreType.DMA((2, n_dev)),
        ],
        compiler_params=pltpu.CompilerParams(has_side_effects=True),
        name="gain_sum",
    )(d_pre, d_post)


def grad_w_kernel(has_prev, split, head_dim, a_ref, d_ref, *refs):
    outs = refs[1:] if has_prev else refs
    n_dev, rows, tile = a_ref.shape
    step = 256

    @pl.loop(0, tile // step)
    def _(m):
        cols = pl.ds(pl.multiple_of(m * step, step), step)
        total = dot_f32(a_ref[:, :, cols].reshape(n_dev * rows, step), d_ref[...], 0, 0)
        if has_prev:
            total = total + refs[0][cols, :]
        if not split:
            outs[0][cols, :] = total
            return
        col = 0
        for out in outs:
            for h in range(out.shape[1]):
                out[cols, h, :] = total[:, col:col + head_dim]
                col += head_dim


def grad_w(gathered, slot, rows, d_lin, heads, head_dim, prev, last):
    n_dev, _, depth = gathered.shape
    seq_len, cols = d_lin.shape
    tile = 768
    flat = pl.BlockSpec((tile, cols), lambda i: (i, 0))
    has_prev = prev is not None
    if last:
        out_specs = [pl.BlockSpec((tile, h, head_dim), lambda i: (i, 0, 0)) for h in heads]
        out_shape = [jax.ShapeDtypeStruct((depth, h, head_dim), jnp.float32) for h in heads]
    else:
        out_specs, out_shape = flat, jax.ShapeDtypeStruct((depth, cols), jnp.float32)
    return pl.pallas_call(
        functools.partial(grad_w_kernel, has_prev, last, head_dim),
        grid=(depth // tile,),
        in_specs=[
            pl.BlockSpec((n_dev, rows, tile), lambda i: (0, slot, i)),
            pl.BlockSpec((seq_len, cols), lambda i: (0, 0), pipeline_mode=pl.Buffered(1)),
        ] + ([flat] if has_prev else []),
        out_specs=out_specs,
        out_shape=out_shape,
        input_output_aliases={2: 0} if has_prev and not last else {},
        compiler_params=pltpu.CompilerParams(vmem_limit_bytes=58 * 1024 * 1024),
        cost_estimate=pl.CostEstimate(flops=2 * seq_len * depth * cols, bytes_accessed=2 * seq_len * (depth + cols) + 8 * depth * cols, transcendentals=0),
        name="grad_w",
    )(gathered, d_lin, *([prev] if has_prev else []))


def grad_wo_kernel(has_prev, o_ref, d_ref, *refs):
    out = refs[-1]
    total = dot_f32(o_ref[...], d_ref[...], 0, 0)
    out[...] = total + refs[0][...] if has_prev else total


def grad_wo_sum(o_all, d_proj, prev):
    seq_len, cols = o_all.shape
    depth = d_proj.shape[1]
    tile = 768
    has_prev = prev is not None
    flat = pl.BlockSpec((cols, tile), lambda i: (0, i))
    return pl.pallas_call(
        functools.partial(grad_wo_kernel, has_prev),
        grid=(depth // tile,),
        in_specs=[
            pl.BlockSpec((seq_len, cols), lambda i: (0, 0), pipeline_mode=pl.Buffered(1)),
            pl.BlockSpec((seq_len, tile), lambda i: (0, i)),
        ] + ([flat] if has_prev else []),
        out_specs=flat,
        out_shape=jax.ShapeDtypeStruct((cols, depth), jnp.float32),
        input_output_aliases={2: 0} if has_prev else {},
        compiler_params=pltpu.CompilerParams(vmem_limit_bytes=54 * 1024 * 1024),
        cost_estimate=pl.CostEstimate(flops=2 * seq_len * depth * cols, bytes_accessed=2 * seq_len * (depth + cols) + 8 * depth * cols, transcendentals=0),
        name="grad_wo",
    )(o_all, d_proj, *([prev] if has_prev else []))


def qkv_kernel(q_cols, k_cols, head_dim, q_scale, a_ref, w_ref, cos_ref, sin_ref, q_ref, k_ref, v_ref):
    n_dev, rows, depth = a_ref.shape
    lin = jnp.dot(a_ref[...].reshape(n_dev * rows, depth), w_ref[...], preferred_element_type=jnp.float32)
    cos_t, sin_t = cos_ref[...], sin_ref[...]
    for h in range((q_cols + k_cols) // head_dim):
        col = h * head_dim
        part = lin[:, col:col + head_dim]
        part = part * cos_t + pltpu.roll(part, head_dim // 2, 1) * sin_t
        if col < q_cols:
            q_ref[:, col:col + head_dim] = (part * q_scale).astype(q_ref.dtype)
        else:
            k_ref[:, col - q_cols:col - q_cols + head_dim] = part.astype(k_ref.dtype)
    v_ref[...] = lin[:, q_cols + k_cols:].astype(v_ref.dtype)


def qkv_project(gathered, slot, rows, w_all, cos_t, sin_t, q_cols, k_cols, head_dim):
    n_dev, _, depth = gathered.shape
    cols = w_all.shape[1]
    v_cols = cols - q_cols - k_cols
    seq_len, tile = n_dev * rows, 2 * rows
    by_row = [pl.BlockSpec((tile, width), lambda i: (i, 0)) for width in (head_dim, head_dim, q_cols, k_cols, v_cols)]
    return pl.pallas_call(
        functools.partial(qkv_kernel, q_cols, k_cols, head_dim, head_dim ** -0.5),
        grid=(n_dev // 2,),
        in_specs=[
            pl.BlockSpec((2, rows, depth), lambda i: (i, slot, 0)),
            pl.BlockSpec((depth, cols), lambda i: (0, 0), pipeline_mode=pl.Buffered(1)),
        ] + by_row[:2],
        out_specs=by_row[2:],
        out_shape=[jax.ShapeDtypeStruct((seq_len, width), jnp.bfloat16) for width in (q_cols, k_cols, v_cols)],
        compiler_params=pltpu.CompilerParams(vmem_limit_bytes=58 * 1024 * 1024),
        cost_estimate=pl.CostEstimate(flops=2 * seq_len * depth * cols, bytes_accessed=2 * (seq_len * depth + depth * cols + seq_len * cols), transcendentals=0),
        name="qkv_project",
    )(gathered, w_all, cos_t, sin_t)


def stack_heads(block, groups, head_dim):
    return jnp.concatenate([block[:, g * head_dim:(g + 1) * head_dim] for g in range(groups)], axis=0)


def keep_mask(key_pos, floor_row, wide, diagonal):
    keep = jnp.concatenate([key_pos] * (wide // LANES), axis=1) > floor_row
    if diagonal:
        key_idx = lax.broadcasted_iota(jnp.int32, (BLK, wide), 0)
        q_idx = lax.broadcasted_iota(jnp.int32, (BLK, wide), 1) % BLK
        keep = keep & (key_idx <= q_idx)
    return keep


def visit_pairs(visit, first, blk):
    odd = (blk - first) % 2

    @pl.when(odd == 0)
    def _():
        visit([blk], True)

    @pl.when(odd == 1)
    def _():
        visit([blk, blk - 1], True)

    @pl.loop(0, (blk - first) // 2)
    def _(i):
        visit([first + 2 * i, first + 2 * i + 1], False)


def attn_fwd_kernel(groups, head_dim, first_ref, q_ref, k_ref, v_ref, pos_ref, key_pos_ref, o_ref, lse_ref, m_scr, l_scr, acc_scr):
    blk = pl.program_id(1)
    q_all = stack_heads(q_ref[...], groups, head_dim)
    floor_row = jnp.concatenate([pos_ref[...]] * groups, axis=1) - WINDOW
    wide = groups * BLK

    def visit(blocks, with_diagonal):
        rows = [pl.ds(pl.multiple_of(kb * BLK, BLK), BLK) for kb in blocks]
        scores = [dot_f32(k_ref[r, :], q_all, 1, 1) for r in rows]
        capped = []
        for i, r in enumerate(rows):
            keep = keep_mask(key_pos_ref[r, :], floor_row, wide, with_diagonal and i == 0)
            capped.append(jnp.where(keep, jnp.tanh(scores[i] * (1.0 / SOFT_CAP)) * (SOFT_CAP * LOG2E), -1e30))
        top = functools.reduce(jnp.maximum, [jnp.max(c, axis=0, keepdims=True) for c in capped])
        if not with_diagonal:
            m_old = m_scr[...]
            top = jnp.maximum(m_old, top)
            alpha = jnp.exp2(m_old - top)
        m_scr[...] = top
        probs = [jnp.exp2(c - top) for c in capped]
        total = sum(jnp.sum(p, axis=0, keepdims=True) for p in probs)
        acc = sum(dot_f32(v_ref[r, :], p.astype(jnp.bfloat16), 0, 0) for r, p in zip(rows, probs))
        if with_diagonal:
            l_scr[...] = total
            acc_scr[...] = acc
        else:
            l_scr[...] = l_scr[...] * alpha + total
            acc_scr[...] = acc_scr[...] * alpha + acc

    visit_pairs(visit, first_ref[blk], blk)

    total = l_scr[...]
    out = (acc_scr[...] / total).T
    for g in range(groups):
        o_ref[:, g * head_dim:(g + 1) * head_dim] = out[g * BLK:(g + 1) * BLK, :].astype(o_ref.dtype)
    lse_ref[0, 0] = m_scr[...] + jnp.log2(total)


def attn_fwd(q_all, k_all, v_all, pos, key_pos, first_blk, groups, head_dim):
    seq_len, q_cols = q_all.shape
    kv_heads = k_all.shape[1] // head_dim
    n_blk = seq_len // BLK
    wide = groups * BLK
    pairs = seq_len * seq_len // 4 * groups * kv_heads
    return pl.pallas_call(
        functools.partial(attn_fwd_kernel, groups, head_dim),
        grid_spec=pltpu.PrefetchScalarGridSpec(
            num_scalar_prefetch=1,
            grid=(kv_heads, n_blk),
            in_specs=[
                pl.BlockSpec((BLK, groups * head_dim), lambda h, i, first: (i, h)),
                pl.BlockSpec((seq_len, head_dim), lambda h, i, first: (0, h)),
                pl.BlockSpec((seq_len, head_dim), lambda h, i, first: (0, h)),
                pl.BlockSpec((1, BLK), lambda h, i, first: (0, i)),
                pl.BlockSpec((seq_len, LANES), lambda h, i, first: (0, 0)),
            ],
            out_specs=[
                pl.BlockSpec((BLK, groups * head_dim), lambda h, i, first: (i, h)),
                pl.BlockSpec((1, 1, 1, wide), lambda h, i, first: (h, i, 0, 0)),
            ],
            scratch_shapes=[
                pltpu.VMEM((1, wide), jnp.float32),
                pltpu.VMEM((1, wide), jnp.float32),
                pltpu.VMEM((head_dim, wide), jnp.float32),
            ],
        ),
        out_shape=[
            jax.ShapeDtypeStruct((seq_len, q_cols), jnp.bfloat16),
            jax.ShapeDtypeStruct((kv_heads, n_blk, 1, wide), jnp.float32),
        ],
        compiler_params=pltpu.CompilerParams(vmem_limit_bytes=48 * 1024 * 1024),
        cost_estimate=pl.CostEstimate(flops=8 * pairs * head_dim, bytes_accessed=8 * seq_len * q_cols, transcendentals=2 * pairs),
        name="attn_fwd",
    )(first_blk, q_all, k_all, v_all, pos, key_pos)


def attn_bwd_kernel(groups, head_dim, q_scale, first_ref, q_ref, k_ref, v_ref, o_ref, do_ref, pos_ref, key_pos_ref, lse_ref, cos_ref, sin_ref,
                    out_ref, delta_scr, dq_scr, dk_scr, dv_scr, dq_out, dk_out, dv_out, dq_sem, kv_sem):
    head, blk = pl.program_id(0), pl.program_id(1)
    n_head, n_blk = pl.num_programs(0), pl.num_programs(1)
    half = head_dim // 2
    wide = groups * BLK
    q_width = groups * head_dim
    slot = blk % 2

    @pl.when(blk == 0)
    def _():
        @pl.loop(0, n_blk)
        def _(i):
            rows = pl.ds(pl.multiple_of(i * BLK, BLK), BLK)
            dk_scr[rows, :] = jnp.zeros((BLK, head_dim), jnp.float32)
            dv_scr[rows, :] = jnp.zeros((BLK, head_dim), jnp.float32)

    q_all = stack_heads(q_ref[...], groups, head_dim)
    do_all = stack_heads(do_ref[...], groups, head_dim)
    o_all = stack_heads(o_ref[...], groups, head_dim)
    floor_row = jnp.concatenate([pos_ref[...]] * groups, axis=1) - WINDOW
    lse_row = lse_ref[0, 0]

    def visit(blocks, with_diagonal):
        if with_diagonal:
            delta = jnp.sum((do_all.astype(jnp.float32) * o_all.astype(jnp.float32)).T, axis=0, keepdims=True)
            delta_scr[...] = delta
        else:
            delta = delta_scr[...]
        rows = [pl.ds(pl.multiple_of(kb * BLK, BLK), BLK) for kb in blocks]
        k_blks = [k_ref[r, :] for r in rows]
        scores = [dot_f32(k_blk, q_all, 1, 1) for k_blk in k_blks]
        d_probs = [dot_f32(v_ref[r, :], do_all, 1, 1) for r in rows]
        dq_new = None
        for i, r in enumerate(rows):
            tanh_s = jnp.tanh(scores[i] * (1.0 / SOFT_CAP))
            keep = keep_mask(key_pos_ref[r, :], floor_row, wide, with_diagonal and i == 0)
            prob = jnp.exp2(jnp.where(keep, tanh_s * (SOFT_CAP * LOG2E) - lse_row, -1e30))
            d_score = (prob * (d_probs[i] - delta) * (1.0 - tanh_s * tanh_s)).astype(jnp.bfloat16)
            dv_scr[r, :] += jnp.dot(prob.astype(jnp.bfloat16), do_all, preferred_element_type=jnp.float32)
            dk_scr[r, :] += jnp.dot(d_score, q_all, preferred_element_type=jnp.float32)
            term = dot_f32(k_blks[i], d_score, 0, 0)
            dq_new = term if dq_new is None else dq_new + term
        if with_diagonal:
            dq_scr[...] = dq_new
        else:
            dq_scr[...] += dq_new

    visit_pairs(visit, first_ref[blk], blk)

    def dq_copy(h, i):
        dst = out_ref.at[pl.ds(pl.multiple_of(i * BLK, BLK), BLK), pl.ds(pl.multiple_of(h * q_width, q_width), q_width)]
        return pltpu.make_async_copy(dq_out.at[slot], dst, dq_sem.at[slot])

    def kv_copy(which, src, h):
        col = n_head * q_width + which * n_head * head_dim + h * head_dim
        dst = out_ref.at[:, pl.ds(pl.multiple_of(col, head_dim), head_dim)]
        return pltpu.make_async_copy(src, dst, kv_sem.at[which])

    @pl.when(head * n_blk + blk >= 2)
    def _():
        dq_copy(head, blk).wait()

    d_q = dq_scr[...].T
    rows = pl.ds(pl.multiple_of(blk * BLK, BLK), BLK)
    cos_t, sin_t = cos_ref[rows, :], sin_ref[rows, :]
    for g in range(groups):
        part = d_q[g * BLK:(g + 1) * BLK, :]
        part = (part * cos_t - pltpu.roll(part, half, 1) * sin_t) * q_scale
        dq_out[slot, :, g * head_dim:(g + 1) * head_dim] = part.astype(dq_out.dtype)
    dq_copy(head, blk).start()

    @pl.when(blk == n_blk - 1)
    def _():
        @pl.loop(0, n_blk)
        def _(i):
            rows = pl.ds(pl.multiple_of(i * BLK, BLK), BLK)
            part = dk_scr[rows, :]
            part = part * cos_ref[rows, :] - pltpu.roll(part, half, 1) * sin_ref[rows, :]
            dk_out[rows, :] = part.astype(dk_out.dtype)
            dv_out[rows, :] = dv_scr[rows, :].astype(dv_out.dtype)

        kv_copy(0, dk_out, head).start()
        kv_copy(1, dv_out, head).start()
        kv_copy(0, dk_out, head).wait()
        kv_copy(1, dv_out, head).wait()

    @pl.when((blk == n_blk - 1) & (head == n_head - 1))
    def _():
        for s in range(2):
            pltpu.make_async_copy(dq_out.at[s], out_ref.at[pl.ds(0, BLK), pl.ds(0, q_width)], dq_sem.at[s]).wait()


def attn_bwd(q_all, k_all, v_all, o_all, d_o, pos, key_pos, lse, first_blk, cos_t, sin_t, groups, head_dim):
    seq_len, q_cols = q_all.shape
    k_cols = k_all.shape[1]
    kv_heads = k_cols // head_dim
    n_blk = seq_len // BLK
    wide = groups * BLK
    pairs = seq_len * seq_len // 4 * groups * kv_heads
    by_q = pl.BlockSpec((BLK, groups * head_dim), lambda h, i, first: (i, h))
    by_h = pl.BlockSpec((seq_len, head_dim), lambda h, i, first: (0, h))
    table = pl.BlockSpec((seq_len, LANES), lambda h, i, first: (0, 0))
    return pl.pallas_call(
        functools.partial(attn_bwd_kernel, groups, head_dim, head_dim ** -0.5),
        grid_spec=pltpu.PrefetchScalarGridSpec(
            num_scalar_prefetch=1,
            grid=(kv_heads, n_blk),
            in_specs=[
                by_q, by_h, by_h, by_q, by_q,
                pl.BlockSpec((1, BLK), lambda h, i, first: (0, i)),
                table,
                pl.BlockSpec((1, 1, 1, wide), lambda h, i, first: (h, i, 0, 0)),
                table, table,
            ],
            out_specs=pl.BlockSpec(memory_space=pl.ANY),
            scratch_shapes=[
                pltpu.VMEM((1, wide), jnp.float32),
                pltpu.VMEM((head_dim, wide), jnp.float32),
                pltpu.VMEM((seq_len, head_dim), jnp.float32),
                pltpu.VMEM((seq_len, head_dim), jnp.float32),
                pltpu.VMEM((2, BLK, groups * head_dim), jnp.bfloat16),
                pltpu.VMEM((seq_len, head_dim), jnp.bfloat16),
                pltpu.VMEM((seq_len, head_dim), jnp.bfloat16),
                pltpu.SemaphoreType.DMA((2,)),
                pltpu.SemaphoreType.DMA((2,)),
            ],
        ),
        out_shape=jax.ShapeDtypeStruct((seq_len, q_cols + 2 * k_cols), jnp.bfloat16),
        compiler_params=pltpu.CompilerParams(vmem_limit_bytes=48 * 1024 * 1024),
        cost_estimate=pl.CostEstimate(flops=20 * pairs * head_dim, bytes_accessed=16 * seq_len * q_cols, transcendentals=2 * pairs),
        name="attn_bwd",
    )(first_blk, q_all, k_all, v_all, o_all, d_o, pos, key_pos, lse, cos_t, sin_t)


SEQ_ORDER = (1, 2, 0)
GW_ORDER = (1, 0, 2)
GWO_ORDER = (1, 2, 0)


def solution(mesh):
    act_spec = P('dp', 'tp', None)
    head_spec = P(None, 'tp', None)
    grad_spec = P('dp', 'tp', None)
    in_specs = (act_spec, P('dp', 'tp'), act_spec, head_spec, head_spec, head_spec, P('tp', None, None), P(None), P(None))
    out_specs = (act_spec, act_spec, grad_spec, grad_spec, grad_spec, P(('dp', 'tp'), None, None), P('dp'), P('dp'))

    def local_body(x_in, positions, grad_out, w_query, w_key, w_value, w_out, gain_pre, gain_post):
        _, _, depth = x_in.shape
        n_dev = mesh.shape['tp']
        heads_loc, head_dim = w_query.shape[1], w_query.shape[2]
        kv_loc = w_key.shape[1]
        groups = heads_loc // kv_loc
        q_cols, k_cols = heads_loc * head_dim, kv_loc * head_dim

        gain_pre_row, gain_post_row = gain_pre[None, :], gain_post[None, :]
        rows = x_in.shape[1]
        normed = {SEQ_ORDER[0]: pre_norm(x_in, gain_pre_row, SEQ_ORDER[0], 1)}
        normed[SEQ_ORDER[0]], positions = lax.optimization_barrier((normed[SEQ_ORDER[0]], positions))
        pos_all = lax.all_gather(positions, 'tp', axis=1, tiled=True)
        w_out_loc, pos_all = lax.optimization_barrier((w_out.reshape(q_cols, depth), pos_all))
        gathered = {}
        for b in SEQ_ORDER:
            if b not in normed:
                normed[b] = pre_norm(x_in, gain_pre_row, b, 1)
            gathered[b] = (lax.all_gather(normed[b], 'tp', axis=0, tiled=True).reshape(n_dev, rows, depth), 0)

        def swap(value, bit):
            return lax.ppermute(value, 'tp', [(d, d ^ bit) for d in range(n_dev)])

        mid = q_cols // 2
        near_w = {bit: swap(w_out_loc, bit) for bit in (1, 2, 4)}
        far_w = (swap(near_w[2][:mid], 4), swap(near_w[4][mid:], 2))
        other_core = [swap(near_w[2], 1), swap(near_w[4], 1)]
        far_other = [swap(part, 1) for part in far_w]
        w_out_pieces = (w_out_loc, near_w[1], near_w[2], near_w[4], *other_core, *far_w, *far_other)

        seq_len = pos_all.shape[1]
        half = head_dim // 2
        inv_freq = ROPE_THETA ** (-2.0 * jnp.arange(half, dtype=jnp.float32) / head_dim)
        before = pos_all[:, None, :] <= pos_all[:, ::BLK, None] - WINDOW
        first_blk = jnp.sum(before.astype(jnp.int32), axis=-1) // BLK
        w_all = jnp.concatenate([w_query.reshape(depth, q_cols), w_key.reshape(depth, k_cols), w_value.reshape(depth, k_cols)], axis=1)
        w_t = w_all.T
        me = lax.axis_index('tp')[None]

        saved, d_proj_all = {}, {}
        y_out, d_post = None, jnp.zeros((1, depth), jnp.float32)
        for b in SEQ_ORDER:
            angles = pos_all[b].astype(jnp.float32)[:, None] * inv_freq
            cos_h, sin_h = jnp.cos(angles), jnp.sin(angles)
            cos_t = jnp.concatenate([cos_h, cos_h], axis=-1)
            sin_t = jnp.concatenate([-sin_h, sin_h], axis=-1)
            pos_b = pos_all[b][None, :]
            key_pos = jnp.broadcast_to(pos_all[b][:, None], (seq_len, LANES))
            q_b, k_b, v_b = qkv_project(*gathered[b], rows, w_all, cos_t, sin_t, q_cols, k_cols, head_dim)
            o_b, lse_b = attn_fwd(q_b, k_b, v_b, pos_b, key_pos, first_blk[b], groups, head_dim)
            o_mine = lax.all_to_all(o_b.reshape(n_dev, rows, q_cols), 'tp', split_axis=0, concat_axis=0, tiled=True)
            proj = out_proj(me, o_mine, w_out_pieces)
            y_out, d_proj, d_post = post_norm(proj, x_in, grad_out, gain_post_row, d_post, y_out, b)
            d_proj_all[b] = lax.all_gather(d_proj, 'tp', axis=0, tiled=True)
            saved[b] = (q_b, k_b, v_b, o_b, pos_b, key_pos, lse_b, cos_t, sin_t)

        grad_x, d_pre = None, jnp.zeros((1, depth), jnp.float32)
        d_lin = {}
        for b in SEQ_ORDER:
            q_b, k_b, v_b, o_b, pos_b, key_pos, lse_b, cos_t, sin_t = saved[b]
            d_o = dot_f32(d_proj_all[b], w_out_loc, 1, 1).astype(jnp.bfloat16)
            d_lin[b] = attn_bwd(q_b, k_b, v_b, o_b, d_o, pos_b, key_pos, lse_b, first_blk[b], cos_t, sin_t, groups, head_dim)
            pair = grad_normed_pair(me ^ 1, d_lin[b], w_t, rows)
            from_pair = swap(pair, 1)
            send_x, keep_x, send_y, keep_y = grad_normed_own(me, d_lin[b], w_t, from_pair)
            near_x = swap(send_x, 2)
            near_y = swap(send_y, 4)
            fold_x, fold_y = fold(keep_x, near_x, keep_y, near_y)
            far_x = swap(fold_x, 4)
            far_y = swap(fold_y, 2)
            grad_x, d_pre = pre_grad((keep_x, near_x, far_x, keep_y, near_y, far_y), x_in, grad_out, gain_pre_row, d_pre, grad_x, b)
        grad_wo = None
        for b in GWO_ORDER:
            grad_wo = grad_wo_sum(saved[b][3], d_proj_all[b], grad_wo)
        grads = None
        for b in GW_ORDER:
            grads = grad_w(*gathered[b], rows, d_lin[b], (heads_loc, kv_loc, kv_loc), head_dim, grads, b == GW_ORDER[-1])
        grad_wq, grad_wk, grad_wv = grads
        grad_pre, grad_post = gain_sum(d_pre, d_post, n_dev)
        grad_pre, grad_post = grad_pre[0], grad_post[0]
        return y_out, grad_x, grad_wq, grad_wk, grad_wv, grad_wo.reshape(w_out.shape), grad_pre, grad_post

    return jax.shard_map(local_body, mesh=mesh, in_specs=in_specs, out_specs=out_specs, check_vma=False)
```

```python
import functools

import jax
import jax.numpy as jnp
from jax import lax
from jax.experimental import pallas as pl
from jax.experimental.pallas import tpu as pltpu
from jax.sharding import PartitionSpec as P


WINDOW = 4096
SOFT_CAP = 50.0
NORM_EPS = 1e-6
ROPE_THETA = 10000.0
LOG2E = 1.4426950408889634
BLK = 256
LANES = 128


def dot_f32(lhs, rhs, lhs_dim, rhs_dim):
    return lax.dot_general(lhs, rhs, (((lhs_dim,), (rhs_dim,)), ((), ())), preferred_element_type=jnp.float32)


ROWS = 64
CHUNK = 16


def row_specs(seq, depth):
    whole = pl.BlockSpec((1, ROWS, depth), lambda i: (seq, i, 0))
    one = pl.BlockSpec((ROWS, depth), lambda i: (i, 0))
    vec = pl.BlockSpec((1, depth), lambda i: (0, 0))
    return whole, one, vec


def inverse_rms(values):
    return lax.rsqrt(jnp.mean(values * values, axis=-1, keepdims=True) + NORM_EPS)


def norm_grad(values, inv, d_out, gain):
    scaled = d_out * gain
    dot = jnp.mean(scaled * values, axis=-1, keepdims=True)
    return scaled * inv - values * (inv * inv * inv * dot)


def fold_rows(block):
    return sum(block[r:r + 8] for r in range(0, CHUNK, 8))


def pre_norm_kernel(x_ref, gain_ref, n_ref):
    gain = 1.0 + gain_ref[...]

    @pl.loop(0, ROWS // CHUNK)
    def _(c):
        rows = pl.ds(pl.multiple_of(c * CHUNK, CHUNK), CHUNK)
        values = x_ref[0, rows, :].astype(jnp.float32)
        n_ref[rows, :] = (values * inverse_rms(values) * gain).astype(n_ref.dtype)


def pre_norm(x_in, gain, first_seq, count):
    _, rows, depth = x_in.shape
    steps = rows // ROWS
    return pl.pallas_call(
        pre_norm_kernel,
        grid=(count, steps),
        in_specs=[pl.BlockSpec((1, ROWS, depth), lambda s, i: (first_seq + s, i, 0)), pl.BlockSpec((1, depth), lambda s, i: (0, 0))],
        out_specs=pl.BlockSpec((ROWS, depth), lambda s, i: (s * steps + i, 0)),
        out_shape=jax.ShapeDtypeStruct((count * rows, depth), jnp.bfloat16),
        compiler_params=pltpu.CompilerParams(vmem_limit_bytes=54 * 1024 * 1024),
        cost_estimate=pl.CostEstimate(flops=count * rows * depth * 400, bytes_accessed=4 * count * rows * depth, transcendentals=count * rows),
        name="pre_norm",
    )(x_in, gain)


def post_norm_kernel(first, proj_ref, x_ref, go_ref, gain_ref, dg_in_ref, *refs):
    y_ref, d_proj_ref, dg_ref, dg_scr = refs[0 if first else 1:]
    step = pl.program_id(0)
    gain = 1.0 + gain_ref[...]

    @pl.when(step == 0)
    def _():
        dg_scr[...] = jnp.zeros_like(dg_scr)

    @pl.loop(0, ROWS // CHUNK)
    def _(c):
        rows = pl.ds(pl.multiple_of(c * CHUNK, CHUNK), CHUNK)
        values = proj_ref[rows, :].astype(jnp.float32)
        inv = inverse_rms(values)
        unit = values * inv
        post = (unit * gain).astype(jnp.bfloat16).astype(jnp.float32)
        y_ref[0, rows, :] = (x_ref[0, rows, :].astype(jnp.float32) + post).astype(y_ref.dtype)
        d_out = go_ref[0, rows, :].astype(jnp.float32)
        dg_scr[...] += fold_rows(d_out * unit)
        d_proj_ref[rows, :] = norm_grad(values, inv, d_out, gain).astype(d_proj_ref.dtype)

    @pl.when(step == pl.num_programs(0) - 1)
    def _():
        dg_ref[...] = dg_in_ref[...] + jnp.sum(dg_scr[...], axis=0, keepdims=True)


def post_norm(proj, x_in, grad_out, gain, dg_in, y_prev, seq):
    _, rows, depth = x_in.shape
    whole, one, vec = row_specs(seq, depth)
    first = y_prev is None
    return pl.pallas_call(
        functools.partial(post_norm_kernel, first),
        grid=(rows // ROWS,),
        in_specs=[one, whole, whole, vec, vec] + ([] if first else [pl.BlockSpec(memory_space=pl.ANY)]),
        out_specs=[whole, one, vec],
        out_shape=[
            jax.ShapeDtypeStruct(x_in.shape, jnp.bfloat16),
            jax.ShapeDtypeStruct((rows, depth), jnp.bfloat16),
            jax.ShapeDtypeStruct((1, depth), jnp.float32),
        ],
        scratch_shapes=[pltpu.VMEM((8, depth), jnp.float32)],
        input_output_aliases={} if first else {5: 0},
        compiler_params=pltpu.CompilerParams(vmem_limit_bytes=54 * 1024 * 1024),
        cost_estimate=pl.CostEstimate(flops=rows * depth * 800, bytes_accessed=10 * rows * depth, transcendentals=rows),
        name="post_norm",
    )(proj, x_in, grad_out, gain, dg_in, *([] if first else [y_prev]))


def pre_grad_kernel(first, *refs):
    pieces, (x_ref, go_ref, gain_ref, dg_in_ref), refs = refs[:6], refs[6:10], refs[10:]
    gx_ref, dg_ref, dg_scr = refs[0 if first else 1:]
    step = pl.program_id(0)
    gain = 1.0 + gain_ref[...]

    @pl.when(step == 0)
    def _():
        dg_scr[...] = jnp.zeros_like(dg_scr)

    @pl.loop(0, ROWS // CHUNK)
    def _(c):
        rows = pl.ds(pl.multiple_of(c * CHUNK, CHUNK), CHUNK)
        values = x_ref[0, rows, :].astype(jnp.float32)
        inv = inverse_rms(values)
        halves = []
        for kept, near, far in (pieces[:3], pieces[3:]):
            halves.append(kept[0, rows, :].astype(jnp.float32) + near[0, rows, :].astype(jnp.float32) + far[rows, :].astype(jnp.float32))
        d_out = jnp.concatenate(halves, axis=1)
        dg_scr[...] += fold_rows(d_out * (values * inv))
        d_x = norm_grad(values, inv, d_out, gain).astype(jnp.bfloat16).astype(jnp.float32)
        gx_ref[0, rows, :] = (go_ref[0, rows, :].astype(jnp.float32) + d_x).astype(gx_ref.dtype)

    @pl.when(step == pl.num_programs(0) - 1)
    def _():
        dg_ref[...] = dg_in_ref[...] + jnp.sum(dg_scr[...], axis=0, keepdims=True)


def pre_grad(pieces, x_in, grad_out, gain, dg_in, gx_prev, seq):
    _, rows, depth = x_in.shape
    whole, _, vec = row_specs(seq, depth)
    pair = pl.BlockSpec((1, ROWS, depth // 2), lambda i: (0, i, 0))
    one = pl.BlockSpec((ROWS, depth // 2), lambda i: (i, 0))
    first = gx_prev is None
    return pl.pallas_call(
        functools.partial(pre_grad_kernel, first),
        grid=(rows // ROWS,),
        in_specs=[pair, pair, one, pair, pair, one, whole, whole, vec, vec] + ([] if first else [pl.BlockSpec(memory_space=pl.ANY)]),
        out_specs=[whole, vec],
        out_shape=[jax.ShapeDtypeStruct(x_in.shape, jnp.bfloat16), jax.ShapeDtypeStruct((1, depth), jnp.float32)],
        scratch_shapes=[pltpu.VMEM((8, depth), jnp.float32)],
        input_output_aliases={} if first else {10: 0},
        compiler_params=pltpu.CompilerParams(vmem_limit_bytes=54 * 1024 * 1024),
        cost_estimate=pl.CostEstimate(flops=rows * depth * 700, bytes_accessed=12 * rows * depth, transcendentals=rows),
        name="pre_grad",
    )(*pieces, x_in, grad_out, gain, dg_in, *([] if first else [gx_prev]))


def out_proj_kernel(me_ref, o_ref, *refs):
    pieces, r_ref = refs[:-1], refs[-1]
    o_all = jnp.concatenate([o_ref[me_ref[0] ^ k] for k in PIECE_DEVICES], axis=1)
    w_all = jnp.concatenate([piece[...] for piece in pieces], axis=0)
    r_ref[...] = jnp.dot(o_all, w_all, preferred_element_type=jnp.float32).astype(r_ref.dtype)


def out_proj(me, o_mine, pieces):
    n_dev, rows, cols = o_mine.shape
    depth = pieces[0].shape[1]
    tile = 768
    return pl.pallas_call(
        out_proj_kernel,
        grid_spec=pltpu.PrefetchScalarGridSpec(
            num_scalar_prefetch=1,
            grid=(depth // tile,),
            in_specs=[pl.BlockSpec((n_dev, rows, cols), lambda i, me: (0, 0, 0), pipeline_mode=pl.Buffered(1))]
            + [pl.BlockSpec((piece.shape[0], tile), lambda i, me: (0, i)) for piece in pieces],
            out_specs=pl.BlockSpec((rows, tile), lambda i, me: (0, i)),
        ),
        out_shape=jax.ShapeDtypeStruct((rows, depth), jnp.bfloat16),
        compiler_params=pltpu.CompilerParams(vmem_limit_bytes=40 * 1024 * 1024),
        cost_estimate=pl.CostEstimate(flops=2 * n_dev * rows * cols * depth, bytes_accessed=2 * n_dev * cols * depth, transcendentals=0),
        name="out_proj",
    )(me, o_mine, *pieces)


PIECE_DEVICES = (0, 1, 2, 4, 3, 5, 6, 7)


PIECE = 1024


def for_columns(width, visit):
    @pl.loop(0, width // PIECE)
    def _(c):
        visit(pl.ds(pl.multiple_of(c * PIECE, PIECE), PIECE))

    if width % PIECE:
        visit(pl.ds(width // PIECE * PIECE, width % PIECE))


def pair_core_kernel(dst_ref, d0_ref, d1_ref, w_ref, out_ref):
    rows = d0_ref.shape[0]
    d_two = jnp.concatenate([d0_ref[...], d1_ref[...]], axis=0)

    def visit(cols):
        value = jnp.dot(d_two, w_ref[:, cols], preferred_element_type=jnp.float32).astype(out_ref.dtype)
        out_ref[0, :, cols] = value[:rows]
        out_ref[1, :, cols] = value[rows:]

    for_columns(w_ref.shape[1], visit)


def grad_normed_pair(dst, d_lin, w_t, rows):
    cols, depth = w_t.shape
    half = depth // 2
    return pl.pallas_call(
        pair_core_kernel,
        grid_spec=pltpu.PrefetchScalarGridSpec(
            num_scalar_prefetch=1,
            grid=(2, 2),
            in_specs=[
                pl.BlockSpec((rows, cols), lambda h, p, dst: (dst[0] ^ (4 * p), 0)),
                pl.BlockSpec((rows, cols), lambda h, p, dst: (dst[0] ^ (4 * p + 2), 0)),
                pl.BlockSpec((cols, half), lambda h, p, dst: (0, h)),
            ],
            out_specs=pl.BlockSpec((2, rows, half), lambda h, p, dst: (p, 0, h)),
        ),
        out_shape=jax.ShapeDtypeStruct((4, rows, depth), jnp.bfloat16),
        compiler_params=pltpu.CompilerParams(vmem_limit_bytes=54 * 1024 * 1024),
        cost_estimate=pl.CostEstimate(flops=8 * rows * cols * depth, bytes_accessed=2 * (4 * rows * depth + cols * depth), transcendentals=0),
        name="grad_normed_pair",
    )(dst, d_lin, d_lin, w_t)


def route(h, j):
    return jnp.where(h == 0, (2 * j + 1) % 5, (j + 2) % 4)


def own_core_kernel(dst_ref, d0_ref, d1_ref, w_ref, add0_ref, add1_ref, *refs):
    outs, (stage, sem) = refs[:4], refs[4:]
    rows = d0_ref.shape[0]
    step = 2 * pl.program_id(0) + pl.program_id(1)
    slot = step % 2
    d_two = jnp.concatenate([d0_ref[...], d1_ref[...]], axis=0)

    def copy_out(out):
        return pltpu.make_async_copy(stage.at[slot], out, sem.at[slot])

    @pl.when(step >= 2)
    def _():
        copy_out(outs[0]).wait()

    def visit(cols):
        value = jnp.dot(d_two, w_ref[:, cols], preferred_element_type=jnp.float32)
        stage[slot, 0, :, cols] = (value[:rows] + add0_ref[0, :, cols].astype(jnp.float32)).astype(stage.dtype)
        stage[slot, 1, :, cols] = (value[rows:] + add1_ref[0, :, cols].astype(jnp.float32)).astype(stage.dtype)

    for_columns(w_ref.shape[1], visit)
    for i, out in enumerate(outs):
        @pl.when(step == i)
        def _(out=out):
            copy_out(out).start()

    @pl.when(step == 3)
    def _():
        for s in range(2):
            pltpu.make_async_copy(stage.at[s], outs[0], sem.at[s]).wait()


def grad_normed_own(dst, d_lin, w_t, from_pair):
    _, rows, depth = from_pair.shape
    cols = w_t.shape[0]
    half = depth // 2
    return pl.pallas_call(
        own_core_kernel,
        grid_spec=pltpu.PrefetchScalarGridSpec(
            num_scalar_prefetch=1,
            grid=(2, 2),
            in_specs=[
                pl.BlockSpec((rows, cols), lambda h, p, dst: (dst[0] ^ (2 * route(h, 2 * p)), 0)),
                pl.BlockSpec((rows, cols), lambda h, p, dst: (dst[0] ^ (2 * route(h, 2 * p + 1)), 0)),
                pl.BlockSpec((cols, half), lambda h, p, dst: (0, h)),
                pl.BlockSpec((1, rows, half), lambda h, p, dst: (route(h, 2 * p), 0, h)),
                pl.BlockSpec((1, rows, half), lambda h, p, dst: (route(h, 2 * p + 1), 0, h)),
            ],
            out_specs=[pl.BlockSpec(memory_space=pl.ANY)] * 4,
            scratch_shapes=[pltpu.VMEM((2, 2, rows, half), jnp.bfloat16), pltpu.SemaphoreType.DMA((2,))],
        ),
        out_shape=[jax.ShapeDtypeStruct((2, rows, half), jnp.bfloat16)] * 4,
        compiler_params=pltpu.CompilerParams(vmem_limit_bytes=56 * 1024 * 1024),
        cost_estimate=pl.CostEstimate(flops=8 * rows * cols * depth, bytes_accessed=2 * (8 * rows * depth + cols * depth), transcendentals=0),
        name="grad_normed_own",
    )(dst, d_lin, d_lin, w_t, from_pair, from_pair)


def fold_kernel(keep_x_ref, near_x_ref, keep_y_ref, near_y_ref, x_ref, y_ref):
    for out, kept, near in ((x_ref, keep_x_ref, near_x_ref), (y_ref, keep_y_ref, near_y_ref)):
        out[...] = (kept[0].astype(jnp.float32) + near[0].astype(jnp.float32)).astype(out.dtype)


def fold(keep_x, near_x, keep_y, near_y):
    _, rows, half = keep_x.shape
    tile = 96
    second = pl.BlockSpec((1, tile, half), lambda i: (1, i, 0))
    out = pl.BlockSpec((tile, half), lambda i: (i, 0))
    return pl.pallas_call(
        fold_kernel,
        grid=(rows // tile,),
        in_specs=[second] * 4,
        out_specs=[out, out],
        out_shape=[jax.ShapeDtypeStruct((rows, half), jnp.bfloat16)] * 2,
        compiler_params=pltpu.CompilerParams(vmem_limit_bytes=54 * 1024 * 1024),
        cost_estimate=pl.CostEstimate(flops=rows * half * 800, bytes_accessed=12 * rows * half, transcendentals=0),
        name="fold",
    )(keep_x, near_x, keep_y, near_y)


def gain_sum_kernel(n_dev, pre_ref, post_ref, pre_out, post_out, slots, local_sem, send_sem, recv_sem):
    me = lax.axis_index('tp')
    sources = (pre_ref, post_ref)
    sends, locals_ = [], []
    for off in range(1, n_dev):
        for which, src in enumerate(sources):
            copy = pltpu.make_async_remote_copy(
                src_ref=src, dst_ref=slots.at[which, me], send_sem=send_sem.at[which, off], recv_sem=recv_sem.at[which, me],
                device_id={'tp': lax.rem(me + off, n_dev)}, device_id_type=pl.DeviceIdType.MESH)
            copy.start()
            sends.append(copy)
    for which, src in enumerate(sources):
        copy = pltpu.make_async_copy(src, slots.at[which, me], local_sem.at[which])
        copy.start()
        locals_.append(copy)
    for copy in locals_:
        copy.wait()
    for off in range(1, n_dev):
        other = lax.rem(me + off, n_dev)
        for which, src in enumerate(sources):
            pltpu.make_async_remote_copy(
                src_ref=src, dst_ref=slots.at[which, other], send_sem=send_sem.at[which, off], recv_sem=recv_sem.at[which, other],
                device_id={'tp': other}, device_id_type=pl.DeviceIdType.MESH).wait_recv()
    for copy in sends:
        copy.wait_send()
    for which, out in enumerate((pre_out, post_out)):
        total = slots[which, 0]
        for d in range(1, n_dev):
            total = total + slots[which, d]
        out[...] = total


def gain_sum(d_pre, d_post, n_dev):
    depth = d_pre.shape[1]
    vmem = pl.BlockSpec(memory_space=pltpu.VMEM)
    return pl.pallas_call(
        functools.partial(gain_sum_kernel, n_dev),
        in_specs=[vmem, vmem],
        out_specs=[vmem, vmem],
        out_shape=[jax.ShapeDtypeStruct((1, depth), jnp.float32)] * 2,
        scratch_shapes=[
            pltpu.VMEM((2, n_dev, 1, depth), jnp.float32),
            pltpu.SemaphoreType.DMA((2,)),
            pltpu.SemaphoreType.DMA((2, n_dev)),
            pltpu.SemaphoreType.DMA((2, n_dev)),
        ],
        compiler_params=pltpu.CompilerParams(has_side_effects=True),
        name="gain_sum",
    )(d_pre, d_post)


def grad_w_kernel(has_prev, split, head_dim, a_ref, d_ref, *refs):
    outs = refs[1:] if has_prev else refs
    n_dev, rows, tile = a_ref.shape
    step = 256

    @pl.loop(0, tile // step)
    def _(m):
        cols = pl.ds(pl.multiple_of(m * step, step), step)
        total = dot_f32(a_ref[:, :, cols].reshape(n_dev * rows, step), d_ref[...], 0, 0)
        if has_prev:
            total = total + refs[0][cols, :]
        if not split:
            outs[0][cols, :] = total
            return
        col = 0
        for out in outs:
            for h in range(out.shape[1]):
                out[cols, h, :] = total[:, col:col + head_dim]
                col += head_dim


def grad_w(gathered, slot, rows, d_lin, heads, head_dim, prev, last):
    n_dev, _, depth = gathered.shape
    seq_len, cols = d_lin.shape
    tile = 768
    flat = pl.BlockSpec((tile, cols), lambda i: (i, 0))
    has_prev = prev is not None
    if last:
        out_specs = [pl.BlockSpec((tile, h, head_dim), lambda i: (i, 0, 0)) for h in heads]
        out_shape = [jax.ShapeDtypeStruct((depth, h, head_dim), jnp.float32) for h in heads]
    else:
        out_specs, out_shape = flat, jax.ShapeDtypeStruct((depth, cols), jnp.float32)
    return pl.pallas_call(
        functools.partial(grad_w_kernel, has_prev, last, head_dim),
        grid=(depth // tile,),
        in_specs=[
            pl.BlockSpec((n_dev, rows, tile), lambda i: (0, slot, i)),
            pl.BlockSpec((seq_len, cols), lambda i: (0, 0), pipeline_mode=pl.Buffered(1)),
        ] + ([flat] if has_prev else []),
        out_specs=out_specs,
        out_shape=out_shape,
        input_output_aliases={2: 0} if has_prev and not last else {},
        compiler_params=pltpu.CompilerParams(vmem_limit_bytes=58 * 1024 * 1024),
        cost_estimate=pl.CostEstimate(flops=2 * seq_len * depth * cols, bytes_accessed=2 * seq_len * (depth + cols) + 8 * depth * cols, transcendentals=0),
        name="grad_w",
    )(gathered, d_lin, *([prev] if has_prev else []))


def grad_wo_kernel(has_prev, o_ref, d_ref, *refs):
    out = refs[-1]
    total = dot_f32(o_ref[...], d_ref[...], 0, 0)
    out[...] = total + refs[0][...] if has_prev else total


def grad_wo_sum(o_all, d_proj, prev):
    seq_len, cols = o_all.shape
    depth = d_proj.shape[1]
    tile = 768
    has_prev = prev is not None
    flat = pl.BlockSpec((cols, tile), lambda i: (0, i))
    return pl.pallas_call(
        functools.partial(grad_wo_kernel, has_prev),
        grid=(depth // tile,),
        in_specs=[
            pl.BlockSpec((seq_len, cols), lambda i: (0, 0), pipeline_mode=pl.Buffered(1)),
            pl.BlockSpec((seq_len, tile), lambda i: (0, i)),
        ] + ([flat] if has_prev else []),
        out_specs=flat,
        out_shape=jax.ShapeDtypeStruct((cols, depth), jnp.float32),
        input_output_aliases={2: 0} if has_prev else {},
        compiler_params=pltpu.CompilerParams(vmem_limit_bytes=54 * 1024 * 1024),
        cost_estimate=pl.CostEstimate(flops=2 * seq_len * depth * cols, bytes_accessed=2 * seq_len * (depth + cols) + 8 * depth * cols, transcendentals=0),
        name="grad_wo",
    )(o_all, d_proj, *([prev] if has_prev else []))


def qkv_kernel(q_cols, k_cols, head_dim, q_scale, dev_ref, *refs):
    pieces, (w_hbm, cos_ref, sin_ref, q_ref, k_ref, v_ref, whole_ref, buf, w_ref, in_sem, out_sem, w_sem) = refs[:-12], refs[-12:]
    n_slot, rows, _ = buf.shape
    groups, taken = [], []
    for piece in pieces:
        taken.append(piece)
        if sum(part.shape[0] for part in taken) == rows:
            groups.append(taken)
            taken = []

    def start_in(p):
        slot = p % n_slot
        for i, group in enumerate(groups):
            @pl.when(p == i)
            def _(group=group):
                row = 0
                for part in group:
                    pltpu.make_async_copy(part, buf.at[slot, pl.ds(row, part.shape[0])], in_sem.at[slot]).start()
                    row += part.shape[0]

    def out_copy(p):
        slot = p % n_slot
        return pltpu.make_async_copy(buf.at[slot], whole_ref.at[dev_ref[p]], out_sem.at[slot])

    w_copy = pltpu.make_async_copy(w_hbm, w_ref, w_sem)
    start_in(0)
    w_copy.start()

    @pl.loop(0, len(groups))
    def _(p):
        slot = p % n_slot
        pltpu.make_async_copy(pieces[0], buf.at[slot], in_sem.at[slot]).wait()
        out_copy(p).start()

        @pl.when(p + 1 < len(groups))
        def _():
            @pl.when(p + 1 >= n_slot)
            def _():
                out_copy(p + 1 - n_slot).wait()

            start_in(p + 1)

        @pl.when(p == 0)
        def _():
            w_copy.wait()

        here = pl.ds(pl.multiple_of(dev_ref[p] * rows, rows), rows)
        lin = jnp.dot(buf[slot], w_ref[...], preferred_element_type=jnp.float32)
        cos_t, sin_t = cos_ref[here, :], sin_ref[here, :]
        for h in range((q_cols + k_cols) // head_dim):
            col = h * head_dim
            part = lin[:, col:col + head_dim]
            part = part * cos_t + pltpu.roll(part, head_dim // 2, 1) * sin_t
            if col < q_cols:
                q_ref[here, col:col + head_dim] = (part * q_scale).astype(q_ref.dtype)
            else:
                k_ref[here, col - q_cols:col - q_cols + head_dim] = part.astype(k_ref.dtype)
        v_ref[here, :] = lin[:, q_cols + k_cols:].astype(v_ref.dtype)

    for p in range(len(groups) - n_slot, len(groups)):
        out_copy(p).wait()


def qkv_project(devices, pieces, w_all, cos_t, sin_t, q_cols, k_cols, head_dim):
    rows, depth = pieces[0].shape
    cols = w_all.shape[1]
    seq_len = cos_t.shape[0]
    n_dev = seq_len // rows
    widths = (q_cols, k_cols, cols - q_cols - k_cols)
    hbm, vmem = pl.BlockSpec(memory_space=pl.ANY), pl.BlockSpec(memory_space=pltpu.VMEM)
    return pl.pallas_call(
        functools.partial(qkv_kernel, q_cols, k_cols, head_dim, head_dim ** -0.5),
        in_specs=[pl.BlockSpec(memory_space=pltpu.SMEM)] + [hbm] * (len(pieces) + 1) + [vmem] * 2,
        out_specs=[vmem] * 3 + [hbm],
        out_shape=[jax.ShapeDtypeStruct((seq_len, width), jnp.bfloat16) for width in widths]
        + [jax.ShapeDtypeStruct((n_dev, rows, depth), jnp.bfloat16)],
        scratch_shapes=[
            pltpu.VMEM((3, rows, depth), jnp.bfloat16),
            pltpu.VMEM((depth, cols), jnp.bfloat16),
            pltpu.SemaphoreType.DMA((3,)),
            pltpu.SemaphoreType.DMA((3,)),
            pltpu.SemaphoreType.DMA,
        ],
        compiler_params=pltpu.CompilerParams(vmem_limit_bytes=56 * 1024 * 1024),
        cost_estimate=pl.CostEstimate(flops=2 * seq_len * depth * cols, bytes_accessed=2 * (2 * seq_len * depth + depth * cols + seq_len * cols), transcendentals=0),
        name="qkv_project",
    )(devices, *pieces, w_all, cos_t, sin_t)


def stack_heads(block, groups, head_dim):
    return jnp.concatenate([block[:, g * head_dim:(g + 1) * head_dim] for g in range(groups)], axis=0)


def keep_mask(key_pos, floor_row, wide, diagonal):
    keep = jnp.concatenate([key_pos] * (wide // LANES), axis=1) > floor_row
    if diagonal:
        key_idx = lax.broadcasted_iota(jnp.int32, (BLK, wide), 0)
        q_idx = lax.broadcasted_iota(jnp.int32, (BLK, wide), 1) % BLK
        keep = keep & (key_idx <= q_idx)
    return keep


def visit_pairs(visit, first, blk):
    odd = (blk - first) % 2

    @pl.when(odd == 0)
    def _():
        visit([blk], True)

    @pl.when(odd == 1)
    def _():
        visit([blk, blk - 1], True)

    @pl.loop(0, (blk - first) // 2)
    def _(i):
        visit([first + 2 * i, first + 2 * i + 1], False)


def attn_fwd_kernel(groups, head_dim, first_ref, q_ref, k_ref, v_ref, pos_ref, key_pos_ref, o_ref, lse_ref, m_scr, l_scr, acc_scr):
    blk = pl.program_id(1)
    q_all = stack_heads(q_ref[...], groups, head_dim)
    floor_row = jnp.concatenate([pos_ref[...]] * groups, axis=1) - WINDOW
    wide = groups * BLK

    def visit(blocks, with_diagonal):
        rows = [pl.ds(pl.multiple_of(kb * BLK, BLK), BLK) for kb in blocks]
        scores = [dot_f32(k_ref[r, :], q_all, 1, 1) for r in rows]
        capped = []
        for i, r in enumerate(rows):
            keep = keep_mask(key_pos_ref[r, :], floor_row, wide, with_diagonal and i == 0)
            capped.append(jnp.where(keep, jnp.tanh(scores[i] * (1.0 / SOFT_CAP)) * (SOFT_CAP * LOG2E), -1e30))
        top = functools.reduce(jnp.maximum, [jnp.max(c, axis=0, keepdims=True) for c in capped])
        if not with_diagonal:
            m_old = m_scr[...]
            top = jnp.maximum(m_old, top)
            alpha = jnp.exp2(m_old - top)
        m_scr[...] = top
        probs = [jnp.exp2(c - top) for c in capped]
        total = sum(jnp.sum(p, axis=0, keepdims=True) for p in probs)
        acc = sum(dot_f32(v_ref[r, :], p.astype(jnp.bfloat16), 0, 0) for r, p in zip(rows, probs))
        if with_diagonal:
            l_scr[...] = total
            acc_scr[...] = acc
        else:
            l_scr[...] = l_scr[...] * alpha + total
            acc_scr[...] = acc_scr[...] * alpha + acc

    visit_pairs(visit, first_ref[blk], blk)

    total = l_scr[...]
    out = (acc_scr[...] / total).T
    for g in range(groups):
        o_ref[:, g * head_dim:(g + 1) * head_dim] = out[g * BLK:(g + 1) * BLK, :].astype(o_ref.dtype)
    lse_ref[0, 0] = m_scr[...] + jnp.log2(total)


def attn_fwd(q_all, k_all, v_all, pos, key_pos, first_blk, groups, head_dim):
    seq_len, q_cols = q_all.shape
    kv_heads = k_all.shape[1] // head_dim
    n_blk = seq_len // BLK
    wide = groups * BLK
    pairs = seq_len * seq_len // 4 * groups * kv_heads
    return pl.pallas_call(
        functools.partial(attn_fwd_kernel, groups, head_dim),
        grid_spec=pltpu.PrefetchScalarGridSpec(
            num_scalar_prefetch=1,
            grid=(kv_heads, n_blk),
            in_specs=[
                pl.BlockSpec((BLK, groups * head_dim), lambda h, i, first: (i, h)),
                pl.BlockSpec((seq_len, head_dim), lambda h, i, first: (0, h)),
                pl.BlockSpec((seq_len, head_dim), lambda h, i, first: (0, h)),
                pl.BlockSpec((1, BLK), lambda h, i, first: (0, i)),
                pl.BlockSpec((seq_len, LANES), lambda h, i, first: (0, 0)),
            ],
            out_specs=[
                pl.BlockSpec((BLK, groups * head_dim), lambda h, i, first: (i, h)),
                pl.BlockSpec((1, 1, 1, wide), lambda h, i, first: (h, i, 0, 0)),
            ],
            scratch_shapes=[
                pltpu.VMEM((1, wide), jnp.float32),
                pltpu.VMEM((1, wide), jnp.float32),
                pltpu.VMEM((head_dim, wide), jnp.float32),
            ],
        ),
        out_shape=[
            jax.ShapeDtypeStruct((seq_len, q_cols), jnp.bfloat16),
            jax.ShapeDtypeStruct((kv_heads, n_blk, 1, wide), jnp.float32),
        ],
        compiler_params=pltpu.CompilerParams(vmem_limit_bytes=48 * 1024 * 1024),
        cost_estimate=pl.CostEstimate(flops=8 * pairs * head_dim, bytes_accessed=8 * seq_len * q_cols, transcendentals=2 * pairs),
        name="attn_fwd",
    )(first_blk, q_all, k_all, v_all, pos, key_pos)


def attn_bwd_kernel(groups, head_dim, q_scale, first_ref, q_ref, k_ref, v_ref, o_ref, do_ref, pos_ref, key_pos_ref, lse_ref, cos_ref, sin_ref,
                    out_ref, delta_scr, dq_scr, dk_scr, dv_scr, dq_out, dk_out, dv_out, dq_sem, kv_sem):
    head, blk = pl.program_id(0), pl.program_id(1)
    n_head, n_blk = pl.num_programs(0), pl.num_programs(1)
    half = head_dim // 2
    wide = groups * BLK
    q_width = groups * head_dim
    slot = blk % 2

    @pl.when(blk == 0)
    def _():
        @pl.loop(0, n_blk)
        def _(i):
            rows = pl.ds(pl.multiple_of(i * BLK, BLK), BLK)
            dk_scr[rows, :] = jnp.zeros((BLK, head_dim), jnp.float32)
            dv_scr[rows, :] = jnp.zeros((BLK, head_dim), jnp.float32)

    q_all = stack_heads(q_ref[...], groups, head_dim)
    do_all = stack_heads(do_ref[...], groups, head_dim)
    o_all = stack_heads(o_ref[...], groups, head_dim)
    floor_row = jnp.concatenate([pos_ref[...]] * groups, axis=1) - WINDOW
    lse_row = lse_ref[0, 0]

    def visit(blocks, with_diagonal):
        if with_diagonal:
            delta = jnp.sum((do_all.astype(jnp.float32) * o_all.astype(jnp.float32)).T, axis=0, keepdims=True)
            delta_scr[...] = delta
        else:
            delta = delta_scr[...]
        rows = [pl.ds(pl.multiple_of(kb * BLK, BLK), BLK) for kb in blocks]
        k_blks = [k_ref[r, :] for r in rows]
        scores = [dot_f32(k_blk, q_all, 1, 1) for k_blk in k_blks]
        d_probs = [dot_f32(v_ref[r, :], do_all, 1, 1) for r in rows]
        dq_new = None
        for i, r in enumerate(rows):
            tanh_s = jnp.tanh(scores[i] * (1.0 / SOFT_CAP))
            keep = keep_mask(key_pos_ref[r, :], floor_row, wide, with_diagonal and i == 0)
            prob = jnp.exp2(jnp.where(keep, tanh_s * (SOFT_CAP * LOG2E) - lse_row, -1e30))
            d_score = (prob * (d_probs[i] - delta) * (1.0 - tanh_s * tanh_s)).astype(jnp.bfloat16)
            dv_scr[r, :] += jnp.dot(prob.astype(jnp.bfloat16), do_all, preferred_element_type=jnp.float32)
            dk_scr[r, :] += jnp.dot(d_score, q_all, preferred_element_type=jnp.float32)
            term = dot_f32(k_blks[i], d_score, 0, 0)
            dq_new = term if dq_new is None else dq_new + term
        if with_diagonal:
            dq_scr[...] = dq_new
        else:
            dq_scr[...] += dq_new

    visit_pairs(visit, first_ref[blk], blk)

    def dq_copy(h, i):
        dst = out_ref.at[pl.ds(pl.multiple_of(i * BLK, BLK), BLK), pl.ds(pl.multiple_of(h * q_width, q_width), q_width)]
        return pltpu.make_async_copy(dq_out.at[slot], dst, dq_sem.at[slot])

    def kv_copy(which, src, h):
        col = n_head * q_width + which * n_head * head_dim + h * head_dim
        dst = out_ref.at[:, pl.ds(pl.multiple_of(col, head_dim), head_dim)]
        return pltpu.make_async_copy(src, dst, kv_sem.at[which])

    @pl.when(head * n_blk + blk >= 2)
    def _():
        dq_copy(head, blk).wait()

    d_q = dq_scr[...].T
    rows = pl.ds(pl.multiple_of(blk * BLK, BLK), BLK)
    cos_t, sin_t = cos_ref[rows, :], sin_ref[rows, :]
    for g in range(groups):
        part = d_q[g * BLK:(g + 1) * BLK, :]
        part = (part * cos_t - pltpu.roll(part, half, 1) * sin_t) * q_scale
        dq_out[slot, :, g * head_dim:(g + 1) * head_dim] = part.astype(dq_out.dtype)
    dq_copy(head, blk).start()

    @pl.when(blk == n_blk - 1)
    def _():
        @pl.loop(0, n_blk)
        def _(i):
            rows = pl.ds(pl.multiple_of(i * BLK, BLK), BLK)
            part = dk_scr[rows, :]
            part = part * cos_ref[rows, :] - pltpu.roll(part, half, 1) * sin_ref[rows, :]
            dk_out[rows, :] = part.astype(dk_out.dtype)
            dv_out[rows, :] = dv_scr[rows, :].astype(dv_out.dtype)

        kv_copy(0, dk_out, head).start()
        kv_copy(1, dv_out, head).start()
        kv_copy(0, dk_out, head).wait()
        kv_copy(1, dv_out, head).wait()

    @pl.when((blk == n_blk - 1) & (head == n_head - 1))
    def _():
        for s in range(2):
            pltpu.make_async_copy(dq_out.at[s], out_ref.at[pl.ds(0, BLK), pl.ds(0, q_width)], dq_sem.at[s]).wait()


def attn_bwd(q_all, k_all, v_all, o_all, d_o, pos, key_pos, lse, first_blk, cos_t, sin_t, groups, head_dim):
    seq_len, q_cols = q_all.shape
    k_cols = k_all.shape[1]
    kv_heads = k_cols // head_dim
    n_blk = seq_len // BLK
    wide = groups * BLK
    pairs = seq_len * seq_len // 4 * groups * kv_heads
    by_q = pl.BlockSpec((BLK, groups * head_dim), lambda h, i, first: (i, h))
    by_h = pl.BlockSpec((seq_len, head_dim), lambda h, i, first: (0, h))
    table = pl.BlockSpec((seq_len, LANES), lambda h, i, first: (0, 0))
    return pl.pallas_call(
        functools.partial(attn_bwd_kernel, groups, head_dim, head_dim ** -0.5),
        grid_spec=pltpu.PrefetchScalarGridSpec(
            num_scalar_prefetch=1,
            grid=(kv_heads, n_blk),
            in_specs=[
                by_q, by_h, by_h, by_q, by_q,
                pl.BlockSpec((1, BLK), lambda h, i, first: (0, i)),
                table,
                pl.BlockSpec((1, 1, 1, wide), lambda h, i, first: (h, i, 0, 0)),
                table, table,
            ],
            out_specs=pl.BlockSpec(memory_space=pl.ANY),
            scratch_shapes=[
                pltpu.VMEM((1, wide), jnp.float32),
                pltpu.VMEM((head_dim, wide), jnp.float32),
                pltpu.VMEM((seq_len, head_dim), jnp.float32),
                pltpu.VMEM((seq_len, head_dim), jnp.float32),
                pltpu.VMEM((2, BLK, groups * head_dim), jnp.bfloat16),
                pltpu.VMEM((seq_len, head_dim), jnp.bfloat16),
                pltpu.VMEM((seq_len, head_dim), jnp.bfloat16),
                pltpu.SemaphoreType.DMA((2,)),
                pltpu.SemaphoreType.DMA((2,)),
            ],
        ),
        out_shape=jax.ShapeDtypeStruct((seq_len, q_cols + 2 * k_cols), jnp.bfloat16),
        compiler_params=pltpu.CompilerParams(vmem_limit_bytes=48 * 1024 * 1024),
        cost_estimate=pl.CostEstimate(flops=20 * pairs * head_dim, bytes_accessed=16 * seq_len * q_cols, transcendentals=2 * pairs),
        name="attn_bwd",
    )(first_blk, q_all, k_all, v_all, o_all, d_o, pos, key_pos, lse, cos_t, sin_t)


SEQ_ORDER = (1, 2, 0)
GW_ORDER = (1, 0, 2)
GWO_ORDER = (2, 1, 0)


def solution(mesh):
    act_spec = P('dp', 'tp', None)
    head_spec = P(None, 'tp', None)
    grad_spec = P('dp', 'tp', None)
    in_specs = (act_spec, P('dp', 'tp'), act_spec, head_spec, head_spec, head_spec, P('tp', None, None), P(None), P(None))
    out_specs = (act_spec, act_spec, grad_spec, grad_spec, grad_spec, P(('dp', 'tp'), None, None), P('dp'), P('dp'))

    def local_body(x_in, positions, grad_out, w_query, w_key, w_value, w_out, gain_pre, gain_post):
        _, _, depth = x_in.shape
        n_dev = mesh.shape['tp']
        heads_loc, head_dim = w_query.shape[1], w_query.shape[2]
        kv_loc = w_key.shape[1]
        groups = heads_loc // kv_loc
        q_cols, k_cols = heads_loc * head_dim, kv_loc * head_dim

        gain_pre_row, gain_post_row = gain_pre[None, :], gain_post[None, :]
        rows = x_in.shape[1]

        def swap(value, bit):
            return lax.ppermute(value, 'tp', [(d, d ^ bit) for d in range(n_dev)])

        def near_of(value):
            return {bit: swap(value, bit) for bit in (1, 2, 4)}

        def pieces_of(value, near):
            mid = value.shape[0] // 2
            far = (swap(near[2][:mid], 4), swap(near[4][mid:], 2))
            other_core = [swap(near[2], 1), swap(near[4], 1)]
            far_other = [swap(part, 1) for part in far]
            return (value, near[1], near[2], near[4], *other_core, *far, *far_other)

        pos_all = lax.all_gather(positions, 'tp', axis=1, tiled=True)
        w_out_loc, x_held, pos_all = lax.optimization_barrier((w_out.reshape(q_cols, depth), x_in, pos_all))
        own, near = {'wo': w_out_loc}, {'wo': near_of(w_out_loc)}
        for b in SEQ_ORDER:
            own[b] = pre_norm(x_held, gain_pre_row, b, 1)
            near[b] = near_of(own[b])

        seq_len = pos_all.shape[1]
        half = head_dim // 2
        inv_freq = ROPE_THETA ** (-2.0 * jnp.arange(half, dtype=jnp.float32) / head_dim)
        before = pos_all[:, None, :] <= pos_all[:, ::BLK, None] - WINDOW
        first_blk = jnp.sum(before.astype(jnp.int32), axis=-1) // BLK
        w_all = jnp.concatenate([w_query.reshape(depth, q_cols), w_key.reshape(depth, k_cols), w_value.reshape(depth, k_cols)], axis=1)
        w_t = w_all.T
        tables = {}
        for b in SEQ_ORDER:
            angles = pos_all[b].astype(jnp.float32)[:, None] * inv_freq
            cos_h, sin_h = jnp.cos(angles), jnp.sin(angles)
            tables[b] = (jnp.concatenate([cos_h, cos_h], axis=-1), jnp.concatenate([-sin_h, sin_h], axis=-1))
        near[SEQ_ORDER[0]], w_all, w_t, tables, first_blk = lax.optimization_barrier((near[SEQ_ORDER[0]], w_all, w_t, tables, first_blk))
        w_out_pieces = pieces_of(own['wo'], near['wo'])
        normed = {b: pieces_of(own[b], near[b]) for b in SEQ_ORDER}

        me = lax.axis_index('tp')[None]
        devices = me ^ jnp.array(PIECE_DEVICES, jnp.int32)
        gathered = {}

        saved, d_proj_all = {}, {}
        y_out, d_post = None, jnp.zeros((1, depth), jnp.float32)
        for b in SEQ_ORDER:
            cos_t, sin_t = tables[b]
            pos_b = pos_all[b][None, :]
            key_pos = jnp.broadcast_to(pos_all[b][:, None], (seq_len, LANES))
            q_b, k_b, v_b, whole = qkv_project(devices, normed[b], w_all, cos_t, sin_t, q_cols, k_cols, head_dim)
            gathered[b] = (whole, 0)
            o_b, lse_b = attn_fwd(q_b, k_b, v_b, pos_b, key_pos, first_blk[b], groups, head_dim)
            o_mine = lax.all_to_all(o_b.reshape(n_dev, rows, q_cols), 'tp', split_axis=0, concat_axis=0, tiled=True)
            proj = out_proj(me, o_mine, w_out_pieces)
            y_out, d_proj, d_post = post_norm(proj, x_in, grad_out, gain_post_row, d_post, y_out, b)
            d_proj_all[b] = lax.all_gather(d_proj, 'tp', axis=0, tiled=True)
            saved[b] = (q_b, k_b, v_b, o_b, pos_b, key_pos, lse_b, cos_t, sin_t)

        grad_x, d_pre = None, jnp.zeros((1, depth), jnp.float32)
        d_lin = {}
        for b in SEQ_ORDER:
            q_b, k_b, v_b, o_b, pos_b, key_pos, lse_b, cos_t, sin_t = saved[b]
            d_o = dot_f32(d_proj_all[b], w_out_loc, 1, 1).astype(jnp.bfloat16)
            d_lin[b] = attn_bwd(q_b, k_b, v_b, o_b, d_o, pos_b, key_pos, lse_b, first_blk[b], cos_t, sin_t, groups, head_dim)
            pair = grad_normed_pair(me ^ 1, d_lin[b], w_t, rows)
            from_pair = swap(pair, 1)
            send_x, keep_x, send_y, keep_y = grad_normed_own(me, d_lin[b], w_t, from_pair)
            near_x = swap(send_x, 2)
            near_y = swap(send_y, 4)
            fold_x, fold_y = fold(keep_x, near_x, keep_y, near_y)
            far_x = swap(fold_x, 4)
            far_y = swap(fold_y, 2)
            grad_x, d_pre = pre_grad((keep_x, near_x, far_x, keep_y, near_y, far_y), x_in, grad_out, gain_pre_row, d_pre, grad_x, b)
        grad_wo = None
        for b in GWO_ORDER:
            grad_wo = grad_wo_sum(saved[b][3], d_proj_all[b], grad_wo)
        grads = None
        for b in GW_ORDER:
            grads = grad_w(*gathered[b], rows, d_lin[b], (heads_loc, kv_loc, kv_loc), head_dim, grads, b == GW_ORDER[-1])
        grad_wq, grad_wk, grad_wv = grads
        grad_pre, grad_post = gain_sum(d_pre, d_post, n_dev)
        grad_pre, grad_post = grad_pre[0], grad_post[0]
        return y_out, grad_x, grad_wq, grad_wk, grad_wv, grad_wo.reshape(w_out.shape), grad_pre, grad_post

    return jax.shard_map(local_body, mesh=mesh, in_specs=in_specs, out_specs=out_specs, check_vma=False)
```

```python
import functools

import jax
import jax.numpy as jnp
from jax import lax
from jax.experimental import pallas as pl
from jax.experimental.pallas import tpu as pltpu
from jax.sharding import PartitionSpec as P


WINDOW = 4096
SOFT_CAP = 50.0
NORM_EPS = 1e-6
ROPE_THETA = 10000.0
LOG2E = 1.4426950408889634
BLK = 256
LANES = 128


def dot_f32(lhs, rhs, lhs_dim, rhs_dim):
    return lax.dot_general(lhs, rhs, (((lhs_dim,), (rhs_dim,)), ((), ())), preferred_element_type=jnp.float32)


ROWS = 64
CHUNK = 16


def row_specs(seq, depth):
    whole = pl.BlockSpec((1, ROWS, depth), lambda i: (seq, i, 0))
    one = pl.BlockSpec((ROWS, depth), lambda i: (i, 0))
    vec = pl.BlockSpec((1, depth), lambda i: (0, 0))
    return whole, one, vec


def inverse_rms(values):
    return lax.rsqrt(jnp.mean(values * values, axis=-1, keepdims=True) + NORM_EPS)


def norm_grad(values, inv, d_out, gain):
    scaled = d_out * gain
    dot = jnp.mean(scaled * values, axis=-1, keepdims=True)
    return scaled * inv - values * (inv * inv * inv * dot)


def fold_rows(block):
    return sum(block[r:r + 8] for r in range(0, CHUNK, 8))


def pre_norm_kernel(x_ref, gain_ref, n_ref):
    gain = 1.0 + gain_ref[...]

    @pl.loop(0, ROWS // CHUNK)
    def _(c):
        rows = pl.ds(pl.multiple_of(c * CHUNK, CHUNK), CHUNK)
        values = x_ref[0, rows, :].astype(jnp.float32)
        n_ref[rows, :] = (values * inverse_rms(values) * gain).astype(n_ref.dtype)


def pre_norm(x_in, gain, first_seq, count):
    _, rows, depth = x_in.shape
    steps = rows // ROWS
    return pl.pallas_call(
        pre_norm_kernel,
        grid=(count, steps),
        in_specs=[pl.BlockSpec((1, ROWS, depth), lambda s, i: (first_seq + s, i, 0)), pl.BlockSpec((1, depth), lambda s, i: (0, 0))],
        out_specs=pl.BlockSpec((ROWS, depth), lambda s, i: (s * steps + i, 0)),
        out_shape=jax.ShapeDtypeStruct((count * rows, depth), jnp.bfloat16),
        compiler_params=pltpu.CompilerParams(vmem_limit_bytes=54 * 1024 * 1024),
        cost_estimate=pl.CostEstimate(flops=count * rows * depth * 400, bytes_accessed=4 * count * rows * depth, transcendentals=count * rows),
        name="pre_norm",
    )(x_in, gain)


def post_norm_kernel(first, proj_ref, x_ref, go_ref, gain_ref, dg_in_ref, *refs):
    y_ref, d_proj_ref, dg_ref, dg_scr = refs[0 if first else 1:]
    step = pl.program_id(0)
    gain = 1.0 + gain_ref[...]

    @pl.when(step == 0)
    def _():
        dg_scr[...] = jnp.zeros_like(dg_scr)

    @pl.loop(0, ROWS // CHUNK)
    def _(c):
        rows = pl.ds(pl.multiple_of(c * CHUNK, CHUNK), CHUNK)
        values = proj_ref[rows, :].astype(jnp.float32)
        inv = inverse_rms(values)
        unit = values * inv
        post = (unit * gain).astype(jnp.bfloat16).astype(jnp.float32)
        y_ref[0, rows, :] = (x_ref[0, rows, :].astype(jnp.float32) + post).astype(y_ref.dtype)
        d_out = go_ref[0, rows, :].astype(jnp.float32)
        dg_scr[...] += fold_rows(d_out * unit)
        d_proj_ref[rows, :] = norm_grad(values, inv, d_out, gain).astype(d_proj_ref.dtype)

    @pl.when(step == pl.num_programs(0) - 1)
    def _():
        dg_ref[...] = dg_in_ref[...] + jnp.sum(dg_scr[...], axis=0, keepdims=True)


def post_norm(proj, x_in, grad_out, gain, dg_in, y_prev, seq):
    _, rows, depth = x_in.shape
    whole, one, vec = row_specs(seq, depth)
    first = y_prev is None
    return pl.pallas_call(
        functools.partial(post_norm_kernel, first),
        grid=(rows // ROWS,),
        in_specs=[one, whole, whole, vec, vec] + ([] if first else [pl.BlockSpec(memory_space=pl.ANY)]),
        out_specs=[whole, one, vec],
        out_shape=[
            jax.ShapeDtypeStruct(x_in.shape, jnp.bfloat16),
            jax.ShapeDtypeStruct((rows, depth), jnp.bfloat16),
            jax.ShapeDtypeStruct((1, depth), jnp.float32),
        ],
        scratch_shapes=[pltpu.VMEM((8, depth), jnp.float32)],
        input_output_aliases={} if first else {5: 0},
        compiler_params=pltpu.CompilerParams(vmem_limit_bytes=54 * 1024 * 1024),
        cost_estimate=pl.CostEstimate(flops=rows * depth * 800, bytes_accessed=10 * rows * depth, transcendentals=rows),
        name="post_norm",
    )(proj, x_in, grad_out, gain, dg_in, *([] if first else [y_prev]))


def pre_grad_kernel(first, *refs):
    pieces, (x_ref, go_ref, gain_ref, dg_in_ref), refs = refs[:6], refs[6:10], refs[10:]
    gx_ref, dg_ref, dg_scr = refs[0 if first else 1:]
    step = pl.program_id(0)
    gain = 1.0 + gain_ref[...]

    @pl.when(step == 0)
    def _():
        dg_scr[...] = jnp.zeros_like(dg_scr)

    @pl.loop(0, ROWS // CHUNK)
    def _(c):
        rows = pl.ds(pl.multiple_of(c * CHUNK, CHUNK), CHUNK)
        values = x_ref[0, rows, :].astype(jnp.float32)
        inv = inverse_rms(values)
        halves = []
        for kept, near, far in (pieces[:3], pieces[3:]):
            halves.append(kept[0, rows, :].astype(jnp.float32) + near[0, rows, :].astype(jnp.float32) + far[rows, :].astype(jnp.float32))
        d_out = jnp.concatenate(halves, axis=1)
        dg_scr[...] += fold_rows(d_out * (values * inv))
        d_x = norm_grad(values, inv, d_out, gain).astype(jnp.bfloat16).astype(jnp.float32)
        gx_ref[0, rows, :] = (go_ref[0, rows, :].astype(jnp.float32) + d_x).astype(gx_ref.dtype)

    @pl.when(step == pl.num_programs(0) - 1)
    def _():
        dg_ref[...] = dg_in_ref[...] + jnp.sum(dg_scr[...], axis=0, keepdims=True)


def pre_grad(pieces, x_in, grad_out, gain, dg_in, gx_prev, seq):
    _, rows, depth = x_in.shape
    whole, _, vec = row_specs(seq, depth)
    pair = pl.BlockSpec((1, ROWS, depth // 2), lambda i: (0, i, 0))
    one = pl.BlockSpec((ROWS, depth // 2), lambda i: (i, 0))
    first = gx_prev is None
    return pl.pallas_call(
        functools.partial(pre_grad_kernel, first),
        grid=(rows // ROWS,),
        in_specs=[pair, pair, one, pair, pair, one, whole, whole, vec, vec] + ([] if first else [pl.BlockSpec(memory_space=pl.ANY)]),
        out_specs=[whole, vec],
        out_shape=[jax.ShapeDtypeStruct(x_in.shape, jnp.bfloat16), jax.ShapeDtypeStruct((1, depth), jnp.float32)],
        scratch_shapes=[pltpu.VMEM((8, depth), jnp.float32)],
        input_output_aliases={} if first else {10: 0},
        compiler_params=pltpu.CompilerParams(vmem_limit_bytes=54 * 1024 * 1024),
        cost_estimate=pl.CostEstimate(flops=rows * depth * 700, bytes_accessed=12 * rows * depth, transcendentals=rows),
        name="pre_grad",
    )(*pieces, x_in, grad_out, gain, dg_in, *([] if first else [gx_prev]))


def out_proj_kernel(me_ref, o_ref, *refs):
    pieces, r_ref = refs[:-1], refs[-1]
    o_all = jnp.concatenate([o_ref[me_ref[0] ^ k] for k in PIECE_DEVICES], axis=1)
    w_all = jnp.concatenate([piece[...] for piece in pieces], axis=0)
    r_ref[...] = jnp.dot(o_all, w_all, preferred_element_type=jnp.float32).astype(r_ref.dtype)


def out_proj(me, o_mine, pieces):
    n_dev, rows, cols = o_mine.shape
    depth = pieces[0].shape[1]
    tile = 768
    return pl.pallas_call(
        out_proj_kernel,
        grid_spec=pltpu.PrefetchScalarGridSpec(
            num_scalar_prefetch=1,
            grid=(depth // tile,),
            in_specs=[pl.BlockSpec((n_dev, rows, cols), lambda i, me: (0, 0, 0), pipeline_mode=pl.Buffered(1))]
            + [pl.BlockSpec((piece.shape[0], tile), lambda i, me: (0, i)) for piece in pieces],
            out_specs=pl.BlockSpec((rows, tile), lambda i, me: (0, i)),
        ),
        out_shape=jax.ShapeDtypeStruct((rows, depth), jnp.bfloat16),
        compiler_params=pltpu.CompilerParams(vmem_limit_bytes=40 * 1024 * 1024),
        cost_estimate=pl.CostEstimate(flops=2 * n_dev * rows * cols * depth, bytes_accessed=2 * n_dev * cols * depth, transcendentals=0),
        name="out_proj",
    )(me, o_mine, *pieces)


PIECE_DEVICES = (0, 1, 2, 4, 3, 5, 6, 7)


PIECE = 1024


def for_columns(width, visit):
    @pl.loop(0, width // PIECE)
    def _(c):
        visit(pl.ds(pl.multiple_of(c * PIECE, PIECE), PIECE))

    if width % PIECE:
        visit(pl.ds(width // PIECE * PIECE, width % PIECE))


def pair_core_kernel(dst_ref, d0_ref, d1_ref, w_ref, out_ref):
    rows = d0_ref.shape[0]
    d_two = jnp.concatenate([d0_ref[...], d1_ref[...]], axis=0)

    def visit(cols):
        value = jnp.dot(d_two, w_ref[:, cols], preferred_element_type=jnp.float32).astype(out_ref.dtype)
        out_ref[0, :, cols] = value[:rows]
        out_ref[1, :, cols] = value[rows:]

    for_columns(w_ref.shape[1], visit)


def grad_normed_pair(dst, d_lin, w_t, rows):
    cols, depth = w_t.shape
    half = depth // 2
    return pl.pallas_call(
        pair_core_kernel,
        grid_spec=pltpu.PrefetchScalarGridSpec(
            num_scalar_prefetch=1,
            grid=(2, 2),
            in_specs=[
                pl.BlockSpec((rows, cols), lambda h, p, dst: (dst[0] ^ (4 * p), 0)),
                pl.BlockSpec((rows, cols), lambda h, p, dst: (dst[0] ^ (4 * p + 2), 0)),
                pl.BlockSpec((cols, half), lambda h, p, dst: (0, h)),
            ],
            out_specs=pl.BlockSpec((2, rows, half), lambda h, p, dst: (p, 0, h)),
        ),
        out_shape=jax.ShapeDtypeStruct((4, rows, depth), jnp.bfloat16),
        compiler_params=pltpu.CompilerParams(vmem_limit_bytes=54 * 1024 * 1024),
        cost_estimate=pl.CostEstimate(flops=8 * rows * cols * depth, bytes_accessed=2 * (4 * rows * depth + cols * depth), transcendentals=0),
        name="grad_normed_pair",
    )(dst, d_lin, d_lin, w_t)


def route(h, j):
    return jnp.where(h == 0, (2 * j + 1) % 5, (j + 2) % 4)


def own_core_kernel(dst_ref, d0_ref, d1_ref, w_ref, add0_ref, add1_ref, *refs):
    outs, (stage, sem) = refs[:4], refs[4:]
    rows = d0_ref.shape[0]
    step = 2 * pl.program_id(0) + pl.program_id(1)
    slot = step % 2
    d_two = jnp.concatenate([d0_ref[...], d1_ref[...]], axis=0)

    def copy_out(out):
        return pltpu.make_async_copy(stage.at[slot], out, sem.at[slot])

    @pl.when(step >= 2)
    def _():
        copy_out(outs[0]).wait()

    def visit(cols):
        value = jnp.dot(d_two, w_ref[:, cols], preferred_element_type=jnp.float32)
        stage[slot, 0, :, cols] = (value[:rows] + add0_ref[0, :, cols].astype(jnp.float32)).astype(stage.dtype)
        stage[slot, 1, :, cols] = (value[rows:] + add1_ref[0, :, cols].astype(jnp.float32)).astype(stage.dtype)

    for_columns(w_ref.shape[1], visit)
    for i, out in enumerate(outs):
        @pl.when(step == i)
        def _(out=out):
            copy_out(out).start()

    @pl.when(step == 3)
    def _():
        for s in range(2):
            pltpu.make_async_copy(stage.at[s], outs[0], sem.at[s]).wait()


def grad_normed_own(dst, d_lin, w_t, from_pair):
    _, rows, depth = from_pair.shape
    cols = w_t.shape[0]
    half = depth // 2
    return pl.pallas_call(
        own_core_kernel,
        grid_spec=pltpu.PrefetchScalarGridSpec(
            num_scalar_prefetch=1,
            grid=(2, 2),
            in_specs=[
                pl.BlockSpec((rows, cols), lambda h, p, dst: (dst[0] ^ (2 * route(h, 2 * p)), 0)),
                pl.BlockSpec((rows, cols), lambda h, p, dst: (dst[0] ^ (2 * route(h, 2 * p + 1)), 0)),
                pl.BlockSpec((cols, half), lambda h, p, dst: (0, h)),
                pl.BlockSpec((1, rows, half), lambda h, p, dst: (route(h, 2 * p), 0, h)),
                pl.BlockSpec((1, rows, half), lambda h, p, dst: (route(h, 2 * p + 1), 0, h)),
            ],
            out_specs=[pl.BlockSpec(memory_space=pl.ANY)] * 4,
            scratch_shapes=[pltpu.VMEM((2, 2, rows, half), jnp.bfloat16), pltpu.SemaphoreType.DMA((2,))],
        ),
        out_shape=[jax.ShapeDtypeStruct((2, rows, half), jnp.bfloat16)] * 4,
        compiler_params=pltpu.CompilerParams(vmem_limit_bytes=56 * 1024 * 1024),
        cost_estimate=pl.CostEstimate(flops=8 * rows * cols * depth, bytes_accessed=2 * (8 * rows * depth + cols * depth), transcendentals=0),
        name="grad_normed_own",
    )(dst, d_lin, d_lin, w_t, from_pair, from_pair)


def fold_kernel(keep_x_ref, near_x_ref, keep_y_ref, near_y_ref, x_ref, y_ref):
    for out, kept, near in ((x_ref, keep_x_ref, near_x_ref), (y_ref, keep_y_ref, near_y_ref)):
        out[...] = (kept[0].astype(jnp.float32) + near[0].astype(jnp.float32)).astype(out.dtype)


def fold(keep_x, near_x, keep_y, near_y):
    _, rows, half = keep_x.shape
    tile = 96
    second = pl.BlockSpec((1, tile, half), lambda i: (1, i, 0))
    out = pl.BlockSpec((tile, half), lambda i: (i, 0))
    return pl.pallas_call(
        fold_kernel,
        grid=(rows // tile,),
        in_specs=[second] * 4,
        out_specs=[out, out],
        out_shape=[jax.ShapeDtypeStruct((rows, half), jnp.bfloat16)] * 2,
        compiler_params=pltpu.CompilerParams(vmem_limit_bytes=54 * 1024 * 1024),
        cost_estimate=pl.CostEstimate(flops=rows * half * 800, bytes_accessed=12 * rows * half, transcendentals=0),
        name="fold",
    )(keep_x, near_x, keep_y, near_y)


def gain_sum_kernel(n_dev, pre_ref, post_ref, pre_out, post_out, slots, local_sem, send_sem, recv_sem):
    me = lax.axis_index('tp')
    sources = (pre_ref, post_ref)
    sends, locals_ = [], []
    for off in range(1, n_dev):
        for which, src in enumerate(sources):
            copy = pltpu.make_async_remote_copy(
                src_ref=src, dst_ref=slots.at[which, me], send_sem=send_sem.at[which, off], recv_sem=recv_sem.at[which, me],
                device_id={'tp': lax.rem(me + off, n_dev)}, device_id_type=pl.DeviceIdType.MESH)
            copy.start()
            sends.append(copy)
    for which, src in enumerate(sources):
        copy = pltpu.make_async_copy(src, slots.at[which, me], local_sem.at[which])
        copy.start()
        locals_.append(copy)
    for copy in locals_:
        copy.wait()
    for off in range(1, n_dev):
        other = lax.rem(me + off, n_dev)
        for which, src in enumerate(sources):
            pltpu.make_async_remote_copy(
                src_ref=src, dst_ref=slots.at[which, other], send_sem=send_sem.at[which, off], recv_sem=recv_sem.at[which, other],
                device_id={'tp': other}, device_id_type=pl.DeviceIdType.MESH).wait_recv()
    for copy in sends:
        copy.wait_send()
    for which, out in enumerate((pre_out, post_out)):
        total = slots[which, 0]
        for d in range(1, n_dev):
            total = total + slots[which, d]
        out[...] = total


def gain_sum(d_pre, d_post, n_dev):
    depth = d_pre.shape[1]
    vmem = pl.BlockSpec(memory_space=pltpu.VMEM)
    return pl.pallas_call(
        functools.partial(gain_sum_kernel, n_dev),
        in_specs=[vmem, vmem],
        out_specs=[vmem, vmem],
        out_shape=[jax.ShapeDtypeStruct((1, depth), jnp.float32)] * 2,
        scratch_shapes=[
            pltpu.VMEM((2, n_dev, 1, depth), jnp.float32),
            pltpu.SemaphoreType.DMA((2,)),
            pltpu.SemaphoreType.DMA((2, n_dev)),
            pltpu.SemaphoreType.DMA((2, n_dev)),
        ],
        compiler_params=pltpu.CompilerParams(has_side_effects=True),
        name="gain_sum",
    )(d_pre, d_post)


def grad_w_kernel(has_prev, split, head_dim, a_ref, d_ref, *refs):
    outs = refs[1:] if has_prev else refs
    n_dev, rows, tile = a_ref.shape
    step = 256

    @pl.loop(0, tile // step)
    def _(m):
        cols = pl.ds(pl.multiple_of(m * step, step), step)
        total = dot_f32(a_ref[:, :, cols].reshape(n_dev * rows, step), d_ref[...], 0, 0)
        if has_prev:
            total = total + refs[0][cols, :]
        if not split:
            outs[0][cols, :] = total
            return
        col = 0
        for out in outs:
            heads = out.shape[1]
            out[cols] = total[:, col:col + heads * head_dim].reshape(step, heads, head_dim)
            col += heads * head_dim


def grad_w(gathered, slot, rows, d_lin, heads, head_dim, prev, last):
    n_dev, _, depth = gathered.shape
    seq_len, cols = d_lin.shape
    tile = 768
    flat = pl.BlockSpec((tile, cols), lambda i: (i, 0))
    has_prev = prev is not None
    if last:
        out_specs = [pl.BlockSpec((tile, h, head_dim), lambda i: (i, 0, 0)) for h in heads]
        out_shape = [jax.ShapeDtypeStruct((depth, h, head_dim), jnp.float32) for h in heads]
    else:
        out_specs, out_shape = flat, jax.ShapeDtypeStruct((depth, cols), jnp.float32)
    return pl.pallas_call(
        functools.partial(grad_w_kernel, has_prev, last, head_dim),
        grid=(depth // tile,),
        in_specs=[
            pl.BlockSpec((n_dev, rows, tile), lambda i: (0, slot, i)),
            pl.BlockSpec((seq_len, cols), lambda i: (0, 0), pipeline_mode=pl.Buffered(1)),
        ] + ([flat] if has_prev else []),
        out_specs=out_specs,
        out_shape=out_shape,
        input_output_aliases={2: 0} if has_prev and not last else {},
        compiler_params=pltpu.CompilerParams(vmem_limit_bytes=58 * 1024 * 1024),
        cost_estimate=pl.CostEstimate(flops=2 * seq_len * depth * cols, bytes_accessed=2 * seq_len * (depth + cols) + 8 * depth * cols, transcendentals=0),
        name="grad_w",
    )(gathered, d_lin, *([prev] if has_prev else []))


def grad_wo_kernel(has_prev, o_ref, d_ref, *refs):
    out = refs[-1]
    total = dot_f32(o_ref[...], d_ref[...], 0, 0)
    out[...] = total + refs[0][...] if has_prev else total


def grad_wo_sum(o_all, d_proj, prev):
    seq_len, cols = o_all.shape
    depth = d_proj.shape[1]
    tile = 768
    has_prev = prev is not None
    flat = pl.BlockSpec((cols, tile), lambda i: (0, i))
    return pl.pallas_call(
        functools.partial(grad_wo_kernel, has_prev),
        grid=(depth // tile,),
        in_specs=[
            pl.BlockSpec((seq_len, cols), lambda i: (0, 0), pipeline_mode=pl.Buffered(1)),
            pl.BlockSpec((seq_len, tile), lambda i: (0, i)),
        ] + ([flat] if has_prev else []),
        out_specs=flat,
        out_shape=jax.ShapeDtypeStruct((cols, depth), jnp.float32),
        input_output_aliases={2: 0} if has_prev else {},
        compiler_params=pltpu.CompilerParams(vmem_limit_bytes=54 * 1024 * 1024),
        cost_estimate=pl.CostEstimate(flops=2 * seq_len * depth * cols, bytes_accessed=2 * seq_len * (depth + cols) + 8 * depth * cols, transcendentals=0),
        name="grad_wo",
    )(o_all, d_proj, *([prev] if has_prev else []))


def qkv_kernel(q_cols, k_cols, head_dim, q_scale, dev_ref, *refs):
    pieces, (w_hbm, cos_ref, sin_ref, q_ref, k_ref, v_ref, whole_ref, buf, w_ref, in_sem, out_sem, w_sem) = refs[:-12], refs[-12:]
    n_slot, rows, _ = buf.shape
    groups, taken = [], []
    for piece in pieces:
        taken.append(piece)
        if sum(part.shape[0] for part in taken) == rows:
            groups.append(taken)
            taken = []

    def start_in(p):
        slot = p % n_slot
        for i, group in enumerate(groups):
            @pl.when(p == i)
            def _(group=group):
                row = 0
                for part in group:
                    pltpu.make_async_copy(part, buf.at[slot, pl.ds(row, part.shape[0])], in_sem.at[slot]).start()
                    row += part.shape[0]

    def out_copy(p):
        slot = p % n_slot
        return pltpu.make_async_copy(buf.at[slot], whole_ref.at[dev_ref[p]], out_sem.at[slot])

    w_copy = pltpu.make_async_copy(w_hbm, w_ref, w_sem)
    start_in(0)
    w_copy.start()

    @pl.loop(0, len(groups))
    def _(p):
        slot = p % n_slot
        pltpu.make_async_copy(pieces[0], buf.at[slot], in_sem.at[slot]).wait()
        out_copy(p).start()

        @pl.when(p + 1 < len(groups))
        def _():
            @pl.when(p + 1 >= n_slot)
            def _():
                out_copy(p + 1 - n_slot).wait()

            start_in(p + 1)

        @pl.when(p == 0)
        def _():
            w_copy.wait()

        here = pl.ds(pl.multiple_of(dev_ref[p] * rows, rows), rows)
        lin = jnp.dot(buf[slot], w_ref[...], preferred_element_type=jnp.float32)
        cos_t, sin_t = cos_ref[here, :], sin_ref[here, :]
        for h in range((q_cols + k_cols) // head_dim):
            col = h * head_dim
            part = lin[:, col:col + head_dim]
            part = part * cos_t + pltpu.roll(part, head_dim // 2, 1) * sin_t
            if col < q_cols:
                q_ref[here, col:col + head_dim] = (part * q_scale).astype(q_ref.dtype)
            else:
                k_ref[here, col - q_cols:col - q_cols + head_dim] = part.astype(k_ref.dtype)
        v_ref[here, :] = lin[:, q_cols + k_cols:].astype(v_ref.dtype)

    for p in range(len(groups) - n_slot, len(groups)):
        out_copy(p).wait()


def qkv_project(devices, pieces, w_all, cos_t, sin_t, q_cols, k_cols, head_dim):
    rows, depth = pieces[0].shape
    cols = w_all.shape[1]
    seq_len = cos_t.shape[0]
    n_dev = seq_len // rows
    widths = (q_cols, k_cols, cols - q_cols - k_cols)
    hbm, vmem = pl.BlockSpec(memory_space=pl.ANY), pl.BlockSpec(memory_space=pltpu.VMEM)
    return pl.pallas_call(
        functools.partial(qkv_kernel, q_cols, k_cols, head_dim, head_dim ** -0.5),
        in_specs=[pl.BlockSpec(memory_space=pltpu.SMEM)] + [hbm] * (len(pieces) + 1) + [vmem] * 2,
        out_specs=[vmem] * 3 + [hbm],
        out_shape=[jax.ShapeDtypeStruct((seq_len, width), jnp.bfloat16) for width in widths]
        + [jax.ShapeDtypeStruct((n_dev, rows, depth), jnp.bfloat16)],
        scratch_shapes=[
            pltpu.VMEM((3, rows, depth), jnp.bfloat16),
            pltpu.VMEM((depth, cols), jnp.bfloat16),
            pltpu.SemaphoreType.DMA((3,)),
            pltpu.SemaphoreType.DMA((3,)),
            pltpu.SemaphoreType.DMA,
        ],
        compiler_params=pltpu.CompilerParams(vmem_limit_bytes=56 * 1024 * 1024),
        cost_estimate=pl.CostEstimate(flops=2 * seq_len * depth * cols, bytes_accessed=2 * (2 * seq_len * depth + depth * cols + seq_len * cols), transcendentals=0),
        name="qkv_project",
    )(devices, *pieces, w_all, cos_t, sin_t)


def stack_heads(block, groups, head_dim):
    return jnp.concatenate([block[:, g * head_dim:(g + 1) * head_dim] for g in range(groups)], axis=0)


def keep_mask(key_pos, floor_row, wide, diagonal):
    keep = jnp.concatenate([key_pos] * (wide // LANES), axis=1) > floor_row
    if diagonal:
        key_idx = lax.broadcasted_iota(jnp.int32, (BLK, wide), 0)
        q_idx = lax.broadcasted_iota(jnp.int32, (BLK, wide), 1) % BLK
        keep = keep & (key_idx <= q_idx)
    return keep


def visit_pairs(visit, first, blk):
    odd = (blk - first) % 2

    @pl.when(odd == 0)
    def _():
        visit([blk], True)

    @pl.when(odd == 1)
    def _():
        visit([blk, blk - 1], True)

    @pl.loop(0, (blk - first) // 2)
    def _(i):
        visit([first + 2 * i, first + 2 * i + 1], False)


def attn_fwd_kernel(groups, head_dim, first_ref, q_ref, k_ref, v_ref, pos_ref, key_pos_ref, o_ref, lse_ref, m_scr, l_scr, acc_scr):
    blk = pl.program_id(1)
    q_all = stack_heads(q_ref[...], groups, head_dim)
    floor_row = jnp.concatenate([pos_ref[...]] * groups, axis=1) - WINDOW
    wide = groups * BLK

    def visit(blocks, with_diagonal):
        rows = [pl.ds(pl.multiple_of(kb * BLK, BLK), BLK) for kb in blocks]
        scores = [dot_f32(k_ref[r, :], q_all, 1, 1) for r in rows]
        capped = []
        for i, r in enumerate(rows):
            keep = keep_mask(key_pos_ref[r, :], floor_row, wide, with_diagonal and i == 0)
            capped.append(jnp.where(keep, jnp.tanh(scores[i] * (1.0 / SOFT_CAP)) * (SOFT_CAP * LOG2E), -1e30))
        top = functools.reduce(jnp.maximum, [jnp.max(c, axis=0, keepdims=True) for c in capped])
        if not with_diagonal:
            m_old = m_scr[...]
            top = jnp.maximum(m_old, top)
            alpha = jnp.exp2(m_old - top)
        m_scr[...] = top
        probs = [jnp.exp2(c - top) for c in capped]
        total = sum(jnp.sum(p, axis=0, keepdims=True) for p in probs)
        acc = sum(dot_f32(v_ref[r, :], p.astype(jnp.bfloat16), 0, 0) for r, p in zip(rows, probs))
        if with_diagonal:
            l_scr[...] = total
            acc_scr[...] = acc
        else:
            l_scr[...] = l_scr[...] * alpha + total
            acc_scr[...] = acc_scr[...] * alpha + acc

    visit_pairs(visit, first_ref[blk], blk)

    total = l_scr[...]
    out = (acc_scr[...] / total).T
    for g in range(groups):
        o_ref[:, g * head_dim:(g + 1) * head_dim] = out[g * BLK:(g + 1) * BLK, :].astype(o_ref.dtype)
    lse_ref[0, 0] = m_scr[...] + jnp.log2(total)


def attn_fwd(q_all, k_all, v_all, pos, key_pos, first_blk, groups, head_dim):
    seq_len, q_cols = q_all.shape
    kv_heads = k_all.shape[1] // head_dim
    n_blk = seq_len // BLK
    wide = groups * BLK
    pairs = seq_len * seq_len // 4 * groups * kv_heads
    return pl.pallas_call(
        functools.partial(attn_fwd_kernel, groups, head_dim),
        grid_spec=pltpu.PrefetchScalarGridSpec(
            num_scalar_prefetch=1,
            grid=(kv_heads, n_blk),
            in_specs=[
                pl.BlockSpec((BLK, groups * head_dim), lambda h, i, first: (i, h)),
                pl.BlockSpec((seq_len, head_dim), lambda h, i, first: (0, h)),
                pl.BlockSpec((seq_len, head_dim), lambda h, i, first: (0, h)),
                pl.BlockSpec((1, BLK), lambda h, i, first: (0, i)),
                pl.BlockSpec((seq_len, LANES), lambda h, i, first: (0, 0)),
            ],
            out_specs=[
                pl.BlockSpec((BLK, groups * head_dim), lambda h, i, first: (i, h)),
                pl.BlockSpec((1, 1, 1, wide), lambda h, i, first: (h, i, 0, 0)),
            ],
            scratch_shapes=[
                pltpu.VMEM((1, wide), jnp.float32),
                pltpu.VMEM((1, wide), jnp.float32),
                pltpu.VMEM((head_dim, wide), jnp.float32),
            ],
        ),
        out_shape=[
            jax.ShapeDtypeStruct((seq_len, q_cols), jnp.bfloat16),
            jax.ShapeDtypeStruct((kv_heads, n_blk, 1, wide), jnp.float32),
        ],
        compiler_params=pltpu.CompilerParams(vmem_limit_bytes=48 * 1024 * 1024),
        cost_estimate=pl.CostEstimate(flops=8 * pairs * head_dim, bytes_accessed=8 * seq_len * q_cols, transcendentals=2 * pairs),
        name="attn_fwd",
    )(first_blk, q_all, k_all, v_all, pos, key_pos)


def attn_bwd_kernel(groups, head_dim, q_scale, first_ref, q_ref, k_ref, v_ref, o_ref, do_ref, pos_ref, key_pos_ref, lse_ref, cos_ref, sin_ref,
                    out_ref, delta_scr, dq_scr, dk_scr, dv_scr, dq_out, dk_out, dv_out, dq_sem, kv_sem):
    head, blk = pl.program_id(0), pl.program_id(1)
    n_head, n_blk = pl.num_programs(0), pl.num_programs(1)
    half = head_dim // 2
    wide = groups * BLK
    q_width = groups * head_dim
    slot = blk % 2

    @pl.when(blk == 0)
    def _():
        @pl.loop(0, n_blk)
        def _(i):
            rows = pl.ds(pl.multiple_of(i * BLK, BLK), BLK)
            dk_scr[rows, :] = jnp.zeros((BLK, head_dim), jnp.float32)
            dv_scr[rows, :] = jnp.zeros((BLK, head_dim), jnp.float32)

    q_all = stack_heads(q_ref[...], groups, head_dim)
    do_all = stack_heads(do_ref[...], groups, head_dim)
    o_all = stack_heads(o_ref[...], groups, head_dim)
    floor_row = jnp.concatenate([pos_ref[...]] * groups, axis=1) - WINDOW
    lse_row = lse_ref[0, 0]

    def visit(blocks, with_diagonal):
        if with_diagonal:
            delta = jnp.sum((do_all.astype(jnp.float32) * o_all.astype(jnp.float32)).T, axis=0, keepdims=True)
            delta_scr[...] = delta
        else:
            delta = delta_scr[...]
        rows = [pl.ds(pl.multiple_of(kb * BLK, BLK), BLK) for kb in blocks]
        k_blks = [k_ref[r, :] for r in rows]
        scores = [dot_f32(k_blk, q_all, 1, 1) for k_blk in k_blks]
        d_probs = [dot_f32(v_ref[r, :], do_all, 1, 1) for r in rows]
        dq_new = None
        for i, r in enumerate(rows):
            tanh_s = jnp.tanh(scores[i] * (1.0 / SOFT_CAP))
            keep = keep_mask(key_pos_ref[r, :], floor_row, wide, with_diagonal and i == 0)
            prob = jnp.exp2(jnp.where(keep, tanh_s * (SOFT_CAP * LOG2E) - lse_row, -1e30))
            d_score = (prob * (d_probs[i] - delta) * (1.0 - tanh_s * tanh_s)).astype(jnp.bfloat16)
            dv_scr[r, :] += jnp.dot(prob.astype(jnp.bfloat16), do_all, preferred_element_type=jnp.float32)
            dk_scr[r, :] += jnp.dot(d_score, q_all, preferred_element_type=jnp.float32)
            term = dot_f32(k_blks[i], d_score, 0, 0)
            dq_new = term if dq_new is None else dq_new + term
        if with_diagonal:
            dq_scr[...] = dq_new
        else:
            dq_scr[...] += dq_new

    visit_pairs(visit, first_ref[blk], blk)

    def dq_copy(h, i):
        dst = out_ref.at[pl.ds(pl.multiple_of(i * BLK, BLK), BLK), pl.ds(pl.multiple_of(h * q_width, q_width), q_width)]
        return pltpu.make_async_copy(dq_out.at[slot], dst, dq_sem.at[slot])

    def kv_copy(which, src, h):
        col = n_head * q_width + which * n_head * head_dim + h * head_dim
        dst = out_ref.at[:, pl.ds(pl.multiple_of(col, head_dim), head_dim)]
        return pltpu.make_async_copy(src, dst, kv_sem.at[which])

    @pl.when(head * n_blk + blk >= 2)
    def _():
        dq_copy(head, blk).wait()

    d_q = dq_scr[...].T
    rows = pl.ds(pl.multiple_of(blk * BLK, BLK), BLK)
    cos_t, sin_t = cos_ref[rows, :], sin_ref[rows, :]
    for g in range(groups):
        part = d_q[g * BLK:(g + 1) * BLK, :]
        part = (part * cos_t - pltpu.roll(part, half, 1) * sin_t) * q_scale
        dq_out[slot, :, g * head_dim:(g + 1) * head_dim] = part.astype(dq_out.dtype)
    dq_copy(head, blk).start()

    @pl.when(blk == n_blk - 1)
    def _():
        @pl.loop(0, n_blk)
        def _(i):
            rows = pl.ds(pl.multiple_of(i * BLK, BLK), BLK)
            part = dk_scr[rows, :]
            part = part * cos_ref[rows, :] - pltpu.roll(part, half, 1) * sin_ref[rows, :]
            dk_out[rows, :] = part.astype(dk_out.dtype)
            dv_out[rows, :] = dv_scr[rows, :].astype(dv_out.dtype)

        kv_copy(0, dk_out, head).start()
        kv_copy(1, dv_out, head).start()
        kv_copy(0, dk_out, head).wait()
        kv_copy(1, dv_out, head).wait()

    @pl.when((blk == n_blk - 1) & (head == n_head - 1))
    def _():
        for s in range(2):
            pltpu.make_async_copy(dq_out.at[s], out_ref.at[pl.ds(0, BLK), pl.ds(0, q_width)], dq_sem.at[s]).wait()


def attn_bwd(q_all, k_all, v_all, o_all, d_o, pos, key_pos, lse, first_blk, cos_t, sin_t, groups, head_dim):
    seq_len, q_cols = q_all.shape
    k_cols = k_all.shape[1]
    kv_heads = k_cols // head_dim
    n_blk = seq_len // BLK
    wide = groups * BLK
    pairs = seq_len * seq_len // 4 * groups * kv_heads
    by_q = pl.BlockSpec((BLK, groups * head_dim), lambda h, i, first: (i, h))
    by_h = pl.BlockSpec((seq_len, head_dim), lambda h, i, first: (0, h))
    table = pl.BlockSpec((seq_len, LANES), lambda h, i, first: (0, 0))
    return pl.pallas_call(
        functools.partial(attn_bwd_kernel, groups, head_dim, head_dim ** -0.5),
        grid_spec=pltpu.PrefetchScalarGridSpec(
            num_scalar_prefetch=1,
            grid=(kv_heads, n_blk),
            in_specs=[
                by_q, by_h, by_h, by_q, by_q,
                pl.BlockSpec((1, BLK), lambda h, i, first: (0, i)),
                table,
                pl.BlockSpec((1, 1, 1, wide), lambda h, i, first: (h, i, 0, 0)),
                table, table,
            ],
            out_specs=pl.BlockSpec(memory_space=pl.ANY),
            scratch_shapes=[
                pltpu.VMEM((1, wide), jnp.float32),
                pltpu.VMEM((head_dim, wide), jnp.float32),
                pltpu.VMEM((seq_len, head_dim), jnp.float32),
                pltpu.VMEM((seq_len, head_dim), jnp.float32),
                pltpu.VMEM((2, BLK, groups * head_dim), jnp.bfloat16),
                pltpu.VMEM((seq_len, head_dim), jnp.bfloat16),
                pltpu.VMEM((seq_len, head_dim), jnp.bfloat16),
                pltpu.SemaphoreType.DMA((2,)),
                pltpu.SemaphoreType.DMA((2,)),
            ],
        ),
        out_shape=jax.ShapeDtypeStruct((seq_len, q_cols + 2 * k_cols), jnp.bfloat16),
        compiler_params=pltpu.CompilerParams(vmem_limit_bytes=48 * 1024 * 1024),
        cost_estimate=pl.CostEstimate(flops=20 * pairs * head_dim, bytes_accessed=16 * seq_len * q_cols, transcendentals=2 * pairs),
        name="attn_bwd",
    )(first_blk, q_all, k_all, v_all, o_all, d_o, pos, key_pos, lse, cos_t, sin_t)


SEQ_ORDER = (1, 2, 0)
GW_ORDER = (1, 0, 2)
GWO_ORDER = (2, 1, 0)


def solution(mesh):
    act_spec = P('dp', 'tp', None)
    head_spec = P(None, 'tp', None)
    grad_spec = P('dp', 'tp', None)
    in_specs = (act_spec, P('dp', 'tp'), act_spec, head_spec, head_spec, head_spec, P('tp', None, None), P(None), P(None))
    out_specs = (act_spec, act_spec, grad_spec, grad_spec, grad_spec, P(('dp', 'tp'), None, None), P('dp'), P('dp'))

    def local_body(x_in, positions, grad_out, w_query, w_key, w_value, w_out, gain_pre, gain_post):
        _, _, depth = x_in.shape
        n_dev = mesh.shape['tp']
        heads_loc, head_dim = w_query.shape[1], w_query.shape[2]
        kv_loc = w_key.shape[1]
        groups = heads_loc // kv_loc
        q_cols, k_cols = heads_loc * head_dim, kv_loc * head_dim

        gain_pre_row, gain_post_row = gain_pre[None, :], gain_post[None, :]
        rows = x_in.shape[1]

        def swap(value, bit):
            return lax.ppermute(value, 'tp', [(d, d ^ bit) for d in range(n_dev)])

        def near_of(value):
            return {bit: swap(value, bit) for bit in (1, 2, 4)}

        def pieces_of(value, near):
            mid = value.shape[0] // 2
            far = (swap(near[2][:mid], 4), swap(near[4][mid:], 2))
            other_core = [swap(near[2], 1), swap(near[4], 1)]
            far_other = [swap(part, 1) for part in far]
            return (value, near[1], near[2], near[4], *other_core, *far, *far_other)

        w_out_loc = w_out.reshape(q_cols, depth)
        own, near = {}, {'wo': near_of(w_out_loc)}
        for b in SEQ_ORDER[:2]:
            own[b] = pre_norm(x_in, gain_pre_row, b, 1)
        positions, own = lax.optimization_barrier((positions, own))
        pos_all = lax.all_gather(positions, 'tp', axis=1, tiled=True)
        own, x_held, pos_all = lax.optimization_barrier((own, x_in, pos_all))
        for b in SEQ_ORDER:
            if b not in own:
                own[b] = pre_norm(x_held, gain_pre_row, b, 1)
            near[b] = near_of(own[b])

        seq_len = pos_all.shape[1]
        half = head_dim // 2
        inv_freq = ROPE_THETA ** (-2.0 * jnp.arange(half, dtype=jnp.float32) / head_dim)
        before = pos_all[:, None, :] <= pos_all[:, ::BLK, None] - WINDOW
        first_blk = jnp.sum(before.astype(jnp.int32), axis=-1) // BLK
        w_all = jnp.concatenate([w_query.reshape(depth, q_cols), w_key.reshape(depth, k_cols), w_value.reshape(depth, k_cols)], axis=1)
        w_t = w_all.T
        tables = {}
        for b in SEQ_ORDER:
            angles = pos_all[b].astype(jnp.float32)[:, None] * inv_freq
            cos_h, sin_h = jnp.cos(angles), jnp.sin(angles)
            tables[b] = (jnp.concatenate([cos_h, cos_h], axis=-1), jnp.concatenate([-sin_h, sin_h], axis=-1))
        near[SEQ_ORDER[0]], w_all, w_t, tables, first_blk = lax.optimization_barrier((near[SEQ_ORDER[0]], w_all, w_t, tables, first_blk))
        w_out_pieces = pieces_of(w_out_loc, near['wo'])
        normed = {b: pieces_of(own[b], near[b]) for b in SEQ_ORDER}

        me = lax.axis_index('tp')[None]
        devices = me ^ jnp.array(PIECE_DEVICES, jnp.int32)
        gathered = {}

        saved, d_proj_all = {}, {}
        y_out, d_post = None, jnp.zeros((1, depth), jnp.float32)
        for b in SEQ_ORDER:
            cos_t, sin_t = tables[b]
            pos_b = pos_all[b][None, :]
            key_pos = jnp.broadcast_to(pos_all[b][:, None], (seq_len, LANES))
            q_b, k_b, v_b, whole = qkv_project(devices, normed[b], w_all, cos_t, sin_t, q_cols, k_cols, head_dim)
            gathered[b] = (whole, 0)
            o_b, lse_b = attn_fwd(q_b, k_b, v_b, pos_b, key_pos, first_blk[b], groups, head_dim)
            o_mine = lax.all_to_all(o_b.reshape(n_dev, rows, q_cols), 'tp', split_axis=0, concat_axis=0, tiled=True)
            proj = out_proj(me, o_mine, w_out_pieces)
            y_out, d_proj, d_post = post_norm(proj, x_in, grad_out, gain_post_row, d_post, y_out, b)
            d_proj_all[b] = lax.all_gather(d_proj, 'tp', axis=0, tiled=True)
            saved[b] = (q_b, k_b, v_b, o_b, pos_b, key_pos, lse_b, cos_t, sin_t)

        grad_x, d_pre = None, jnp.zeros((1, depth), jnp.float32)
        d_lin = {}
        for b in SEQ_ORDER:
            q_b, k_b, v_b, o_b, pos_b, key_pos, lse_b, cos_t, sin_t = saved[b]
            d_o = dot_f32(d_proj_all[b], w_out_loc, 1, 1).astype(jnp.bfloat16)
            d_lin[b] = attn_bwd(q_b, k_b, v_b, o_b, d_o, pos_b, key_pos, lse_b, first_blk[b], cos_t, sin_t, groups, head_dim)
            pair = grad_normed_pair(me ^ 1, d_lin[b], w_t, rows)
            from_pair = swap(pair, 1)
            send_x, keep_x, send_y, keep_y = grad_normed_own(me, d_lin[b], w_t, from_pair)
            near_x = swap(send_x, 2)
            near_y = swap(send_y, 4)
            fold_x, fold_y = fold(keep_x, near_x, keep_y, near_y)
            far_x = swap(fold_x, 4)
            far_y = swap(fold_y, 2)
            grad_x, d_pre = pre_grad((keep_x, near_x, far_x, keep_y, near_y, far_y), x_in, grad_out, gain_pre_row, d_pre, grad_x, b)
        grad_wo = None
        for b in GWO_ORDER:
            grad_wo = grad_wo_sum(saved[b][3], d_proj_all[b], grad_wo)
        grads = None
        for b in GW_ORDER:
            grads = grad_w(*gathered[b], rows, d_lin[b], (heads_loc, kv_loc, kv_loc), head_dim, grads, b == GW_ORDER[-1])
        grad_wq, grad_wk, grad_wv = grads
        grad_pre, grad_post = gain_sum(d_pre, d_post, n_dev)
        grad_pre, grad_post = grad_pre[0], grad_post[0]
        return y_out, grad_x, grad_wq, grad_wk, grad_wv, grad_wo.reshape(w_out.shape), grad_pre, grad_post

    return jax.shard_map(local_body, mesh=mesh, in_specs=in_specs, out_specs=out_specs, check_vma=False)
```
